32 devices in a mesh: ea: 4 (over y, x), row: 4 (over z), col: 2 (over core).
Axes of the slice: x: 2, y: 2, z: 4, core: 2. Of those that a mesh axis runs over, the one named last changes fastest.
Arguments:
- weights: float32 [4, 256, 2048], P('ea', 'row', 'col'), parts along dimension 0, may hold values from -6 to 6
- codebook: float32 [4, 16, 2, 256], P('ea', 'col'), parts along dimension 0, may hold values from -4 to 4
- assign: int32 [4, 256, 1024], P('ea', 'row', 'col'), parts along dimension 0, may hold values from 0 to 255
- chol_upper: float32 [4, 2048, 2048], P('ea', 'row', 'col'), parts along dimension 0, may hold values from 0 to 1.4, as said below
- inv_blocks: float32 [4, 16, 128, 128], P('ea', 'col'), parts along dimension 0, may hold values from -1 to 1.5, as said below
Outputs:
- errors: float32 [4, 256, 2048], P('ea', 'row', 'col'), parts along dimension 0
- row_loss: float32 [4, 256], P('ea', 'row'), parts along dimension 0
- codeword_mass: float32 [4, 16, 256], P('ea', 'col'), parts along dimension 0
The draws below stay inside these ranges and needn't reach their ends.
There are 4 independent parts, one for each index of `ea`. The reference program is written for one: setup_inputs(seed, part) draws one part's arguments, and reference() takes and returns one part's arrays. A program takes and returns all parts, laid end to end along the dimension named above; each array names one. Nothing has to cross between parts.
Inputs may be any that keep to these rules, and one draw needn't show every extreme that they name: `chol_upper`: upper triangular with a positive diagonal. inv_blocks[x, b] is the inverse of the diagonal block of chol_upper[x] on rows and columns [b * 128, (b + 1) * 128).
All inputs are finite; a program needn't handle non-finite values.
Results may differ from the reference program's by a relative error of at most 0.0001.
Values sent between devices are 32-bit elements; how exact they have to be, the bound alone decides.
A program may use at most 64 MiB of HBM per device.

```python
import jax
import jax.numpy as jnp
from jax import lax

EXP_PART = 1
COLS = 2048
BLOCK = 128
CODES = 256
ROWS = 256
NBLK = 16


def upper_factor(key):
    folded = jax.random.fold_in(key, 7)
    key_diag, key_near, key_far = jax.random.split(folded, 3)
    diagonal = jax.random.uniform(key_diag, (EXP_PART, COLS), jnp.float32, 0.7, 1.4)
    near_part = jax.random.uniform(key_near, (EXP_PART, COLS, COLS), jnp.float32, 0.0, 0.03)
    far_part = jax.random.uniform(key_far, (EXP_PART, COLS, COLS), jnp.float32, 0.0, 0.03)
    positions = jnp.arange(COLS, dtype=jnp.int32)
    same_block = positions[:, None] // BLOCK == positions[None, :] // BLOCK
    strictly_upper = positions[:, None] < positions[None, :]
    offdiag = jnp.where(same_block[None], near_part, far_part) * strictly_upper[None].astype(jnp.float32)
    return offdiag + diagonal[:, :, None] * jnp.eye(COLS, dtype=jnp.float32)[None]


def draw_chol_upper(key, part):
    return upper_factor(key)


def draw_inv_blocks(key, part):
    factor = upper_factor(key)
    blocked = factor.reshape(EXP_PART, NBLK, BLOCK, NBLK, BLOCK)
    which = jnp.arange(NBLK, dtype=jnp.int32)
    diagonal_blocks = jnp.transpose(blocked[:, which, :, which, :], (1, 0, 2, 3))
    return jnp.linalg.inv(diagonal_blocks)


def place_ends(array, key, smallest, high):
    shape = array.shape
    place = [jax.random.randint(jax.random.fold_in(key, axis), (), 0, shape[axis]) for axis in range(len(shape))]
    array = array.at[tuple(place)].set(smallest)
    longest = shape.index(max(shape))
    place[longest] = (place[longest] + 1) % shape[longest]
    return array.at[tuple(place)].set(high)


def levels(stream_key, shape, cuts, least, top_value):
    gain, own = 1.0, jax.random.fold_in(stream_key, 6)
    for axis_at, blocks in cuts:
        draws = jnp.exp(jax.random.uniform(jax.random.fold_in(own, axis_at), (blocks,), jnp.float32, least / len(cuts), top_value / len(cuts)))
        gain = gain * jnp.repeat(draws, shape[axis_at] // blocks).reshape([-1 if axis == axis_at else 1 for axis in range(len(shape))])
    return gain


def gaussian(key, dims, width, bound, shards=(), kind=jnp.bfloat16):
    drawn = width * jax.random.normal(key, dims, jnp.float32)
    if shards:
        drawn = drawn * levels(key, dims, shards, -0.22, 0.18)
    return jnp.clip(drawn, -bound, bound).astype(kind)


def setup_inputs(seed: int = 0, part: int = 0) -> dict:
    key_of = jax.random.split(jax.random.key(seed), 6)
    own_keys = jax.random.split(jax.random.fold_in(key_of[5], part), 6)
    weights = gaussian(own_keys[0], (EXP_PART, ROWS, COLS), 1.0, 6.0, ((1, 4), (2, 2)), jnp.float32)
    codebook = gaussian(own_keys[1], (EXP_PART, NBLK, 2, CODES), 1.0, 4.0, ((1, 2),), jnp.float32)
    assign = place_ends(jax.random.randint(own_keys[2], (EXP_PART, ROWS, COLS // 2), 0, CODES), jax.random.fold_in(own_keys[2], 1), 0, CODES - 1).astype(jnp.int32)
    chol_upper = draw_chol_upper(jax.random.fold_in(jax.random.fold_in(key_of[5], part), 71), part)
    inv_blocks = draw_inv_blocks(jax.random.fold_in(jax.random.fold_in(key_of[5], part), 71), part)
    return {"weights": weights, "codebook": codebook, "assign": assign, "chol_upper": chol_upper, "inv_blocks": inv_blocks}


def lookup(codebook, assign, half_block, code_count):
    pair_count = assign.shape[2]
    offsets = jnp.arange(pair_count, dtype=jnp.int32) // half_block * code_count
    flat_index = (assign + offsets[None, None, :]).astype(jnp.int32)
    experts = codebook.shape[0]
    code_table = jnp.transpose(codebook, (0, 2, 1, 3)).reshape(experts, 2, -1)

    def select(rows_table, indices):
        return jnp.stack([jnp.take(rows_table[0], indices), jnp.take(rows_table[1], indices)], axis=-1)
    picked = jax.vmap(select)(code_table, flat_index)
    return (picked.reshape(assign.shape[0], assign.shape[1], 2 * pair_count), flat_index)

def mass_by_code(errors, flat_index, segments):
    squared = errors * errors
    extent = errors.shape
    paired = squared.reshape(extent[0], extent[1], extent[2] // 2, 2).sum(axis=3)

    def summed(values, labels):
        return jax.ops.segment_sum(values.reshape(-1), labels.reshape(-1), num_segments=segments)
    return jax.vmap(summed)(paired, flat_index)

def reference(weights, codebook, assign, chol_upper, inv_blocks):
    quantized, flat_index = lookup(codebook, assign, BLOCK // 2, CODES)
    current = weights
    pieces = []
    for number in range(NBLK):
        first_col = number * BLOCK
        finish = first_col + BLOCK
        error_block = jnp.einsum('xrc,xcd->xrd', current[:, :, first_col:finish] - quantized[:, :, first_col:finish], inv_blocks[:, number], precision=lax.Precision.HIGHEST)
        pieces.append(error_block)
        if finish < COLS:
            change = jnp.einsum('xrc,xcd->xrd', error_block, chol_upper[:, first_col:finish, finish:], precision=lax.Precision.HIGHEST)
            current = jnp.concatenate([current[:, :, :finish], current[:, :, finish:] - change], axis=2)
    errors = jnp.concatenate(pieces, axis=2)
    row_loss = jnp.sum(errors * errors, axis=2)
    codeword_mass = mass_by_code(errors, flat_index, NBLK * CODES).reshape(EXP_PART, NBLK, CODES)
    return (errors, row_loss, codeword_mass)
```

```python
import functools

import jax
import jax.numpy as jnp
from jax import lax
from jax.experimental import pallas as pl
from jax.experimental.pallas import tpu as pltpu
from jax.sharding import PartitionSpec as P

F32 = jnp.float32
BF16 = jnp.bfloat16
LOW = 16
PIECES = 2
scope = jax.named_scope


def halves(value):
    high = value.astype(BF16)
    return high, (value - high.astype(F32)).astype(BF16)


def dot(a, b):
    return jnp.dot(a, b, preferred_element_type=F32)


def dot3(a, b_high, b_low):
    rows = a.shape[0]
    high, low = halves(a)
    both = dot(jnp.concatenate([high, low], axis=0), b_high)
    return both[:rows] + both[rows:] + dot(high, b_low)


def dot_full(a, b):
    b_high, b_low = halves(b)
    return dot3(a, b_high, b_low)


def take(table, index):
    return jnp.take_along_axis(table, index, axis=1, mode="promise_in_bounds")


def kernel(
    nr, nc,
    weights_hbm, codebook_hbm, assign_hbm, inverse_hbm, factor,
    errors_out, loss_out, mass_out,
    weights, codebook, assign, inverse, u_raw, u_high, u_low, v_full, v_high, v_low, delta, codes, delta_in, run_in, run_out,
    err_block, err_own, mass_all, loss_all,
    u_sem, d_send, d_recv, run_send, run_recv, core_send, core_recv, own_send, own_recv,
    mass_send, mass_recv, loss_send, loss_recv,
):
    z = lax.axis_index("row")
    c = lax.axis_index("col")
    rows, width = weights.shape
    span = factor.shape[0]
    m = width // span
    block = inverse.shape[1]
    k = span // block
    code_count = codebook.shape[2]
    owner = z // m
    slot = z % m
    steps = nr * PIECES
    piece = rows // PIECES
    is_owner = c == owner

    def remote(src, dst, send, recv, row, col):
        return pltpu.make_async_remote_copy(
            src_ref=src, dst_ref=dst, send_sem=send, recv_sem=recv,
            device_id={"row": row, "col": col}, device_id_type=pl.DeviceIdType.MESH,
        )

    loads = [
        pltpu.make_async_copy(source, target, u_sem.at[number])
        for number, (source, target) in enumerate((
            (assign_hbm, assign), (codebook_hbm, codebook), (weights_hbm, weights),
            (inverse_hbm, inverse), (factor, u_raw),
        ))
    ]
    for load in loads:
        load.start()

    barrier = pltpu.get_barrier_semaphore()
    for step in range(1, nr * nc):
        other = lax.rem(z * nc + c + step, nr * nc)
        pl.semaphore_signal(
            barrier, inc=1, device_id={"row": other // nc, "col": other % nc},
            device_id_type=pl.DeviceIdType.MESH,
        )

    with scope("first_loads"):
        for load in loads[:3]:
            load.wait()

    lane = lax.broadcasted_iota(jnp.int32, (rows, block), 1)
    for b in range(width // block):
        first = b * (block // 2)
        tile = first // block * block
        code = take(assign[:, tile:tile + block], first - tile + lane // 2)
        codes[b] = code
        inner = code % block
        value = jnp.zeros((rows, block), F32)
        for part in range(code_count // block):
            picked = []
            for comp in range(2):
                table = codebook[b, comp:comp + 1, part * block:(part + 1) * block]
                picked.append(take(jnp.broadcast_to(table, (rows, block)), inner))
            both = jnp.where(lane % 2 == 0, picked[0], picked[1])
            value = jnp.where(code // block == part, both, value)
        j, at = b * block // span, b * block % span
        delta[j, :, at:at + block] = weights[:, b * block:(b + 1) * block] - value

    @pl.when(z == 0)
    def _():
        run_in[...] = jnp.zeros_like(run_in)

    @pl.when(z > 0)
    def _():
        with scope("entry"):
            pl.semaphore_wait(barrier, nr * nc - 1)

    def delta_copy(j):
        return remote(delta.at[j], delta_in.at[z], d_send.at[j], d_recv.at[z], c * m + j, c)

    for j in range(m):
        @pl.when(c * m + j < z)
        def _():
            delta_copy(j).start()

    with scope("factor_loads"):
        for load in loads[3:]:
            load.wait()

    @pl.when(is_owner)
    def _():
        v_full[...] = jnp.zeros_like(v_full)
        base = slot * span

        def invert(lo, hi):
            if hi - lo == 1:
                v_full[lo * block:hi * block, lo * block:hi * block] = inverse[slot * k + lo]
                return
            mid = (lo + hi) // 2
            invert(lo, mid)
            invert(mid, hi)
            top, middle, end = lo * block, mid * block, hi * block
            right = u_raw[top:middle, pl.ds(pl.multiple_of(base + middle, block), end - middle)]
            product = dot_full(v_full[top:middle, top:middle], right)
            v_full[top:middle, middle:end] = -dot_full(product, v_full[middle:end, middle:end])

        invert(0, k)
        high, low = halves(v_full[...])
        v_high[...] = high
        v_low[...] = low

    for j in range(m):
        @pl.when(c * m + j > z)
        def _():
            high, low = halves(u_raw[:, j * span:(j + 1) * span])
            u_high[:, j * span:(j + 1) * span] = high
            u_low[:, j * span:(j + 1) * span] = low

    @pl.when(z == 0)
    def _():
        with scope("entry"):
            pl.semaphore_wait(barrier, nr * nc - 1)

    def run_copy(g, j):
        return remote(run_out.at[g, j], run_in.at[g, j], run_send.at[g, j], run_recv.at[g, j], z + 1, c)

    def core_copy(g, col):
        return remote(err_block.at[g], err_block.at[g], core_send.at[g, col], core_recv.at[g], z, col)

    def part_rows(q):
        return pl.ds(pl.multiple_of(q % PIECES * piece, piece), piece)

    def own_copy(q):
        return remote(
            err_block.at[q], err_own.at[slot, part_rows(q)],
            own_send.at[q], own_recv.at[slot, q % PIECES], q // PIECES, owner,
        )

    def arrived(ref, sem):
        pltpu.make_async_copy(ref, ref, sem).wait()

    def held(q, j):
        return (c > owner) & (q >= PIECES) & (j > 0)

    def stage(q, _):
        g = q // PIECES
        at = part_rows(q)

        @pl.when(is_owner)
        def _():
            @pl.when(z > 0)
            def _():
                with scope("wait_own_sum"):
                    arrived(run_in.at[q, slot], run_recv.at[q, slot])

            @pl.when(g > z)
            def _():
                @pl.when(q % PIECES == 0)
                def _():
                    with scope("wait_delta"):
                        arrived(delta_in.at[g], d_recv.at[g])

                run_in[q, slot] = run_in[q, slot] + delta_in[g, at]

            @pl.when(g == z)
            def _():
                run_in[q, slot] = run_in[q, slot] + delta[slot, at]

            error = dot3(run_in[q, slot], v_high[...], v_low[...])
            err_block[q] = error

            @pl.when(g == z)
            def _():
                err_own[slot, at] = error

            for col in range(1, nc):
                @pl.when(col > c)
                def _():
                    core_copy(q, col).start()

            @pl.when(g < z)
            def _():
                own_copy(q).start()

        @pl.when(c > owner)
        def _():
            with scope("wait_core"):
                arrived(err_block.at[q], core_recv.at[q])

        for j in range(m):
            @pl.when(c * m + j > z)
            def _():
                change = dot3(
                    err_block[q], u_high[:, j * span:(j + 1) * span], u_low[:, j * span:(j + 1) * span]
                )
                local = jnp.where(g == z, delta[j, at], 0.0)
                later = held(q, j)

                @pl.when(later)
                def _():
                    run_out[q, j] = local - change

                @pl.when(jnp.logical_not(later))
                def _():
                    @pl.when(z > 0)
                    def _():
                        with scope("wait_near_sum"):
                            arrived(run_in.at[q, j], run_recv.at[q, j])

                    run_out[q, j] = run_in[q, j] + local - change
                    run_copy(q, j).start()

        return 0

    lax.fori_loop(0, steps, stage, 0)

    for j in range(1, m):
        @pl.when((c * m + j > z) & (c > owner))
        def _():
            def release(q, _):
                @pl.when(z > 0)
                def _():
                    with scope("wait_far_sum"):
                        arrived(run_in.at[q, j], run_recv.at[q, j])
                    run_out[q, j] = run_out[q, j] + run_in[q, j]

                run_copy(q, j).start()
                return 0

            lax.fori_loop(PIECES, steps, release, 0)

    @pl.when(c == nc - 1)
    def _():
        def upward(i, _):
            q = steps - 1 - i

            @pl.when(q // PIECES > z)
            def _():
                own_copy(q).start()

            return 0

        lax.fori_loop(0, steps, upward, 0)

    high_count = code_count // LOW
    group = 2 * high_count
    chunk = 8
    start = jnp.clip(z - c * m, 0, m - 1)

    def finish(turn, loss):
        j = lax.rem(start + turn, m)

        @pl.when(c * m + j != z)
        def _():
            with scope("wait_error"):
                for h in range(PIECES):
                    arrived(err_own.at[j, h * piece:(h + 1) * piece], own_recv.at[j, h])

        error = err_own[j]
        errors_out[:, pl.ds(pl.multiple_of(j * span, span), span)] = error
        squared = error * error
        loss = loss + lax.dot_general(
            jnp.ones((8, span), F32), squared, (((1,), (1,)), ((), ())),
            precision=lax.Precision.HIGHEST, preferred_element_type=F32,
        )

        def gather(step, total):
            at = pl.ds(pl.multiple_of(step * chunk, chunk), chunk)
            iota_high = lax.broadcasted_iota(jnp.int32, (high_count, block), 0)
            iota_low = lax.broadcasted_iota(jnp.int32, (LOW, block), 0)
            left, right = [], []
            for b in range(k):
                code = codes[j * k + b, at, :]
                value = err_own[j, at, b * block:(b + 1) * block]
                value = value * value
                coarse = value.astype(BF16).astype(F32)
                fine = value - coarse
                code_high, code_low = code // LOW, code % LOW
                top, bottom, marks = [], [], []
                for r in range(chunk):
                    hit = jnp.broadcast_to(code_high[r:r + 1], (high_count, block)) == iota_high
                    top.append(jnp.where(hit, jnp.broadcast_to(coarse[r:r + 1], (high_count, block)), 0.0).astype(BF16))
                    bottom.append(jnp.where(hit, jnp.broadcast_to(fine[r:r + 1], (high_count, block)), 0.0).astype(BF16))
                    low_hit = jnp.broadcast_to(code_low[r:r + 1], (LOW, block)) == iota_low
                    marks.append(jnp.where(low_hit, 1.0, 0.0).astype(BF16))
                left += [jnp.concatenate(top, axis=1), jnp.concatenate(bottom, axis=1)]
                right.append(jnp.concatenate(marks, axis=1))
            return total + lax.dot_general(
                jnp.concatenate(left, axis=0), jnp.concatenate(right, axis=0),
                (((1,), (1,)), ((), ())), preferred_element_type=F32,
            )

        total = lax.fori_loop(0, rows // chunk, gather, jnp.zeros((k * group, k * LOW), F32), unroll=4)
        row_id = lax.broadcasted_iota(jnp.int32, total.shape, 0)
        col_id = lax.broadcasted_iota(jnp.int32, total.shape, 1)
        total = jnp.where(row_id // group == col_id // LOW, total, 0.0)
        wide_row = lax.broadcasted_iota(jnp.int32, (k * LOW, code_count), 0)
        wide_col = lax.broadcasted_iota(jnp.int32, (k * LOW, code_count), 1)
        spread = jnp.where(wide_row % LOW == wide_col % LOW, 1.0, 0.0)
        spread = jnp.dot(total, spread, precision=lax.Precision.HIGHEST, preferred_element_type=F32)
        out_row = lax.broadcasted_iota(jnp.int32, spread.shape, 0)
        out_col = lax.broadcasted_iota(jnp.int32, spread.shape, 1)
        spread = jnp.where(out_row % high_count == out_col // LOW, spread, 0.0)
        for b in range(k):
            mass_all[z, pl.ds(j * k + b, 1), :] = jnp.sum(
                spread[b * group:(b + 1) * group], axis=0, keepdims=True
            )
        return loss

    loss_all[c, :, :rows] = lax.fori_loop(0, m, finish, jnp.zeros((8, rows), F32))

    def mass_copy(row):
        return remote(mass_all.at[z], mass_all.at[z], mass_send.at[row], mass_recv.at[z], row, c)

    def loss_copy(col):
        return remote(loss_all.at[c], loss_all.at[c], loss_send.at[col], loss_recv.at[c], z, col)

    for row in range(nr):
        @pl.when(row != z)
        def _():
            mass_copy(row).start()
    for col in range(nc):
        @pl.when(col != c)
        def _():
            loss_copy(col).start()

    for j in range(m):
        @pl.when(c * m + j < z)
        def _():
            delta_copy(j).wait_send()

    def drain(q, _):
        for j in range(m):
            @pl.when(c * m + j > z)
            def _():
                run_copy(q, j).wait_send()

        @pl.when(is_owner)
        def _():
            for col in range(1, nc):
                @pl.when(col > c)
                def _():
                    core_copy(q, col).wait_send()

        @pl.when((is_owner & (q // PIECES < z)) | ((c == nc - 1) & (q // PIECES > z)))
        def _():
            own_copy(q).wait_send()

        return 0

    with scope("drain"):
        lax.fori_loop(0, steps, drain, 0)

    for col in range(nc):
        @pl.when(col != c)
        def _():
            with scope("wait_loss"):
                arrived(loss_all.at[col], loss_recv.at[col])
    loss_sum = loss_all[0, 0:1, :rows]
    for col in range(1, nc):
        loss_sum = loss_sum + loss_all[col, 0:1, :rows]
    loss_out[...] = loss_sum
    for row in range(nr):
        @pl.when(row != z)
        def _():
            with scope("wait_mass"):
                arrived(mass_all.at[row], mass_recv.at[row])
    mass_sum = mass_all[0]
    for row in range(1, nr):
        mass_sum = mass_sum + mass_all[row]
    mass_out[...] = mass_sum

    for row in range(nr):
        @pl.when(row != z)
        def _():
            mass_copy(row).wait_send()
    for col in range(nc):
        @pl.when(col != c)
        def _():
            loss_copy(col).wait_send()


def store(errors, loss, mass, errors_out, loss_out, mass_out, sems):
    copies = [
        pltpu.make_async_copy(source, target, sems.at[number])
        for number, (source, target) in enumerate(((errors, errors_out), (loss, loss_out), (mass, mass_out)))
    ]
    for copy in copies:
        copy.start()
    for copy in copies:
        copy.wait()


def local(nr, nc, weights, codebook, assign, chol_upper, inv_blocks):
    rows, width = weights.shape[1:]
    span = chol_upper.shape[1]
    m = width // span
    steps, piece = nr * PIECES, rows // PIECES
    blocks, code_count = codebook.shape[1], codebook.shape[3]
    block = inv_blocks.shape[2]
    dma = pltpu.SemaphoreType.DMA
    vmem = pl.BlockSpec(memory_space=pltpu.VMEM)
    shapes = ((rows, width), (1, rows), (blocks, code_count))
    results = pl.pallas_call(
        functools.partial(kernel, nr, nc),
        out_shape=tuple(pltpu.VMEM(shape, F32) for shape in shapes),
        in_specs=[pl.BlockSpec(memory_space=pltpu.HBM)] * 5,
        out_specs=(vmem, vmem, vmem),
        scratch_shapes=[
            pltpu.VMEM(weights.shape[1:], F32),
            pltpu.VMEM(codebook.shape[1:], F32),
            pltpu.VMEM(assign.shape[1:], jnp.int32),
            pltpu.VMEM(inv_blocks.shape[1:], F32),
            pltpu.VMEM((span, width), F32),
            pltpu.VMEM((span, width), BF16),
            pltpu.VMEM((span, width), BF16),
            pltpu.VMEM((span, span), F32),
            pltpu.VMEM((span, span), BF16),
            pltpu.VMEM((span, span), BF16),
            pltpu.VMEM((m, rows, span), F32),
            pltpu.VMEM((blocks, rows, block), jnp.int32),
            pltpu.VMEM((nr, rows, span), F32),
            pltpu.VMEM((steps, m, piece, span), F32),
            pltpu.VMEM((steps, m, piece, span), F32),
            pltpu.VMEM((steps, piece, span), F32),
            pltpu.VMEM((m, rows, span), F32),
            pltpu.VMEM((nr, blocks, code_count), F32),
            pltpu.VMEM((nc, 8, max(rows, 128)), F32),
            dma((5,)),
            dma((m,)), dma((nr,)),
            dma((steps, m)), dma((steps, m)),
            dma((steps, nc)), dma((steps,)),
            dma((steps,)), dma((m, PIECES)),
            dma((nr,)), dma((nr,)),
            dma((nc,)), dma((nc,)),
        ],
        compiler_params=pltpu.CompilerParams(
            collective_id=0, has_side_effects=True, vmem_limit_bytes=40 * 1024 * 1024
        ),
    )(*(pltpu.with_memory_space_constraint(value[0], pltpu.HBM) for value in (
        weights, codebook, assign, inv_blocks, chol_upper,
    )))
    errors, loss, mass = pl.pallas_call(
        store,
        out_shape=tuple(jax.ShapeDtypeStruct(shape, F32) for shape in shapes),
        in_specs=[vmem] * 3,
        out_specs=[pl.BlockSpec(memory_space=pltpu.HBM)] * 3,
        scratch_shapes=[dma((3,))],
        compiler_params=pltpu.CompilerParams(vmem_limit_bytes=1024 * 1024),
    )(*results)
    return errors[None], loss, mass[None]


def solution(mesh):
    return jax.shard_map(
        functools.partial(local, mesh.shape["row"], mesh.shape["col"]),
        mesh=mesh,
        in_specs=(
            P("ea", "row", "col"),
            P("ea", "col", None, None),
            P("ea", "row", "col"),
            P("ea", "row", "col"),
            P("ea", "col", None, None),
        ),
        out_specs=(P("ea", "row", "col"), P("ea", "row"), P("ea", "col", None)),
        check_vma=False,
    )
```

```python
import functools

import jax
import jax.numpy as jnp
from jax import lax
from jax.experimental import pallas as pl
from jax.experimental.pallas import tpu as pltpu
from jax.sharding import PartitionSpec as P

F32 = jnp.float32
BF16 = jnp.bfloat16
LOW = 16
PIECES = 2
scope = jax.named_scope


def halves(value):
    high = value.astype(BF16)
    return high, (value - high.astype(F32)).astype(BF16)


def dot(a, b):
    return jnp.dot(a, b, preferred_element_type=F32)


def dot3(a, b_high, b_low):
    rows = a.shape[0]
    high, low = halves(a)
    both = dot(jnp.concatenate([high, low], axis=0), b_high)
    return both[:rows] + both[rows:] + dot(high, b_low)


def dot_full(a, b):
    b_high, b_low = halves(b)
    return dot3(a, b_high, b_low)


def take(table, index):
    return jnp.take_along_axis(table, index, axis=1, mode="promise_in_bounds")


def kernel(
    nr, nc,
    weights_hbm, codebook_hbm, assign_hbm, inverse_hbm, factor,
    errors_out, loss_out, mass_out,
    weights, codebook, assign, inverse, u_raw, u_high, u_low, triangle, v_full, v_high, v_low, w_high, w_low,
    delta, codes, delta_in, codes_in, run_in, run_out, last_in, last_out,
    err_block, err_own, tally, mass_all, mass_own, mass_sent, loss_all,
    u_sem, d_send, d_recv, code_send, code_recv, tri_send, tri_recv, run_send, run_recv, last_send, last_recv,
    core_send, core_recv, own_send, own_recv, part_send, part_recv, mass_send, mass_recv, loss_send, loss_recv,
):
    z = lax.axis_index("row")
    c = lax.axis_index("col")
    rows, width = weights.shape
    span = factor.shape[0]
    m = width // span
    block = inverse.shape[1]
    k = span // block
    code_count = codebook.shape[2]
    owner = z // m
    slot = z % m
    steps = nr * PIECES
    piece = rows // PIECES
    final = nr - 1
    is_owner = (c == owner) & (z < final)
    is_last = c == nc - 1

    def remote(src, dst, send, recv, row, col):
        return pltpu.make_async_remote_copy(
            src_ref=src, dst_ref=dst, send_sem=send, recv_sem=recv,
            device_id={"row": row, "col": col}, device_id_type=pl.DeviceIdType.MESH,
        )

    def arrived(ref, sem):
        pltpu.make_async_copy(ref, ref, sem).wait()

    loads = [
        pltpu.make_async_copy(source, target, u_sem.at[number])
        for number, (source, target) in enumerate((
            (assign_hbm, assign), (codebook_hbm, codebook), (weights_hbm, weights),
            (inverse_hbm, inverse), (factor, u_raw),
        ))
    ]
    for load in loads:
        load.start()

    barrier = pltpu.get_barrier_semaphore()
    for step in range(1, nr * nc):
        other = lax.rem(z * nc + c + step, nr * nc)
        pl.semaphore_signal(
            barrier, inc=1, device_id={"row": other // nc, "col": other % nc},
            device_id_type=pl.DeviceIdType.MESH,
        )

    def enter():
        with scope("entry"):
            pl.semaphore_wait(barrier, nr * nc - 1)

    def order(place):
        if nr < 3:
            return place
        return jnp.where(place == nr - 2, nr - 1, jnp.where(place == nr - 1, nr - 2, place))

    def group(q):
        return order(q // PIECES)

    def part_rows(q):
        return pl.ds(pl.multiple_of(q % PIECES * piece, piece), piece)

    def delta_copy(j):
        return remote(delta.at[j], delta_in.at[z], d_send.at[j], d_recv.at[z], c * m + j, c)

    def code_copy(j):
        return remote(codes.at[j * k:(j + 1) * k], codes_in.at[z], code_send.at[j], code_recv.at[z], c * m + j, 0)

    def code_sent(j):
        return (c * m + j <= z) & (c * m + j < final) & ((c > 0) | (c * m + j < z))

    def tri_copy(row, i):
        low = (m - 1) * span
        return remote(
            u_raw.at[i * block:(i + 1) * block, low + (i + 1) * block:low + span],
            triangle.at[i * block:(i + 1) * block, (i + 1) * block:span],
            tri_send.at[row, i], tri_recv.at[i], row, c,
        )

    def run_copy(q, j):
        return remote(run_out.at[q, j], run_in.at[q, j], run_send.at[q, j], run_recv.at[q, j], z + 1, c)

    def last_copy(q):
        return remote(
            last_out.at[q], last_in.at[z, q % PIECES], last_send.at[q], last_recv.at[z, q % PIECES], group(q), c
        )

    def core_copy(q, col):
        return remote(err_block.at[q], err_block.at[q], core_send.at[q, col], core_recv.at[q], z, col)

    def own_copy(q):
        return remote(
            err_block.at[q], err_own.at[slot, part_rows(q)],
            own_send.at[q], own_recv.at[slot, q % PIECES], group(q), owner,
        )

    with scope("first_loads"):
        for load in loads[:3]:
            load.wait()

    lane = lax.broadcasted_iota(jnp.int32, (rows, block), 1)
    for b in range(width // block):
        first = b * (block // 2)
        tile = first // block * block
        code = take(assign[:, tile:tile + block], first - tile + lane // 2)
        codes[b] = code
        inner = code % block
        value = jnp.zeros((rows, block), F32)
        for part in range(code_count // block):
            picked = []
            for comp in range(2):
                table = codebook[b, comp:comp + 1, part * block:(part + 1) * block]
                picked.append(take(jnp.broadcast_to(table, (rows, block)), inner))
            both = jnp.where(lane % 2 == 0, picked[0], picked[1])
            value = jnp.where(code // block == part, both, value)
        j, at = b * block // span, b * block % span
        delta[j, :, at:at + block] = weights[:, b * block:(b + 1) * block] - value

    @pl.when(z > 0)
    def _():
        enter()

    for j in range(m):
        @pl.when(c * m + j < z)
        def _():
            delta_copy(j).start()

    with scope("factor_loads"):
        for load in loads[3:]:
            load.wait()

    @pl.when((z == final) & is_last)
    def _():
        for row in reversed(range(final)):
            for i in range(k - 1):
                tri_copy(row, i).start()

    def inverted(first, right):
        v_full[...] = jnp.zeros_like(v_full)

        def invert(lo, hi):
            if hi - lo == 1:
                v_full[lo * block:hi * block, lo * block:hi * block] = inverse[first + lo]
                return
            mid = (lo + hi) // 2
            invert(lo, mid)
            invert(mid, hi)
            top, middle, end = lo * block, mid * block, hi * block
            product = dot_full(v_full[top:middle, top:middle], right(top, middle, end))
            v_full[top:middle, middle:end] = -dot_full(product, v_full[middle:end, middle:end])

        invert(0, k)
        return halves(v_full[...])

    @pl.when(is_owner)
    def _():
        base = slot * span
        high, low = inverted(slot * k, lambda top, middle, end: u_raw[
            top:middle, pl.ds(pl.multiple_of(base + middle, block), end - middle)
        ])
        v_high[...] = high
        v_low[...] = low

    for j in range(m):
        @pl.when(c * m + j > z)
        def _():
            high, low = halves(u_raw[:, j * span:(j + 1) * span])
            u_high[:, j * span:(j + 1) * span] = high
            u_low[:, j * span:(j + 1) * span] = low

    def invert_last():
        @pl.when(z == final)
        def _():
            triangle[...] = u_raw[:, (m - 1) * span:]

        @pl.when(z < final)
        def _():
            with scope("wait_triangle"):
                for i in range(k - 1):
                    part = triangle.at[i * block:(i + 1) * block, (i + 1) * block:span]
                    arrived(part, tri_recv.at[i])

        high, low = inverted((m - 1) * k, lambda top, middle, end: triangle[top:middle, middle:end])
        w_high[...] = high
        w_low[...] = low

    @pl.when(z == 0)
    def _():
        enter()

    for j in range(m):
        @pl.when(code_sent(j))
        def _():
            code_copy(j).start()

        @pl.when((c == 0) & (z == j) & (z < final))
        def _():
            codes_in[z] = codes[j * k:(j + 1) * k]

    late_core = (z == 0) & (c > owner)

    def stage(q, _):
        g = group(q)
        at = part_rows(q)

        @pl.when(is_last & (((z == final) & (q == 0)) | ((z == final - 1) & (q == PIECES))))
        def _():
            invert_last()

        @pl.when(is_owner)
        def _():
            @pl.when(z == 0)
            def _():
                run_in[q, slot] = jnp.zeros((piece, span), F32)

            @pl.when(z > 0)
            def _():
                with scope("wait_own_sum"):
                    arrived(run_in.at[q, slot], run_recv.at[q, slot])

            @pl.when(g > z)
            def _():
                @pl.when(q % PIECES == 0)
                def _():
                    with scope("wait_delta"):
                        arrived(delta_in.at[g], d_recv.at[g])

                run_in[q, slot] = run_in[q, slot] + delta_in[g, at]

            @pl.when(g == z)
            def _():
                run_in[q, slot] = run_in[q, slot] + delta[slot, at]

            error = dot3(run_in[q, slot], v_high[...], v_low[...])
            err_block[q] = error

            @pl.when(g == z)
            def _():
                err_own[slot, at] = error

            for col in range(nc):
                @pl.when((col > c) | ((col == 0) & (c > 0) & (g >= z)))
                def _():
                    core_copy(q, col).start()

            @pl.when(g < z)
            def _():
                own_copy(q).start()

        @pl.when((c > owner) & (z < final))
        def _():
            with scope("wait_core"):
                arrived(err_block.at[q], core_recv.at[q])

        late = late_core & (q >= PIECES)
        for j in range(m):
            target = c * m + j

            @pl.when((target > z) & (target < final))
            def _():
                change = dot3(
                    err_block[q], u_high[:, j * span:(j + 1) * span], u_low[:, j * span:(j + 1) * span]
                )
                run_out[q, j] = jnp.where(g == z, delta[j, at], 0.0) - change

                @pl.when(z > 0)
                def _():
                    with scope("wait_near_sum"):
                        arrived(run_in.at[q, j], run_recv.at[q, j])
                    run_out[q, j] = run_out[q, j] + run_in[q, j]

                @pl.when(jnp.logical_not(late))
                def _():
                    run_copy(q, j).start()

        @pl.when(is_last & (z < final))
        def _():
            j = m - 1
            change = dot3(
                err_block[q], u_high[:, j * span:(j + 1) * span], u_low[:, j * span:(j + 1) * span]
            )

            @pl.when(g == z)
            def _():
                last_in[z, q % PIECES] = change

            @pl.when(g != z)
            def _():
                last_out[q] = change

                @pl.when(jnp.logical_not(late))
                def _():
                    last_copy(q).start()

        return 0

    lax.fori_loop(0, steps, stage, 0)

    for j in range(m):
        @pl.when(late_core & (c * m + j < final))
        def _():
            def release(q, _):
                run_copy(q, j).start()
                return 0

            lax.fori_loop(PIECES, steps, release, 0)

    @pl.when(late_core & is_last)
    def _():
        def release(i, _):
            last_copy(steps - 1 - i).start()
            return 0

        lax.fori_loop(0, steps - PIECES, release, 0)

    @pl.when(is_last & (z < final))
    def _():
        def upward(i, _):
            q = steps - 1 - i

            @pl.when(group(q) > z)
            def _():
                own_copy(q).start()

            return 0

        lax.fori_loop(0, steps, upward, 0)

    @pl.when(is_last & (z < final - 1))
    def _():
        invert_last()

    high_count = code_count // LOW
    fold = 2 * high_count
    chunk = 8

    def count(error_at, code_at):
        def gather(step, total):
            at = pl.ds(pl.multiple_of(step * chunk, chunk), chunk)
            iota_high = lax.broadcasted_iota(jnp.int32, (high_count, block), 0)
            iota_low = lax.broadcasted_iota(jnp.int32, (LOW, block), 0)
            left, right = [], []
            for b in range(k):
                code = code_at(b)[at, :]
                value = error_at[at, b * block:(b + 1) * block]
                value = value * value
                coarse = value.astype(BF16).astype(F32)
                fine = value - coarse
                code_high, code_low = code // LOW, code % LOW
                top, bottom, marks = [], [], []
                for r in range(chunk):
                    hit = jnp.broadcast_to(code_high[r:r + 1], (high_count, block)) == iota_high
                    top.append(jnp.where(hit, jnp.broadcast_to(coarse[r:r + 1], (high_count, block)), 0.0).astype(BF16))
                    bottom.append(jnp.where(hit, jnp.broadcast_to(fine[r:r + 1], (high_count, block)), 0.0).astype(BF16))
                    low_hit = jnp.broadcast_to(code_low[r:r + 1], (LOW, block)) == iota_low
                    marks.append(jnp.where(low_hit, 1.0, 0.0).astype(BF16))
                left += [jnp.concatenate(top, axis=1), jnp.concatenate(bottom, axis=1)]
                right.append(jnp.concatenate(marks, axis=1))
            return total + lax.dot_general(
                jnp.concatenate(left, axis=0), jnp.concatenate(right, axis=0),
                (((1,), (1,)), ((), ())), preferred_element_type=F32,
            )

        total = lax.fori_loop(0, piece // chunk, gather, jnp.zeros(tally.shape, F32), unroll=4)
        tally[...] = tally[...] + total

    def spread(store):
        total = tally[...]
        row_id = lax.broadcasted_iota(jnp.int32, total.shape, 0)
        col_id = lax.broadcasted_iota(jnp.int32, total.shape, 1)
        total = jnp.where(row_id // fold == col_id // LOW, total, 0.0)
        wide_row = lax.broadcasted_iota(jnp.int32, (k * LOW, code_count), 0)
        wide_col = lax.broadcasted_iota(jnp.int32, (k * LOW, code_count), 1)
        wide = jnp.where(wide_row % LOW == wide_col % LOW, 1.0, 0.0)
        wide = jnp.dot(total, wide, precision=lax.Precision.HIGHEST, preferred_element_type=F32)
        out_row = lax.broadcasted_iota(jnp.int32, wide.shape, 0)
        out_col = lax.broadcasted_iota(jnp.int32, wide.shape, 1)
        wide = jnp.where(out_row % high_count == out_col // LOW, wide, 0.0)
        for b in range(k):
            store(b, jnp.sum(wide[b * fold:(b + 1) * fold], axis=0, keepdims=True))
        tally[...] = jnp.zeros_like(tally)

    tally[...] = jnp.zeros_like(tally)
    mass_all[z] = jnp.zeros(mass_all.shape[1:], F32)
    counts = (c == 0) & (z < final)

    def part_copy(row):
        return remote(mass_sent, mass_own.at[slot], part_send.at[row], part_recv.at[slot], row, owner)

    def part_remote(row):
        return counts & ((row != z) | (owner != 0))

    @pl.when(counts)
    def _():
        def own_part(q, _):
            g = group(q)

            @pl.when(g >= z)
            def _():
                with scope("wait_part"):
                    @pl.when(owner != 0)
                    def _():
                        arrived(err_block.at[q], core_recv.at[q])

                    @pl.when(((g != z) | (owner != 0)) & (q % PIECES == 0))
                    def _():
                        arrived(codes_in.at[g], code_recv.at[g])

                count(err_block.at[q], lambda b: codes_in.at[g, b, part_rows(q)])

            return 0

        lax.fori_loop(0, steps, own_part, 0)

        def store(b, value):
            mass_sent[b:b + 1, :] = value

        spread(store)

        @pl.when(owner == 0)
        def _():
            mass_own[slot] = mass_sent[...]

    for row in range(nr):
        @pl.when(part_remote(row))
        def _():
            part_copy(row).start()

    def own_spread(j):
        def store(b, value):
            mass_all[z, j * k + b:j * k + b + 1, :] = value

        spread(store)

    for j in range(m):
        @pl.when((c * m + j > z) & (c * m + j < final))
        def _():
            for h in range(PIECES):
                with scope("wait_down"):
                    arrived(err_own.at[j, h * piece:(h + 1) * piece], own_recv.at[j, h])
                count(
                    err_own.at[j, h * piece:(h + 1) * piece],
                    lambda b: codes.at[j * k + b, h * piece:(h + 1) * piece],
                )
            own_spread(j)

    @pl.when(is_last)
    def _():
        j = m - 1
        for h in range(PIECES):
            at = slice(h * piece, (h + 1) * piece)
            with scope("wait_last"):
                for row in range(final):
                    @pl.when(row != z)
                    def _():
                        arrived(last_in.at[row, h], last_recv.at[row, h])
            total = delta[j, at]
            for row in range(final):
                total = total - last_in[row, h]
            err_own[j, at] = dot3(total, w_high[...], w_low[...])
            count(err_own.at[j, at], lambda b: codes.at[j * k + b, at])
        own_spread(j)

    def mass_copy(row):
        return remote(mass_all.at[z], mass_all.at[z], mass_send.at[row], mass_recv.at[z], row, c)

    def loss_copy(col):
        return remote(loss_all.at[c], loss_all.at[c], loss_send.at[col], loss_recv.at[c], z, col)

    for row in range(nr):
        @pl.when(row != z)
        def _():
            mass_copy(row).start()

    loss = jnp.zeros((8, rows), F32)
    for j in reversed(range(m)):
        @pl.when(c * m + j < z)
        def _():
            with scope("wait_up"):
                for h in range(PIECES):
                    arrived(err_own.at[j, h * piece:(h + 1) * piece], own_recv.at[j, h])

        error = err_own[j]
        errors_out[:, j * span:(j + 1) * span] = error
        squared = error * error
        loss = loss + lax.dot_general(
            jnp.ones((8, span), F32), squared, (((1,), (1,)), ((), ())),
            precision=lax.Precision.HIGHEST, preferred_element_type=F32,
        )
    loss_all[c, :, :rows] = loss

    for col in range(nc):
        @pl.when(col != c)
        def _():
            loss_copy(col).start()

    for j in range(m):
        @pl.when(c * m + j < z)
        def _():
            delta_copy(j).wait_send()

        @pl.when(code_sent(j))
        def _():
            code_copy(j).wait_send()

    @pl.when((z == final) & is_last)
    def _():
        for row in range(final):
            for i in range(k - 1):
                tri_copy(row, i).wait_send()

    def drain(q, _):
        g = group(q)
        for j in range(m):
            @pl.when((c * m + j > z) & (c * m + j < final))
            def _():
                run_copy(q, j).wait_send()

        @pl.when(is_last & (z < final) & (g != z))
        def _():
            last_copy(q).wait_send()

        for col in range(nc):
            @pl.when(is_owner & ((col > c) | ((col == 0) & (c > 0) & (g >= z))))
            def _():
                core_copy(q, col).wait_send()

        @pl.when((is_owner & (g < z)) | (is_last & (z < final) & (g > z)))
        def _():
            own_copy(q).wait_send()

        return 0

    with scope("drain"):
        lax.fori_loop(0, steps, drain, 0)

    for col in range(nc):
        @pl.when(col != c)
        def _():
            with scope("wait_loss"):
                arrived(loss_all.at[col], loss_recv.at[col])
    loss_sum = loss_all[0, 0:1, :rows]
    for col in range(1, nc):
        loss_sum = loss_sum + loss_all[col, 0:1, :rows]
    loss_out[...] = loss_sum

    for row in range(nr):
        @pl.when(row != z)
        def _():
            with scope("wait_mass"):
                arrived(mass_all.at[row], mass_recv.at[row])
    mass_sum = mass_all[0]
    for row in range(1, nr):
        mass_sum = mass_sum + mass_all[row]
    mass_out[...] = mass_sum
    for j in range(m):
        @pl.when(c * m + j < final)
        def _():
            @pl.when((c * m + j != z) | (c != 0))
            def _():
                with scope("wait_mass_part"):
                    arrived(mass_own.at[j], part_recv.at[j])
            mass_out[j * k:(j + 1) * k, :] = mass_out[j * k:(j + 1) * k, :] + mass_own[j]

    for row in range(nr):
        @pl.when(row != z)
        def _():
            mass_copy(row).wait_send()

        @pl.when(part_remote(row))
        def _():
            part_copy(row).wait_send()
    for col in range(nc):
        @pl.when(col != c)
        def _():
            loss_copy(col).wait_send()


def store(errors, loss, mass, errors_out, loss_out, mass_out, sems):
    copies = [
        pltpu.make_async_copy(source, target, sems.at[number])
        for number, (source, target) in enumerate(((errors, errors_out), (loss, loss_out), (mass, mass_out)))
    ]
    for copy in copies:
        copy.start()
    for copy in copies:
        copy.wait()


def local(nr, nc, weights, codebook, assign, chol_upper, inv_blocks):
    rows, width = weights.shape[1:]
    span = chol_upper.shape[1]
    m = width // span
    steps, piece = nr * PIECES, rows // PIECES
    blocks, code_count = codebook.shape[1], codebook.shape[3]
    block = inv_blocks.shape[2]
    k = span // block
    edges = max(k - 1, 1)
    dma = pltpu.SemaphoreType.DMA
    vmem = pl.BlockSpec(memory_space=pltpu.VMEM)
    hbm = pl.BlockSpec(memory_space=pltpu.HBM)
    shapes = ((rows, width), (1, rows), (blocks, code_count))
    results = pl.pallas_call(
        functools.partial(kernel, nr, nc),
        out_shape=tuple(pltpu.VMEM(shape, F32) for shape in shapes),
        in_specs=[hbm] * 5,
        out_specs=(vmem, vmem, vmem),
        scratch_shapes=[
            pltpu.VMEM(weights.shape[1:], F32),
            pltpu.VMEM(codebook.shape[1:], F32),
            pltpu.VMEM(assign.shape[1:], jnp.int32),
            pltpu.VMEM(inv_blocks.shape[1:], F32),
            pltpu.VMEM((span, width), F32),
            pltpu.VMEM((span, width), BF16),
            pltpu.VMEM((span, width), BF16),
            pltpu.VMEM((span, span), F32),
            pltpu.VMEM((span, span), F32),
            pltpu.VMEM((span, span), BF16),
            pltpu.VMEM((span, span), BF16),
            pltpu.VMEM((span, span), BF16),
            pltpu.VMEM((span, span), BF16),
            pltpu.VMEM((m, rows, span), F32),
            pltpu.VMEM((blocks, rows, block), jnp.int32),
            pltpu.VMEM((nr, rows, span), F32),
            pltpu.VMEM((nr, k, rows, block), jnp.int32),
            pltpu.VMEM((steps, m, piece, span), F32),
            pltpu.VMEM((steps, m, piece, span), F32),
            pltpu.VMEM((nr, PIECES, piece, span), F32),
            pltpu.VMEM((steps, piece, span), F32),
            pltpu.VMEM((steps, piece, span), F32),
            pltpu.VMEM((m, rows, span), F32),
            pltpu.VMEM((k * 2 * (code_count // LOW), k * LOW), F32),
            pltpu.VMEM((nr, blocks, code_count), F32),
            pltpu.VMEM((m, k, code_count), F32),
            pltpu.VMEM((k, code_count), F32),
            pltpu.VMEM((nc, 8, max(rows, 128)), F32),
            dma((5,)),
            dma((m,)), dma((nr,)),
            dma((m,)), dma((nr,)),
            dma((nr, edges)), dma((edges,)),
            dma((steps, m)), dma((steps, m)),
            dma((steps,)), dma((nr, PIECES)),
            dma((steps, nc)), dma((steps,)),
            dma((steps,)), dma((m, PIECES)),
            dma((nr,)), dma((m,)),
            dma((nr,)), dma((nr,)),
            dma((nc,)), dma((nc,)),
        ],
        compiler_params=pltpu.CompilerParams(
            collective_id=0, has_side_effects=True, vmem_limit_bytes=40 * 1024 * 1024
        ),
    )(*(pltpu.with_memory_space_constraint(value[0], pltpu.HBM) for value in (
        weights, codebook, assign, inv_blocks, chol_upper,
    )))
    errors, loss, mass = pl.pallas_call(
        store,
        out_shape=tuple(jax.ShapeDtypeStruct(shape, F32) for shape in shapes),
        in_specs=[vmem] * 3,
        out_specs=[hbm] * 3,
        scratch_shapes=[dma((3,))],
        compiler_params=pltpu.CompilerParams(vmem_limit_bytes=1024 * 1024),
    )(*results)
    return errors[None], loss, mass[None]


def solution(mesh):
    return jax.shard_map(
        functools.partial(local, mesh.shape["row"], mesh.shape["col"]),
        mesh=mesh,
        in_specs=(
            P("ea", "row", "col"),
            P("ea", "col", None, None),
            P("ea", "row", "col"),
            P("ea", "row", "col"),
            P("ea", "col", None, None),
        ),
        out_specs=(P("ea", "row", "col"), P("ea", "row"), P("ea", "col", None)),
        check_vma=False,
    )
```

```python
import functools

import jax
import jax.numpy as jnp
from jax import lax
from jax.experimental import pallas as pl
from jax.experimental.pallas import tpu as pltpu
from jax.sharding import PartitionSpec as P

F32 = jnp.float32
BF16 = jnp.bfloat16
LOW = 16
PIECES = 2
scope = jax.named_scope


def halves(value):
    high = value.astype(BF16)
    return high, (value - high.astype(F32)).astype(BF16)


def dot(a, b):
    return jnp.dot(a, b, preferred_element_type=F32)


def dot3(a, b_high, b_low):
    rows = a.shape[0]
    high, low = halves(a)
    both = dot(jnp.concatenate([high, low], axis=0), b_high)
    return both[:rows] + both[rows:] + dot(high, b_low)


def dot_full(a, b):
    b_high, b_low = halves(b)
    return dot3(a, b_high, b_low)


def take(table, index):
    return jnp.take_along_axis(table, index, axis=1, mode="promise_in_bounds")


def kernel(
    nr, nc,
    weights_hbm, codebook_hbm, assign_hbm, inverse_hbm, factor,
    errors_out, loss_out, mass_out,
    weights, codebook, assign, inverse, u_raw, u_high, u_low, triangle, v_full, v_high, v_low, w_high, w_low,
    delta, codes, delta_in, codes_in, run_in, run_out, last_in, last_out,
    err_block, err_own, err_zero, tally, mass_all, mass_own, mass_sent, loss_all,
    u_sem, d_send, d_recv, code_send, code_recv, tri_send, tri_recv, run_send, run_recv, last_send, last_recv,
    core_send, core_recv, own_send, own_recv, zero_send, part_send, part_recv, mass_send, mass_recv,
    loss_send, loss_recv, ready,
):
    z = lax.axis_index("row")
    c = lax.axis_index("col")
    rows, width = weights.shape
    span = factor.shape[0]
    m = width // span
    block = inverse.shape[1]
    k = span // block
    code_count = codebook.shape[2]
    owner = z // m
    slot = z % m
    steps = nr * PIECES
    piece = rows // PIECES
    final = nr - 1
    pairs = span // 2
    window = max(pairs, block)
    is_owner = (c == owner) & (z < final)
    is_last = c == nc - 1

    def remote(src, dst, send, recv, row, col):
        return pltpu.make_async_remote_copy(
            src_ref=src, dst_ref=dst, send_sem=send, recv_sem=recv,
            device_id={"row": row, "col": col}, device_id_type=pl.DeviceIdType.MESH,
        )

    def arrived(ref, sem):
        pltpu.make_async_copy(ref, ref, sem).wait()

    loads = [
        pltpu.make_async_copy(source, target, u_sem.at[number])
        for number, (source, target) in enumerate((
            (assign_hbm, assign), (codebook_hbm, codebook), (weights_hbm, weights),
            (inverse_hbm, inverse), (factor, u_raw),
        ))
    ]
    for load in loads:
        load.start()

    barrier = pltpu.get_barrier_semaphore()
    for step in range(1, nr * nc):
        other = lax.rem(z * nc + c + step, nr * nc)

        @pl.when(z <= other // nc + 1)
        def _():
            pl.semaphore_signal(
                barrier, inc=1, device_id={"row": other // nc, "col": other % nc},
                device_id_type=pl.DeviceIdType.MESH,
            )

    def enter():
        with scope("entry"):
            pl.semaphore_wait(barrier, (jnp.minimum(z + 1, nr - 1) + 1) * nc - 1)

    def wait_ready():
        with scope("wait_ready"):
            pl.semaphore_wait(ready, (nr - 2 - z) * nc)

    def order(place):
        if nr < 3:
            return place
        return jnp.where(place == nr - 2, nr - 1, jnp.where(place == nr - 1, nr - 2, place))

    def group(q):
        return order(q // PIECES)

    def part_rows(q):
        return pl.ds(pl.multiple_of(q % PIECES * piece, piece), piece)

    def delta_copy(j):
        return remote(delta.at[j], delta_in.at[z], d_send.at[j], d_recv.at[z], c * m + j, c)

    def code_copy(j):
        low = j * pairs // window * window
        return remote(
            assign.at[:, low:low + window], codes_in.at[z], code_send.at[j], code_recv.at[z], c * m + j, 0
        )

    def code_sent(j):
        return (c * m + j <= z) & (c * m + j < final) & ((c > 0) | (c * m + j < z))

    def tri_copy(row, i):
        low = (m - 1) * span
        return remote(
            u_raw.at[i * block:(i + 1) * block, low + (i + 1) * block:low + span],
            triangle.at[i * block:(i + 1) * block, (i + 1) * block:span],
            tri_send.at[row, i], tri_recv.at[i], row, c,
        )

    def run_copy(q, j):
        return remote(run_out.at[q, j], run_in.at[q, j], run_send.at[q, j], run_recv.at[q, j], z + 1, c)

    def first(g):
        return jnp.where(g == 0, 1, 0)

    def solver(g):
        return jnp.maximum(g, 1)

    def last_copy(q):
        at = first(group(q)), z, q % PIECES
        return remote(last_out.at[q], last_in.at[at], last_send.at[q], last_recv.at[at], solver(group(q)), c)

    def zero_copy(h):
        return remote(
            err_zero.at[h], err_own.at[m - 1, h * piece:(h + 1) * piece],
            zero_send.at[h], own_recv.at[m - 1, h], 0, c,
        )

    def core_copy(q, col):
        return remote(err_block.at[q], err_block.at[q], core_send.at[q, col], core_recv.at[q], z, col)

    def own_copy(q):
        return remote(
            err_block.at[q], err_own.at[slot, part_rows(q)],
            own_send.at[q], own_recv.at[slot, q % PIECES], group(q), owner,
        )

    with scope("first_loads"):
        for load in loads[:3]:
            load.wait()

    lane = lax.broadcasted_iota(jnp.int32, (rows, block), 1)
    for b in range(width // block):
        low = b * (block // 2)
        tile = low // block * block
        code = take(assign[:, tile:tile + block], low - tile + lane // 2)
        codes[b] = code
        inner = code % block
        value = jnp.zeros((rows, block), F32)
        for part in range(code_count // block):
            picked = []
            for comp in range(2):
                table = codebook[b, comp:comp + 1, part * block:(part + 1) * block]
                picked.append(take(jnp.broadcast_to(table, (rows, block)), inner))
            both = jnp.where(lane % 2 == 0, picked[0], picked[1])
            value = jnp.where(code // block == part, both, value)
        j, at = b * block // span, b * block % span
        delta[j, :, at:at + block] = weights[:, b * block:(b + 1) * block] - value
        if at + block == span:
            if j == 0:
                @pl.when(z > 0)
                def _():
                    enter()

            @pl.when(c * m + j < z)
            def _():
                delta_copy(j).start()

    for row in range(nr - 2):
        for col in range(nc):
            @pl.when(row + 1 < z)
            def _():
                pl.semaphore_signal(
                    ready, inc=1, device_id={"row": row, "col": col}, device_id_type=pl.DeviceIdType.MESH,
                )

    with scope("factor_loads"):
        for load in loads[3:]:
            load.wait()

    @pl.when((z == final) & is_last)
    def _():
        for row in reversed(range(1, final)):
            for i in range(k - 1):
                tri_copy(row, i).start()

    def inverted(first, right):
        v_full[...] = jnp.zeros_like(v_full)

        def invert(lo, hi):
            if hi - lo == 1:
                v_full[lo * block:hi * block, lo * block:hi * block] = inverse[first + lo]
                return
            mid = (lo + hi) // 2
            invert(lo, mid)
            invert(mid, hi)
            top, middle, end = lo * block, mid * block, hi * block
            product = dot_full(v_full[top:middle, top:middle], right(top, middle, end))
            v_full[top:middle, middle:end] = -dot_full(product, v_full[middle:end, middle:end])

        invert(0, k)
        return halves(v_full[...])

    @pl.when(is_owner)
    def _():
        base = slot * span
        high, low = inverted(slot * k, lambda top, middle, end: u_raw[
            top:middle, pl.ds(pl.multiple_of(base + middle, block), end - middle)
        ])
        v_high[...] = high
        v_low[...] = low

    for j in range(m):
        @pl.when(c * m + j > z)
        def _():
            high, low = halves(u_raw[:, j * span:(j + 1) * span])
            u_high[:, j * span:(j + 1) * span] = high
            u_low[:, j * span:(j + 1) * span] = low

    def invert_last():
        @pl.when(z == final)
        def _():
            triangle[...] = u_raw[:, (m - 1) * span:]

        @pl.when(z < final)
        def _():
            with scope("wait_triangle"):
                for i in range(k - 1):
                    part = triangle.at[i * block:(i + 1) * block, (i + 1) * block:span]
                    arrived(part, tri_recv.at[i])

        high, low = inverted((m - 1) * k, lambda top, middle, end: triangle[top:middle, middle:end])
        w_high[...] = high
        w_low[...] = low

    @pl.when(z == 0)
    def _():
        enter()

    for j in range(m):
        @pl.when(code_sent(j))
        def _():
            code_copy(j).start()

        @pl.when((c == 0) & (z == j) & (z < final))
        def _():
            low = j * pairs // window * window
            codes_in[z] = assign[:, low:low + window]

    late_core = (z == 0) & (c > owner)
    relay_core = (z > 0) & (z < final) & (c > owner)
    early_up = (z > 0) & (owner < nc - 1)

    def stage(q, _):
        g = group(q)
        at = part_rows(q)

        @pl.when(is_last & (((z == final) & (q == 0)) | ((z == final - 1) & (q == PIECES))))
        def _():
            invert_last()

        @pl.when((z > 0) & (z < nr - 2) & (q == (z + 1) * PIECES))
        def _():
            wait_ready()

        @pl.when(is_owner)
        def _():
            @pl.when(z == 0)
            def _():
                run_in[q, slot] = jnp.zeros((piece, span), F32)

            @pl.when(z > 0)
            def _():
                with scope("wait_own_sum"):
                    arrived(run_in.at[q, slot], run_recv.at[q, slot])

            @pl.when(g > z)
            def _():
                @pl.when(q % PIECES == 0)
                def _():
                    with scope("wait_delta"):
                        arrived(delta_in.at[g], d_recv.at[g])

                run_in[q, slot] = run_in[q, slot] + delta_in[g, at]

            @pl.when(g == z)
            def _():
                run_in[q, slot] = run_in[q, slot] + delta[slot, at]

            error = dot3(run_in[q, slot], v_high[...], v_low[...])
            err_block[q] = error

            @pl.when(g == z)
            def _():
                err_own[slot, at] = error

            for col in range(nc):
                @pl.when((col > c) | ((col == 0) & (c > 0) & (g >= z)))
                def _():
                    core_copy(q, col).start()

            @pl.when((g < z) | ((g > z) & early_up))
            def _():
                own_copy(q).start()

        @pl.when((c > owner) & (z < final))
        def _():
            with scope("wait_core"):
                arrived(err_block.at[q], core_recv.at[q])

        late = late_core & (q >= 2 * PIECES)
        relay = relay_core & (q >= PIECES)
        @pl.when(is_last & (z < final))
        def _():
            j = m - 1
            change = dot3(
                err_block[q], u_high[:, j * span:(j + 1) * span], u_low[:, j * span:(j + 1) * span]
            )
            change = change - jnp.where((g == 0) & (z == 0), delta[j, at], 0.0)

            @pl.when(solver(g) == z)
            def _():
                last_in[first(g), z, q % PIECES] = change

            @pl.when(solver(g) != z)
            def _():
                last_out[q] = change

                @pl.when(jnp.logical_not(late))
                def _():
                    last_copy(q).start()

        for j in range(m):
            target = c * m + j

            @pl.when((target > z) & (target < final))
            def _():
                change = dot3(
                    err_block[q], u_high[:, j * span:(j + 1) * span], u_low[:, j * span:(j + 1) * span]
                )
                run_out[q, j] = jnp.where(g == z, delta[j, at], 0.0) - change

                @pl.when((z > 0) & jnp.logical_not(relay))
                def _():
                    with scope("wait_near_sum"):
                        arrived(run_in.at[q, j], run_recv.at[q, j])
                    run_out[q, j] = run_out[q, j] + run_in[q, j]

                @pl.when(jnp.logical_not(late | relay))
                def _():
                    run_copy(q, j).start()

        return 0

    lax.fori_loop(0, steps, stage, 0)

    @pl.when((z == 0) & (nr > 2))
    def _():
        wait_ready()

    for j in range(m):
        @pl.when(late_core & (c * m + j < final))
        def _():
            def release(q, _):
                run_copy(q, j).start()
                return 0

            lax.fori_loop(2 * PIECES, steps, release, 0)

        @pl.when(relay_core & (c * m + j < final))
        def _():
            def release(q, _):
                with scope("wait_far_sum"):
                    arrived(run_in.at[q, j], run_recv.at[q, j])
                run_out[q, j] = run_out[q, j] + run_in[q, j]
                run_copy(q, j).start()
                return 0

            lax.fori_loop(PIECES, steps, release, 0)

    @pl.when(late_core & is_last)
    def _():
        def release(i, _):
            last_copy(steps - 1 - i).start()
            return 0

        lax.fori_loop(0, steps - 2 * PIECES, release, 0)

    @pl.when(is_last & (z < final) & jnp.logical_not(early_up))
    def _():
        def upward(i, _):
            q = steps - 1 - i

            @pl.when(group(q) > z)
            def _():
                own_copy(q).start()

            return 0

        lax.fori_loop(0, steps, upward, 0)

    @pl.when(is_last & (z > 0) & (z < final - 1))
    def _():
        invert_last()

    def solved(which, h):
        with scope("wait_last"):
            for row in range(final):
                @pl.when(row != z)
                def _():
                    arrived(last_in.at[which, row, h], last_recv.at[which, row, h])
        total = -last_in[which, 0, h]
        for row in range(1, final):
            total = total - last_in[which, row, h]
        if which == 0:
            total = total + delta[m - 1, h * piece:(h + 1) * piece]
        return dot3(total, w_high[...], w_low[...])

    @pl.when(is_last & (z == 1))
    def _():
        for h in range(PIECES):
            err_zero[h] = solved(1, h)
            zero_copy(h).start()

    high_count = code_count // LOW
    fold = 2 * high_count
    chunk = 8

    def count(error_at, code_at):
        def gather(step, total):
            at = pl.ds(pl.multiple_of(step * chunk, chunk), chunk)
            iota_high = lax.broadcasted_iota(jnp.int32, (high_count, block), 0)
            iota_low = lax.broadcasted_iota(jnp.int32, (LOW, block), 0)
            left, right = [], []
            for b in range(k):
                code = code_at(b, at)
                value = error_at[at, b * block:(b + 1) * block]
                value = value * value
                coarse = value.astype(BF16).astype(F32)
                fine = value - coarse
                code_high, code_low = code // LOW, code % LOW
                top, bottom, marks = [], [], []
                for r in range(chunk):
                    hit = jnp.broadcast_to(code_high[r:r + 1], (high_count, block)) == iota_high
                    top.append(jnp.where(hit, jnp.broadcast_to(coarse[r:r + 1], (high_count, block)), 0.0).astype(BF16))
                    bottom.append(jnp.where(hit, jnp.broadcast_to(fine[r:r + 1], (high_count, block)), 0.0).astype(BF16))
                    low_hit = jnp.broadcast_to(code_low[r:r + 1], (LOW, block)) == iota_low
                    marks.append(jnp.where(low_hit, 1.0, 0.0).astype(BF16))
                left += [jnp.concatenate(top, axis=1), jnp.concatenate(bottom, axis=1)]
                right.append(jnp.concatenate(marks, axis=1))
            return total + lax.dot_general(
                jnp.concatenate(left, axis=0), jnp.concatenate(right, axis=0),
                (((1,), (1,)), ((), ())), preferred_element_type=F32,
            )

        total = lax.fori_loop(0, piece // chunk, gather, jnp.zeros(tally.shape, F32), unroll=4)
        tally[...] = tally[...] + total

    def spread(store):
        total = tally[...]
        row_id = lax.broadcasted_iota(jnp.int32, total.shape, 0)
        col_id = lax.broadcasted_iota(jnp.int32, total.shape, 1)
        total = jnp.where(row_id // fold == col_id // LOW, total, 0.0)
        wide_row = lax.broadcasted_iota(jnp.int32, (k * LOW, code_count), 0)
        wide_col = lax.broadcasted_iota(jnp.int32, (k * LOW, code_count), 1)
        wide = jnp.where(wide_row % LOW == wide_col % LOW, 1.0, 0.0)
        wide = jnp.dot(total, wide, precision=lax.Precision.HIGHEST, preferred_element_type=F32)
        out_row = lax.broadcasted_iota(jnp.int32, wide.shape, 0)
        out_col = lax.broadcasted_iota(jnp.int32, wide.shape, 1)
        wide = jnp.where(out_row % high_count == out_col // LOW, wide, 0.0)
        for b in range(k):
            store(b, jnp.sum(wide[b * fold:(b + 1) * fold], axis=0, keepdims=True))
        tally[...] = jnp.zeros_like(tally)

    tally[...] = jnp.zeros_like(tally)
    mass_all[z] = jnp.zeros(mass_all.shape[1:], F32)
    counts = (c == 0) & (z < final)

    def part_copy(row):
        return remote(mass_sent, mass_own.at[slot], part_send.at[row], part_recv.at[slot], row, owner)

    def part_remote(row):
        return counts & ((row != z) | (owner != 0))

    @pl.when(counts)
    def _():
        def own_part(q, _):
            g = group(q)

            @pl.when(g >= z)
            def _():
                with scope("wait_part"):
                    @pl.when(owner != 0)
                    def _():
                        arrived(err_block.at[q], core_recv.at[q])

                    @pl.when(((g != z) | (owner != 0)) & (q % PIECES == 0))
                    def _():
                        arrived(codes_in.at[g], code_recv.at[g])

                shift = 0 if window == pairs else lax.rem(slot * pairs, window)

                def code_at(b, at):
                    low = b * (block // 2)
                    tile = low // block * block
                    source = codes_in[g, pl.ds(q % PIECES * piece + at.start, chunk), tile:tile + block]
                    return take(source, shift + low - tile + lane[:chunk] // 2)

                count(err_block.at[q], code_at)

            return 0

        lax.fori_loop(0, steps, own_part, 0)

        def store(b, value):
            mass_sent[b:b + 1, :] = value

        spread(store)

        @pl.when(owner == 0)
        def _():
            mass_own[slot] = mass_sent[...]

    for row in range(nr):
        @pl.when(part_remote(row))
        def _():
            part_copy(row).start()

    def own_spread(j):
        def store(b, value):
            mass_all[z, j * k + b:j * k + b + 1, :] = value

        spread(store)

    for j in range(m):
        @pl.when((c * m + j > z) & ((c * m + j < final) | (z == 0)))
        def _():
            for h in range(PIECES):
                with scope("wait_down"):
                    arrived(err_own.at[j, h * piece:(h + 1) * piece], own_recv.at[j, h])
                count(
                    err_own.at[j, h * piece:(h + 1) * piece],
                    lambda b, at: codes[j * k + b, pl.ds(h * piece + at.start, chunk), :],
                )
            own_spread(j)

    @pl.when(is_last & (z > 0))
    def _():
        j = m - 1
        for h in range(PIECES):
            err_own[j, h * piece:(h + 1) * piece] = solved(0, h)
            count(
                err_own.at[j, h * piece:(h + 1) * piece],
                lambda b, at: codes[j * k + b, pl.ds(h * piece + at.start, chunk), :],
            )
        own_spread(j)

    def mass_copy(row):
        return remote(mass_all.at[z], mass_all.at[z], mass_send.at[row], mass_recv.at[z], row, c)

    def loss_copy(col):
        return remote(loss_all.at[c], loss_all.at[c], loss_send.at[col], loss_recv.at[c], z, col)

    for row in range(nr):
        @pl.when(row != z)
        def _():
            mass_copy(row).start()

    loss = jnp.zeros((8, rows), F32)
    for j in reversed(range(m)):
        @pl.when(c * m + j < z)
        def _():
            with scope("wait_up"):
                for h in range(PIECES):
                    arrived(err_own.at[j, h * piece:(h + 1) * piece], own_recv.at[j, h])

        error = err_own[j]
        errors_out[:, j * span:(j + 1) * span] = error
        squared = error * error
        loss = loss + lax.dot_general(
            jnp.ones((8, span), F32), squared, (((1,), (1,)), ((), ())),
            precision=lax.Precision.HIGHEST, preferred_element_type=F32,
        )
    loss_all[c, :, :rows] = loss

    for col in range(nc):
        @pl.when(col != c)
        def _():
            loss_copy(col).start()

    for j in range(m):
        @pl.when(c * m + j < z)
        def _():
            delta_copy(j).wait_send()

        @pl.when(code_sent(j))
        def _():
            code_copy(j).wait_send()

    @pl.when((z == final) & is_last)
    def _():
        for row in range(1, final):
            for i in range(k - 1):
                tri_copy(row, i).wait_send()

    def drain(q, _):
        g = group(q)
        for j in range(m):
            @pl.when((c * m + j > z) & (c * m + j < final))
            def _():
                run_copy(q, j).wait_send()

        @pl.when(is_last & (z < final) & (solver(g) != z))
        def _():
            last_copy(q).wait_send()

        for col in range(nc):
            @pl.when(is_owner & ((col > c) | ((col == 0) & (c > 0) & (g >= z))))
            def _():
                core_copy(q, col).wait_send()

        down = is_owner & ((g < z) | ((g > z) & early_up))

        @pl.when(down | (is_last & (z < final) & (g > z) & jnp.logical_not(early_up)))
        def _():
            own_copy(q).wait_send()

        return 0

    with scope("drain"):
        lax.fori_loop(0, steps, drain, 0)

    @pl.when(is_last & (z == 1))
    def _():
        for h in range(PIECES):
            zero_copy(h).wait_send()

    for col in range(nc):
        @pl.when(col != c)
        def _():
            with scope("wait_loss"):
                arrived(loss_all.at[col], loss_recv.at[col])
    loss_sum = loss_all[0, 0:1, :rows]
    for col in range(1, nc):
        loss_sum = loss_sum + loss_all[col, 0:1, :rows]
    loss_out[...] = loss_sum

    for row in range(nr):
        @pl.when(row != z)
        def _():
            with scope("wait_mass"):
                arrived(mass_all.at[row], mass_recv.at[row])
    mass_sum = mass_all[0]
    for row in range(1, nr):
        mass_sum = mass_sum + mass_all[row]
    mass_out[...] = mass_sum
    for j in range(m):
        @pl.when(c * m + j < final)
        def _():
            @pl.when((c * m + j != z) | (c != 0))
            def _():
                with scope("wait_mass_part"):
                    arrived(mass_own.at[j], part_recv.at[j])
            mass_out[j * k:(j + 1) * k, :] = mass_out[j * k:(j + 1) * k, :] + mass_own[j]

    for row in range(nr):
        @pl.when(row != z)
        def _():
            mass_copy(row).wait_send()

        @pl.when(part_remote(row))
        def _():
            part_copy(row).wait_send()
    for col in range(nc):
        @pl.when(col != c)
        def _():
            loss_copy(col).wait_send()


def store(errors, loss, mass, errors_out, loss_out, mass_out, sems):
    copies = [
        pltpu.make_async_copy(source, target, sems.at[number])
        for number, (source, target) in enumerate(((errors, errors_out), (loss, loss_out), (mass, mass_out)))
    ]
    for copy in copies:
        copy.start()
    for copy in copies:
        copy.wait()


def local(nr, nc, weights, codebook, assign, chol_upper, inv_blocks):
    rows, width = weights.shape[1:]
    span = chol_upper.shape[1]
    m = width // span
    steps, piece = nr * PIECES, rows // PIECES
    blocks, code_count = codebook.shape[1], codebook.shape[3]
    block = inv_blocks.shape[2]
    k = span // block
    edges = max(k - 1, 1)
    dma = pltpu.SemaphoreType.DMA
    vmem = pl.BlockSpec(memory_space=pltpu.VMEM)
    hbm = pl.BlockSpec(memory_space=pltpu.HBM)
    shapes = ((rows, width), (1, rows), (blocks, code_count))
    results = pl.pallas_call(
        functools.partial(kernel, nr, nc),
        out_shape=tuple(pltpu.VMEM(shape, F32) for shape in shapes),
        in_specs=[hbm] * 5,
        out_specs=(vmem, vmem, vmem),
        scratch_shapes=[
            pltpu.VMEM(weights.shape[1:], F32),
            pltpu.VMEM(codebook.shape[1:], F32),
            pltpu.VMEM(assign.shape[1:], jnp.int32),
            pltpu.VMEM(inv_blocks.shape[1:], F32),
            pltpu.VMEM((span, width), F32),
            pltpu.VMEM((span, width), BF16),
            pltpu.VMEM((span, width), BF16),
            pltpu.VMEM((span, span), F32),
            pltpu.VMEM((span, span), F32),
            pltpu.VMEM((span, span), BF16),
            pltpu.VMEM((span, span), BF16),
            pltpu.VMEM((span, span), BF16),
            pltpu.VMEM((span, span), BF16),
            pltpu.VMEM((m, rows, span), F32),
            pltpu.VMEM((blocks, rows, block), jnp.int32),
            pltpu.VMEM((nr, rows, span), F32),
            pltpu.VMEM((nr, rows, max(span // 2, block)), jnp.int32),
            pltpu.VMEM((steps, m, piece, span), F32),
            pltpu.VMEM((steps, m, piece, span), F32),
            pltpu.VMEM((2, nr, PIECES, piece, span), F32),
            pltpu.VMEM((steps, piece, span), F32),
            pltpu.VMEM((steps, piece, span), F32),
            pltpu.VMEM((m, rows, span), F32),
            pltpu.VMEM((PIECES, piece, span), F32),
            pltpu.VMEM((k * 2 * (code_count // LOW), k * LOW), F32),
            pltpu.VMEM((nr, blocks, code_count), F32),
            pltpu.VMEM((m, k, code_count), F32),
            pltpu.VMEM((k, code_count), F32),
            pltpu.VMEM((nc, 8, max(rows, 128)), F32),
            dma((5,)),
            dma((m,)), dma((nr,)),
            dma((m,)), dma((nr,)),
            dma((nr, edges)), dma((edges,)),
            dma((steps, m)), dma((steps, m)),
            dma((steps,)), dma((2, nr, PIECES)),
            dma((steps, nc)), dma((steps,)),
            dma((steps,)), dma((m, PIECES)), dma((PIECES,)),
            dma((nr,)), dma((m,)),
            dma((nr,)), dma((nr,)),
            dma((nc,)), dma((nc,)), pltpu.SemaphoreType.REGULAR,
        ],
        compiler_params=pltpu.CompilerParams(
            collective_id=0, has_side_effects=True, vmem_limit_bytes=40 * 1024 * 1024
        ),
    )(*(pltpu.with_memory_space_constraint(value[0], pltpu.HBM) for value in (
        weights, codebook, assign, inv_blocks, chol_upper,
    )))
    errors, loss, mass = pl.pallas_call(
        store,
        out_shape=tuple(jax.ShapeDtypeStruct(shape, F32) for shape in shapes),
        in_specs=[vmem] * 3,
        out_specs=[hbm] * 3,
        scratch_shapes=[dma((3,))],
        compiler_params=pltpu.CompilerParams(vmem_limit_bytes=1024 * 1024),
    )(*results)
    return errors[None], loss, mass[None]


def solution(mesh):
    return jax.shard_map(
        functools.partial(local, mesh.shape["row"], mesh.shape["col"]),
        mesh=mesh,
        in_specs=(
            P("ea", "row", "col"),
            P("ea", "col", None, None),
            P("ea", "row", "col"),
            P("ea", "row", "col"),
            P("ea", "col", None, None),
        ),
        out_specs=(P("ea", "row", "col"), P("ea", "row"), P("ea", "col", None)),
        check_vma=False,
    )
```

```python
import functools

import jax
import jax.numpy as jnp
from jax import lax
from jax.experimental import pallas as pl
from jax.experimental.pallas import tpu as pltpu
from jax.sharding import PartitionSpec as P

F32 = jnp.float32
BF16 = jnp.bfloat16
LOW = 16
PIECES = 2
scope = jax.named_scope


def halves(value):
    high = value.astype(BF16)
    return high, (value - high.astype(F32)).astype(BF16)


def dot(a, b):
    return jnp.dot(a, b, preferred_element_type=F32)


def dot3(a, b_high, b_low):
    rows = a.shape[0]
    high, low = halves(a)
    both = dot(jnp.concatenate([high, low], axis=0), b_high)
    return both[:rows] + both[rows:] + dot(high, b_low)


def dot_full(a, b):
    b_high, b_low = halves(b)
    return dot3(a, b_high, b_low)


def take(table, index):
    return jnp.take_along_axis(table, index, axis=1, mode="promise_in_bounds")


def kernel(
    nr, nc,
    weights_hbm, codebook_hbm, assign_hbm, inverse_hbm, factor,
    errors_out, loss_out, mass_out,
    weights, codebook, assign, inverse, u_raw, u_high, u_low, triangle, v_full, v_high, v_low, w_high, w_low,
    delta, codes, delta_in, codes_in, run_in, run_out, last_in, last_out, zero_in,
    err_block, err_own, err_zero, tally, mass_all, mass_own, mass_sent, loss_all,
    u_sem, d_send, d_recv, code_send, code_recv, tri_send, tri_recv, run_send, run_recv, last_send, last_recv, zero_recv,
    core_send, core_recv, own_send, own_recv, zero_send, part_send, part_recv, mass_send, mass_recv,
    loss_send, loss_recv, ready,
):
    z = lax.axis_index("row")
    c = lax.axis_index("col")
    rows, width = weights.shape
    span = factor.shape[0]
    m = width // span
    block = inverse.shape[1]
    k = span // block
    code_count = codebook.shape[2]
    owner = z // m
    slot = z % m
    steps = nr * PIECES
    piece = rows // PIECES
    final = nr - 1
    pairs = span // 2
    window = max(pairs, block)
    is_owner = (c == owner) & (z < final)
    is_last = c == nc - 1

    def remote(src, dst, send, recv, row, col):
        return pltpu.make_async_remote_copy(
            src_ref=src, dst_ref=dst, send_sem=send, recv_sem=recv,
            device_id={"row": row, "col": col}, device_id_type=pl.DeviceIdType.MESH,
        )

    def arrived(ref, sem):
        pltpu.make_async_copy(ref, ref, sem).wait()

    loads = [
        pltpu.make_async_copy(source, target, u_sem.at[number])
        for number, (source, target) in enumerate((
            (assign_hbm, assign), (codebook_hbm, codebook), (weights_hbm, weights),
            (inverse_hbm, inverse), (factor, u_raw),
        ))
    ]
    for load in loads:
        load.start()

    barrier = pltpu.get_barrier_semaphore()
    for step in range(1, nr * nc):
        other = lax.rem(z * nc + c + step, nr * nc)

        @pl.when(z <= other // nc + 1)
        def _():
            pl.semaphore_signal(
                barrier, inc=1, device_id={"row": other // nc, "col": other % nc},
                device_id_type=pl.DeviceIdType.MESH,
            )

    def enter():
        with scope("entry"):
            pl.semaphore_wait(barrier, (jnp.minimum(z + 1, nr - 1) + 1) * nc - 1)

    def wait_ready():
        with scope("wait_ready"):
            pl.semaphore_wait(ready, (nr - 2 - z) * nc)

    def order(place):
        if nr < 3:
            return place
        return jnp.where(place == nr - 2, nr - 1, jnp.where(place == nr - 1, nr - 2, place))

    def group(q):
        return order(q // PIECES)

    def farthest(i):
        return order(nr - 1 - i // PIECES) * PIECES + i % PIECES

    def nearest(i):
        return order(i // PIECES) * PIECES + i % PIECES

    def part_rows(q):
        return pl.ds(pl.multiple_of(q % PIECES * piece, piece), piece)

    def delta_copy(j, h):
        at = slice(h * piece, (h + 1) * piece)
        return remote(delta.at[j, at], delta_in.at[z, at], d_send.at[j, h], d_recv.at[z, h], c * m + j, c)

    def send_delta(j, when):
        @pl.when((c * m + j < z) & when)
        def _():
            for h in range(PIECES):
                delta_copy(j, h).start()

    def urgent(j):
        return (c * m + j == 0) & (z != nr - 2)

    def code_copy(j):
        low = j * pairs // window * window
        return remote(
            assign.at[:, low:low + window], codes_in.at[z], code_send.at[j], code_recv.at[z], c * m + j, 0
        )

    def code_sent(j):
        return (c * m + j <= z) & (c * m + j < final) & ((c > 0) | (c * m + j < z))

    def tri_copy(row, i):
        low = (m - 1) * span
        return remote(
            u_raw.at[i * block:(i + 1) * block, low + (i + 1) * block:low + span],
            triangle.at[i * block:(i + 1) * block, (i + 1) * block:span],
            tri_send.at[row, i], tri_recv.at[i], row, c,
        )

    def run_copy(q, j):
        return remote(run_out.at[q, j], run_in.at[q, j], run_send.at[q, j], run_recv.at[q, j], z + 1, c)

    def first(g):
        return jnp.where(g == 0, 1, 0)

    def solver(g):
        return jnp.maximum(g, 1)

    def last_copy(q):
        at = first(group(q)), z, q % PIECES
        return remote(last_out.at[q], last_in.at[at], last_send.at[q], last_recv.at[at], solver(group(q)), c)

    def zero_sum(q):
        return remote(last_out.at[q], zero_in.at[q], last_send.at[q], zero_recv.at[q], 1, c)

    def zero_copy(h):
        return remote(
            err_zero.at[h], err_own.at[m - 1, h * piece:(h + 1) * piece],
            zero_send.at[h], own_recv.at[m - 1, h], 0, c,
        )

    def core_copy(q, col):
        return remote(err_block.at[q], err_block.at[q], core_send.at[q, col], core_recv.at[q], z, col)

    def own_copy(q):
        return remote(
            err_block.at[q], err_own.at[slot, part_rows(q)],
            own_send.at[q], own_recv.at[slot, q % PIECES], group(q), owner,
        )

    with scope("first_loads"):
        for load in loads[:3]:
            load.wait()

    lane = lax.broadcasted_iota(jnp.int32, (rows, block), 1)
    for b in range(width // block):
        low = b * (block // 2)
        tile = low // block * block
        code = take(assign[:, tile:tile + block], low - tile + lane // 2)
        codes[b] = code
        inner = code % block
        value = jnp.zeros((rows, block), F32)
        for part in range(code_count // block):
            picked = []
            for comp in range(2):
                table = codebook[b, comp:comp + 1, part * block:(part + 1) * block]
                picked.append(take(jnp.broadcast_to(table, (rows, block)), inner))
            both = jnp.where(lane % 2 == 0, picked[0], picked[1])
            value = jnp.where(code // block == part, both, value)
        j, at = b * block // span, b * block % span
        delta[j, :, at:at + block] = weights[:, b * block:(b + 1) * block] - value
        if at + block == span:
            if j == 0:
                @pl.when(z > 0)
                def _():
                    enter()

            send_delta(j, urgent(j))

    for row in range(nr - 2):
        for col in range(nc):
            @pl.when(row + 1 < z)
            def _():
                pl.semaphore_signal(
                    ready, inc=1, device_id={"row": row, "col": col}, device_id_type=pl.DeviceIdType.MESH,
                )

    with scope("factor_loads"):
        for load in loads[3:]:
            load.wait()

    @pl.when((z == final) & is_last)
    def _():
        for row in reversed(range(1, final)):
            for i in range(k - 1):
                tri_copy(row, i).start()

    def inverted(first, right):
        v_full[...] = jnp.zeros_like(v_full)

        def invert(lo, hi):
            if hi - lo == 1:
                v_full[lo * block:hi * block, lo * block:hi * block] = inverse[first + lo]
                return
            mid = (lo + hi) // 2
            invert(lo, mid)
            invert(mid, hi)
            top, middle, end = lo * block, mid * block, hi * block
            product = dot_full(v_full[top:middle, top:middle], right(top, middle, end))
            v_full[top:middle, middle:end] = -dot_full(product, v_full[middle:end, middle:end])

        invert(0, k)
        return halves(v_full[...])

    @pl.when(is_owner)
    def _():
        base = slot * span
        high, low = inverted(slot * k, lambda top, middle, end: u_raw[
            top:middle, pl.ds(pl.multiple_of(base + middle, block), end - middle)
        ])
        v_high[...] = high
        v_low[...] = low

    for j in range(m):
        @pl.when(c * m + j > z)
        def _():
            high, low = halves(u_raw[:, j * span:(j + 1) * span])
            u_high[:, j * span:(j + 1) * span] = high
            u_low[:, j * span:(j + 1) * span] = low

    def invert_last():
        @pl.when(z == final)
        def _():
            triangle[...] = u_raw[:, (m - 1) * span:]

        @pl.when(z < final)
        def _():
            with scope("wait_triangle"):
                for i in range(k - 1):
                    part = triangle.at[i * block:(i + 1) * block, (i + 1) * block:span]
                    arrived(part, tri_recv.at[i])

        high, low = inverted((m - 1) * k, lambda top, middle, end: triangle[top:middle, middle:end])
        w_high[...] = high
        w_low[...] = low

    @pl.when(z == 0)
    def _():
        enter()

    for j in range(m):
        send_delta(j, jnp.logical_not(urgent(j)))

    for j in range(m):
        @pl.when(code_sent(j))
        def _():
            code_copy(j).start()

        @pl.when((c == 0) & (z == j) & (z < final))
        def _():
            low = j * pairs // window * window
            codes_in[z] = assign[:, low:low + window]

    late_core = (z == 0) & (c > owner)
    relay_core = (z > 0) & (z < final) & (c > owner)
    early_up = z < 0

    def forward(q, j):
        with scope("wait_far_sum"):
            arrived(run_in.at[q, j], run_recv.at[q, j])
        run_out[q, j] = run_out[q, j] + run_in[q, j]
        run_copy(q, j).start()

    def stage(q, _):
        g = group(q)
        at = part_rows(q)

        @pl.when(is_last & (((z == final) & (q == 0)) | ((z == final - 1) & (q == PIECES))))
        def _():
            invert_last()

        @pl.when((z > 0) & (z < nr - 2) & (q == (z + 1) * PIECES))
        def _():
            wait_ready()

        @pl.when(is_owner)
        def _():
            @pl.when(z == 0)
            def _():
                run_in[q, slot] = jnp.zeros((piece, span), F32)

            @pl.when(z > 0)
            def _():
                with scope("wait_own_sum"):
                    arrived(run_in.at[q, slot], run_recv.at[q, slot])

            @pl.when(g > z)
            def _():
                with scope("wait_delta"):
                    arrived(delta_in.at[g, at], d_recv.at[g, q % PIECES])

                run_in[q, slot] = run_in[q, slot] + delta_in[g, at]

            @pl.when(g == z)
            def _():
                run_in[q, slot] = run_in[q, slot] + delta[slot, at]

            error = dot3(run_in[q, slot], v_high[...], v_low[...])
            err_block[q] = error

            @pl.when(g == z)
            def _():
                err_own[slot, at] = error

            for col in range(nc):
                @pl.when((col > c) | ((col == 0) & (c > 0) & (g >= z)))
                def _():
                    core_copy(q, col).start()

            @pl.when((g < z) | ((g > z) & early_up))
            def _():
                own_copy(q).start()

        @pl.when((c > owner) & (z < final))
        def _():
            with scope("wait_core"):
                arrived(err_block.at[q], core_recv.at[q])

        late = late_core & (q >= 2 * PIECES)
        relay = relay_core & (q >= PIECES)
        @pl.when(is_last & (z < final))
        def _():
            j = m - 1
            change = dot3(
                err_block[q], u_high[:, j * span:(j + 1) * span], u_low[:, j * span:(j + 1) * span]
            )
            change = change - jnp.where((g == 0) & (z == 0), delta[j, at], 0.0)

            @pl.when((z <= 1) | (solver(g) != z))
            def _():
                last_out[q] = change

            @pl.when((z > 1) & (solver(g) == z))
            def _():
                last_in[first(g), z, q % PIECES] = change

            @pl.when((z == 0) & (q < PIECES))
            def _():
                zero_sum(q).start()

            @pl.when((z > 1) & (solver(g) != z))
            def _():
                last_copy(q).start()

        for j in range(m):
            target = c * m + j

            @pl.when((target > z) & (target < final))
            def _():
                change = dot3(
                    err_block[q], u_high[:, j * span:(j + 1) * span], u_low[:, j * span:(j + 1) * span]
                )
                run_out[q, j] = jnp.where(g == z, delta[j, at], 0.0) - change

                @pl.when((z > 0) & jnp.logical_not(relay))
                def _():
                    with scope("wait_near_sum"):
                        arrived(run_in.at[q, j], run_recv.at[q, j])
                    run_out[q, j] = run_out[q, j] + run_in[q, j]

                @pl.when(jnp.logical_not(late | relay))
                def _():
                    run_copy(q, j).start()

                @pl.when(relay & (q >= 2 * PIECES))
                def _():
                    forward(q - PIECES, j)

        return 0

    lax.fori_loop(0, steps, stage, 0)

    @pl.when((z == 0) & (nr > 2))
    def _():
        wait_ready()

    for j in range(m):
        @pl.when(late_core & (c * m + j < final))
        def _():
            def release(q, _):
                run_copy(q, j).start()
                return 0

            lax.fori_loop(2 * PIECES, steps, release, 0)

        @pl.when(relay_core & (c * m + j < final))
        def _():
            def release(q, _):
                forward(q, j)
                return 0

            lax.fori_loop(steps - PIECES, steps, release, 0)

    @pl.when(late_core & is_last)
    def _():
        def release(i, _):
            zero_sum(farthest(i)).start()
            return 0

        lax.fori_loop(0, steps - PIECES, release, 0)

    def joined(q):
        with scope("wait_zero"):
            arrived(zero_in.at[q], zero_recv.at[q])
        return last_out[q] + zero_in[q]

    @pl.when(is_last & (z == 1) & (z < final))
    def _():
        def relayed(i, _):
            q = farthest(i)
            last_out[q] = joined(q)
            last_copy(q).start()
            return 0

        lax.fori_loop(0, steps - 2 * PIECES, relayed, 0)

    @pl.when(is_last & (z > 0) & (z < final - 1))
    def _():
        invert_last()

    def solved(which, h):
        with scope("wait_last"):
            for row in range(1, final):
                @pl.when(row != z)
                def _():
                    arrived(last_in.at[which, row, h], last_recv.at[which, row, h])
        total = -last_in[which, 1, h]
        for row in range(2, final):
            total = total - last_in[which, row, h]
        if which == 0:
            total = total + delta[m - 1, h * piece:(h + 1) * piece]
        return dot3(total, w_high[...], w_low[...])

    @pl.when(is_last & (z == 1))
    def _():
        for h in range(PIECES):
            last_in[1, 1, h] = joined(h)
            err_zero[h] = solved(1, h)
            zero_copy(h).start()
        for h in range(PIECES):
            last_in[0, 1, h] = joined(PIECES + h)

    @pl.when(is_last & (z < final) & jnp.logical_not(early_up))
    def _():
        def upward(i, _):
            q = nearest(i)

            @pl.when(group(q) > z)
            def _():
                own_copy(q).start()

            return 0

        lax.fori_loop(0, steps, upward, 0)

    high_count = code_count // LOW
    fold = 2 * high_count
    chunk = 8

    def count(error_at, code_at):
        def gather(step, total):
            at = pl.ds(pl.multiple_of(step * chunk, chunk), chunk)
            iota_high = lax.broadcasted_iota(jnp.int32, (high_count, block), 0)
            iota_low = lax.broadcasted_iota(jnp.int32, (LOW, block), 0)
            left, right = [], []
            for b in range(k):
                code = code_at(b, at)
                value = error_at[at, b * block:(b + 1) * block]
                value = value * value
                coarse = value.astype(BF16).astype(F32)
                fine = value - coarse
                code_high, code_low = code // LOW, code % LOW
                top, bottom, marks = [], [], []
                for r in range(chunk):
                    hit = jnp.broadcast_to(code_high[r:r + 1], (high_count, block)) == iota_high
                    top.append(jnp.where(hit, jnp.broadcast_to(coarse[r:r + 1], (high_count, block)), 0.0).astype(BF16))
                    bottom.append(jnp.where(hit, jnp.broadcast_to(fine[r:r + 1], (high_count, block)), 0.0).astype(BF16))
                    low_hit = jnp.broadcast_to(code_low[r:r + 1], (LOW, block)) == iota_low
                    marks.append(jnp.where(low_hit, 1.0, 0.0).astype(BF16))
                left += [jnp.concatenate(top, axis=1), jnp.concatenate(bottom, axis=1)]
                right.append(jnp.concatenate(marks, axis=1))
            return total + lax.dot_general(
                jnp.concatenate(left, axis=0), jnp.concatenate(right, axis=0),
                (((1,), (1,)), ((), ())), preferred_element_type=F32,
            )

        total = lax.fori_loop(0, piece // chunk, gather, jnp.zeros((k * fold, k * LOW), F32), unroll=4)
        tally[:, :k * LOW] = tally[:, :k * LOW] + total

    def spread(store):
        spot = lax.broadcasted_iota(jnp.int32, (high_count, block), 1)
        level = lax.broadcasted_iota(jnp.int32, (high_count, block), 0)
        for b in range(k):
            total = tally[b * fold:b * fold + high_count] + tally[b * fold + high_count:(b + 1) * fold]
            total = take(total, b * LOW + spot % LOW)
            for part in range(code_count // block):
                mine = level == part * (block // LOW) + spot // LOW
                store(b, part, jnp.sum(jnp.where(mine, total, 0.0), axis=0, keepdims=True))
        tally[...] = jnp.zeros_like(tally)

    tally[...] = jnp.zeros_like(tally)
    mass_all[z] = jnp.zeros(mass_all.shape[1:], F32)
    counts = (c == 0) & (z < final)

    def part_copy(row):
        return remote(mass_sent, mass_own.at[slot], part_send.at[row], part_recv.at[slot], row, owner)

    def part_remote(row):
        return counts & ((row != z) | (owner != 0))

    @pl.when(counts)
    def _():
        def own_part(q, _):
            g = group(q)

            @pl.when(g >= z)
            def _():
                with scope("wait_part"):
                    @pl.when(owner != 0)
                    def _():
                        arrived(err_block.at[q], core_recv.at[q])

                    @pl.when(((g != z) | (owner != 0)) & (q % PIECES == 0))
                    def _():
                        arrived(codes_in.at[g], code_recv.at[g])

                shift = 0 if window == pairs else lax.rem(slot * pairs, window)

                def code_at(b, at):
                    low = b * (block // 2)
                    tile = low // block * block
                    source = codes_in[g, pl.ds(q % PIECES * piece + at.start, chunk), tile:tile + block]
                    return take(source, shift + low - tile + lane[:chunk] // 2)

                count(err_block.at[q], code_at)

            return 0

        lax.fori_loop(0, steps, own_part, 0)

        def store(b, part, value):
            mass_sent[b:b + 1, part * block:(part + 1) * block] = value

        spread(store)

        @pl.when(owner == 0)
        def _():
            mass_own[slot] = mass_sent[...]

    for row in range(nr):
        @pl.when(part_remote(row))
        def _():
            part_copy(row).start()

    def own_spread(j):
        def store(b, part, value):
            mass_all[z, j * k + b:j * k + b + 1, part * block:(part + 1) * block] = value

        spread(store)

    for j in range(m):
        @pl.when((c * m + j > z) & ((c * m + j < final) | (z == 0)))
        def _():
            for h in range(PIECES):
                with scope("wait_down"):
                    arrived(err_own.at[j, h * piece:(h + 1) * piece], own_recv.at[j, h])
                count(
                    err_own.at[j, h * piece:(h + 1) * piece],
                    lambda b, at: codes[j * k + b, pl.ds(h * piece + at.start, chunk), :],
                )
            own_spread(j)

    @pl.when(is_last & (z > 0))
    def _():
        j = m - 1
        for h in range(PIECES):
            err_own[j, h * piece:(h + 1) * piece] = solved(0, h)
            count(
                err_own.at[j, h * piece:(h + 1) * piece],
                lambda b, at: codes[j * k + b, pl.ds(h * piece + at.start, chunk), :],
            )
        own_spread(j)

    def mass_copy(row):
        return remote(mass_all.at[z], mass_all.at[z], mass_send.at[row], mass_recv.at[z], row, c)

    def loss_copy(col):
        return remote(loss_all.at[c], loss_all.at[c], loss_send.at[col], loss_recv.at[c], z, col)

    for row in range(nr):
        @pl.when(row != z)
        def _():
            mass_copy(row).start()

    loss = jnp.zeros((8, rows), F32)
    for j in reversed(range(m)):
        @pl.when(c * m + j < z)
        def _():
            with scope("wait_up"):
                for h in range(PIECES):
                    arrived(err_own.at[j, h * piece:(h + 1) * piece], own_recv.at[j, h])

        error = err_own[j]
        errors_out[:, j * span:(j + 1) * span] = error
        squared = error * error
        loss = loss + lax.dot_general(
            jnp.ones((8, span), F32), squared, (((1,), (1,)), ((), ())),
            precision=lax.Precision.HIGHEST, preferred_element_type=F32,
        )
    loss_all[c, :, :rows] = loss

    for col in range(nc):
        @pl.when(col != c)
        def _():
            loss_copy(col).start()

    for j in range(m):
        @pl.when(c * m + j < z)
        def _():
            for h in range(PIECES):
                delta_copy(j, h).wait_send()

        @pl.when(code_sent(j))
        def _():
            code_copy(j).wait_send()

    @pl.when((z == final) & is_last)
    def _():
        for row in range(1, final):
            for i in range(k - 1):
                tri_copy(row, i).wait_send()

    def drain(q, _):
        g = group(q)
        for j in range(m):
            @pl.when((c * m + j > z) & (c * m + j < final))
            def _():
                run_copy(q, j).wait_send()

        @pl.when(is_last & (z == 0))
        def _():
            zero_sum(q).wait_send()

        @pl.when(is_last & (z > 0) & (z < final) & (solver(g) != z))
        def _():
            last_copy(q).wait_send()

        for col in range(nc):
            @pl.when(is_owner & ((col > c) | ((col == 0) & (c > 0) & (g >= z))))
            def _():
                core_copy(q, col).wait_send()

        down = is_owner & ((g < z) | ((g > z) & early_up))

        @pl.when(down | (is_last & (z < final) & (g > z) & jnp.logical_not(early_up)))
        def _():
            own_copy(q).wait_send()

        return 0

    with scope("drain"):
        lax.fori_loop(0, steps, drain, 0)

    @pl.when(is_last & (z == 1))
    def _():
        for h in range(PIECES):
            zero_copy(h).wait_send()

    for col in range(nc):
        @pl.when(col != c)
        def _():
            with scope("wait_loss"):
                arrived(loss_all.at[col], loss_recv.at[col])
    loss_sum = loss_all[0, 0:1, :rows]
    for col in range(1, nc):
        loss_sum = loss_sum + loss_all[col, 0:1, :rows]
    loss_out[...] = loss_sum

    for row in range(nr):
        @pl.when(row != z)
        def _():
            with scope("wait_mass"):
                arrived(mass_all.at[row], mass_recv.at[row])
    mass_sum = mass_all[0]
    for row in range(1, nr):
        mass_sum = mass_sum + mass_all[row]
    mass_out[...] = mass_sum
    for j in range(m):
        @pl.when(c * m + j < final)
        def _():
            @pl.when((c * m + j != z) | (c != 0))
            def _():
                with scope("wait_mass_part"):
                    arrived(mass_own.at[j], part_recv.at[j])
            mass_out[j * k:(j + 1) * k, :] = mass_out[j * k:(j + 1) * k, :] + mass_own[j]

    for row in range(nr):
        @pl.when(row != z)
        def _():
            mass_copy(row).wait_send()

        @pl.when(part_remote(row))
        def _():
            part_copy(row).wait_send()
    for col in range(nc):
        @pl.when(col != c)
        def _():
            loss_copy(col).wait_send()


def store(errors, loss, mass, errors_out, loss_out, mass_out, sems):
    copies = [
        pltpu.make_async_copy(source, target, sems.at[number])
        for number, (source, target) in enumerate(((errors, errors_out), (loss, loss_out), (mass, mass_out)))
    ]
    for copy in copies:
        copy.start()
    for copy in copies:
        copy.wait()


def local(nr, nc, weights, codebook, assign, chol_upper, inv_blocks):
    rows, width = weights.shape[1:]
    span = chol_upper.shape[1]
    m = width // span
    steps, piece = nr * PIECES, rows // PIECES
    blocks, code_count = codebook.shape[1], codebook.shape[3]
    block = inv_blocks.shape[2]
    k = span // block
    edges = max(k - 1, 1)
    dma = pltpu.SemaphoreType.DMA
    vmem = pl.BlockSpec(memory_space=pltpu.VMEM)
    hbm = pl.BlockSpec(memory_space=pltpu.HBM)
    shapes = ((rows, width), (1, rows), (blocks, code_count))
    results = pl.pallas_call(
        functools.partial(kernel, nr, nc),
        out_shape=tuple(pltpu.VMEM(shape, F32) for shape in shapes),
        in_specs=[hbm] * 5,
        out_specs=(vmem, vmem, vmem),
        scratch_shapes=[
            pltpu.VMEM(weights.shape[1:], F32),
            pltpu.VMEM(codebook.shape[1:], F32),
            pltpu.VMEM(assign.shape[1:], jnp.int32),
            pltpu.VMEM(inv_blocks.shape[1:], F32),
            pltpu.VMEM((span, width), F32),
            pltpu.VMEM((span, width), BF16),
            pltpu.VMEM((span, width), BF16),
            pltpu.VMEM((span, span), F32),
            pltpu.VMEM((span, span), F32),
            pltpu.VMEM((span, span), BF16),
            pltpu.VMEM((span, span), BF16),
            pltpu.VMEM((span, span), BF16),
            pltpu.VMEM((span, span), BF16),
            pltpu.VMEM((m, rows, span), F32),
            pltpu.VMEM((blocks, rows, block), jnp.int32),
            pltpu.VMEM((nr, rows, span), F32),
            pltpu.VMEM((nr, rows, max(span // 2, block)), jnp.int32),
            pltpu.VMEM((steps, m, piece, span), F32),
            pltpu.VMEM((steps, m, piece, span), F32),
            pltpu.VMEM((2, nr, PIECES, piece, span), F32),
            pltpu.VMEM((steps, piece, span), F32),
            pltpu.VMEM((steps, piece, span), F32),
            pltpu.VMEM((steps, piece, span), F32),
            pltpu.VMEM((m, rows, span), F32),
            pltpu.VMEM((PIECES, piece, span), F32),
            pltpu.VMEM((k * 2 * (code_count // LOW), block), F32),
            pltpu.VMEM((nr, blocks, code_count), F32),
            pltpu.VMEM((m, k, code_count), F32),
            pltpu.VMEM((k, code_count), F32),
            pltpu.VMEM((nc, 8, max(rows, 128)), F32),
            dma((5,)),
            dma((m, PIECES)), dma((nr, PIECES)),
            dma((m,)), dma((nr,)),
            dma((nr, edges)), dma((edges,)),
            dma((steps, m)), dma((steps, m)),
            dma((steps,)), dma((2, nr, PIECES)), dma((steps,)),
            dma((steps, nc)), dma((steps,)),
            dma((steps,)), dma((m, PIECES)), dma((PIECES,)),
            dma((nr,)), dma((m,)),
            dma((nr,)), dma((nr,)),
            dma((nc,)), dma((nc,)), pltpu.SemaphoreType.REGULAR,
        ],
        compiler_params=pltpu.CompilerParams(
            collective_id=0, has_side_effects=True, vmem_limit_bytes=40 * 1024 * 1024
        ),
    )(*(pltpu.with_memory_space_constraint(value[0], pltpu.HBM) for value in (
        weights, codebook, assign, inv_blocks, chol_upper,
    )))
    errors, loss, mass = pl.pallas_call(
        store,
        out_shape=tuple(jax.ShapeDtypeStruct(shape, F32) for shape in shapes),
        in_specs=[vmem] * 3,
        out_specs=[hbm] * 3,
        scratch_shapes=[dma((3,))],
        compiler_params=pltpu.CompilerParams(vmem_limit_bytes=1024 * 1024),
    )(*results)
    return errors[None], loss, mass[None]


def solution(mesh):
    return jax.shard_map(
        functools.partial(local, mesh.shape["row"], mesh.shape["col"]),
        mesh=mesh,
        in_specs=(
            P("ea", "row", "col"),
            P("ea", "col", None, None),
            P("ea", "row", "col"),
            P("ea", "row", "col"),
            P("ea", "col", None, None),
        ),
        out_specs=(P("ea", "row", "col"), P("ea", "row"), P("ea", "col", None)),
        check_vma=False,
    )
```

```python
import functools

import jax
import jax.numpy as jnp
from jax import lax
from jax.experimental import pallas as pl
from jax.experimental.pallas import tpu as pltpu
from jax.sharding import PartitionSpec as P

F32 = jnp.float32
BF16 = jnp.bfloat16
LOW = 16
PIECES = 2
scope = jax.named_scope


def halves(value):
    high = value.astype(BF16)
    return high, (value - high.astype(F32)).astype(BF16)


def dot(a, b):
    return jnp.dot(a, b, preferred_element_type=F32)


def dot3(a, b_high, b_low):
    rows = a.shape[0]
    high, low = halves(a)
    both = dot(jnp.concatenate([high, low], axis=0), b_high)
    return both[:rows] + both[rows:] + dot(high, b_low)


def dot_full(a, b):
    b_high, b_low = halves(b)
    return dot3(a, b_high, b_low)


def take(table, index):
    return jnp.take_along_axis(table, index, axis=1, mode="promise_in_bounds")


def kernel(
    nr, nc,
    weights_hbm, codebook_hbm, assign_hbm, inverse_hbm, factor,
    errors_out, loss_out, mass_out,
    weights, codebook, assign, inverse, u_raw, u_high, u_low, triangle, v_full, v_high, v_low, w_high, w_low,
    delta, codes, delta_in, codes_in, run_in, run_out, last_in, last_out, zero_in,
    err_block, err_own, err_zero, tally, mass_all, mass_own, mass_sent, loss_all, loss_up, loss_in,
    u_sem, d_send, d_recv, code_send, code_recv, tri_send, tri_recv, run_send, run_recv, last_send, last_recv, zero_recv,
    core_send, core_recv, own_send, own_recv, zero_send, part_send, part_recv, mass_send, mass_recv,
    loss_send, loss_recv, up_send, up_recv, ready,
):
    z = lax.axis_index("row")
    c = lax.axis_index("col")
    rows, width = weights.shape
    span = factor.shape[0]
    m = width // span
    block = inverse.shape[1]
    k = span // block
    code_count = codebook.shape[2]
    owner = z // m
    slot = z % m
    steps = nr * PIECES
    piece = rows // PIECES
    final = nr - 1
    pairs = span // 2
    window = max(pairs, block)
    is_owner = (c == owner) & (z < final)
    is_last = c == nc - 1

    def remote(src, dst, send, recv, row, col):
        return pltpu.make_async_remote_copy(
            src_ref=src, dst_ref=dst, send_sem=send, recv_sem=recv,
            device_id={"row": row, "col": col}, device_id_type=pl.DeviceIdType.MESH,
        )

    def arrived(ref, sem):
        pltpu.make_async_copy(ref, ref, sem).wait()

    loads = [
        pltpu.make_async_copy(source, target, u_sem.at[number])
        for number, (source, target) in enumerate((
            (assign_hbm, assign), (codebook_hbm, codebook), (weights_hbm, weights),
            (inverse_hbm, inverse), (factor, u_raw),
        ))
    ]
    for load in loads:
        load.start()

    barrier = pltpu.get_barrier_semaphore()
    for step in range(1, nr * nc):
        other = lax.rem(z * nc + c + step, nr * nc)

        @pl.when(z <= other // nc + 1)
        def _():
            pl.semaphore_signal(
                barrier, inc=1, device_id={"row": other // nc, "col": other % nc},
                device_id_type=pl.DeviceIdType.MESH,
            )

    def enter():
        with scope("entry"):
            pl.semaphore_wait(barrier, (jnp.minimum(z + 1, nr - 1) + 1) * nc - 1)

    def wait_ready():
        with scope("wait_ready"):
            pl.semaphore_wait(ready, (nr - 2 - z) * nc)

    def order(place):
        if nr < 3:
            return place
        return jnp.where(place == nr - 2, nr - 1, jnp.where(place == nr - 1, nr - 2, place))

    def group(q):
        return order(q // PIECES)

    def early_up(g):
        return (z > 0) & (owner < nc - 1) & (g == nr)

    def farthest(i):
        return order(nr - 1 - i // PIECES) * PIECES + i % PIECES

    def zero_order(i):
        turn = i // PIECES
        return farthest(jnp.where(turn == nr - 2, i + PIECES, jnp.where(turn == nr - 1, i - PIECES, i)))

    def nearest(i):
        return order(i // PIECES) * PIECES + i % PIECES

    def part_rows(q):
        return pl.ds(pl.multiple_of(q % PIECES * piece, piece), piece)

    def delta_copy(j, h):
        at = slice(h * piece, (h + 1) * piece)
        return remote(delta.at[j, at], delta_in.at[z, at], d_send.at[j, h], d_recv.at[z, h], c * m + j, c)

    def send_delta(j, when):
        @pl.when((c * m + j < z) & when)
        def _():
            for h in range(PIECES):
                delta_copy(j, h).start()

    def urgent(j):
        return (c * m + j == 0) & (z != nr - 2)

    def code_copy(j):
        low = j * pairs // window * window
        return remote(
            assign.at[:, low:low + window], codes_in.at[z], code_send.at[j], code_recv.at[z], c * m + j, 0
        )

    def code_sent(j):
        return (c * m + j <= z) & (c * m + j < final) & ((c > 0) | (c * m + j < z))

    def tri_copy(row, i):
        low = (m - 1) * span
        return remote(
            u_raw.at[i * block:(i + 1) * block, low + (i + 1) * block:low + span],
            triangle.at[i * block:(i + 1) * block, (i + 1) * block:span],
            tri_send.at[row, i], tri_recv.at[i], row, c,
        )

    def run_copy(q, j):
        return remote(run_out.at[q, j], run_in.at[q, j], run_send.at[q, j], run_recv.at[q, j], z + 1, c)

    def first(g):
        return jnp.where(g == 0, 1, 0)

    def solver(g):
        return jnp.maximum(g, 1)

    def last_copy(q):
        at = first(group(q)), z, q % PIECES
        return remote(last_out.at[q], last_in.at[at], last_send.at[q], last_recv.at[at], solver(group(q)), c)

    def zero_sum(q):
        return remote(last_out.at[q], zero_in.at[q], last_send.at[q], zero_recv.at[q], 1, c)

    def zero_copy(h):
        return remote(
            err_zero.at[h], err_own.at[m - 1, h * piece:(h + 1) * piece],
            zero_send.at[h], own_recv.at[m - 1, h], 0, c,
        )

    def core_copy(q, col):
        return remote(err_block.at[q], err_block.at[q], core_send.at[q, col], core_recv.at[q], z, col)

    def own_copy(q):
        return remote(
            err_block.at[q], err_own.at[slot, part_rows(q)],
            own_send.at[q], own_recv.at[slot, q % PIECES], group(q), owner,
        )

    with scope("first_loads"):
        for load in loads[:3]:
            load.wait()

    lane = lax.broadcasted_iota(jnp.int32, (rows, block), 1)

    def subtract(j):
        for b in range(j * k, (j + 1) * k):
            low = b * (block // 2)
            tile = low // block * block
            code = take(assign[:, tile:tile + block], low - tile + lane // 2)
            codes[b] = code
            inner = code % block
            value = jnp.zeros((rows, block), F32)
            for part in range(code_count // block):
                picked = []
                for comp in range(2):
                    table = codebook[b, comp:comp + 1, part * block:(part + 1) * block]
                    picked.append(take(jnp.broadcast_to(table, (rows, block)), inner))
                both = jnp.where(lane % 2 == 0, picked[0], picked[1])
                value = jnp.where(code // block == part, both, value)
            at = (b - j * k) * block
            delta[j, :, at:at + block] = weights[:, b * block:(b + 1) * block] - value

    subtract(0)

    @pl.when(z > 0)
    def _():
        enter()

    send_delta(0, urgent(0))

    for row in range(nr - 2):
        for col in range(nc):
            @pl.when(row + 1 < z)
            def _():
                pl.semaphore_signal(
                    ready, inc=1, device_id={"row": row, "col": col}, device_id_type=pl.DeviceIdType.MESH,
                )

    with scope("factor_loads"):
        for load in loads[3:]:
            load.wait()

    def rest():
        for j in range(1, m):
            subtract(j)

    @pl.when((z == final) & is_last)
    def _():
        for row in reversed(range(1, final)):
            for i in range(k - 1):
                tri_copy(row, i).start()

    def inverted(first, right):
        v_full[...] = jnp.zeros_like(v_full)

        def invert(lo, hi):
            if hi - lo == 1:
                v_full[lo * block:hi * block, lo * block:hi * block] = inverse[first + lo]
                return
            mid = (lo + hi) // 2
            invert(lo, mid)
            invert(mid, hi)
            top, middle, end = lo * block, mid * block, hi * block
            product = dot_full(v_full[top:middle, top:middle], right(top, middle, end))
            v_full[top:middle, middle:end] = -dot_full(product, v_full[middle:end, middle:end])

        invert(0, k)
        return halves(v_full[...])

    @pl.when(is_owner)
    def _():
        rest()
        base = slot * span
        high, low = inverted(slot * k, lambda top, middle, end: u_raw[
            top:middle, pl.ds(pl.multiple_of(base + middle, block), end - middle)
        ])
        v_high[...] = high
        v_low[...] = low

    @pl.when(jnp.logical_not(is_owner))
    def _():
        rest()

    for j in range(m):
        @pl.when(c * m + j > z)
        def _():
            high, low = halves(u_raw[:, j * span:(j + 1) * span])
            u_high[:, j * span:(j + 1) * span] = high
            u_low[:, j * span:(j + 1) * span] = low

    def invert_last():
        @pl.when(z == final)
        def _():
            triangle[...] = u_raw[:, (m - 1) * span:]

        @pl.when(z < final)
        def _():
            with scope("wait_triangle"):
                for i in range(k - 1):
                    part = triangle.at[i * block:(i + 1) * block, (i + 1) * block:span]
                    arrived(part, tri_recv.at[i])

        high, low = inverted((m - 1) * k, lambda top, middle, end: triangle[top:middle, middle:end])
        w_high[...] = high
        w_low[...] = low

    @pl.when(z == 0)
    def _():
        enter()

    for j in range(m):
        send_delta(j, jnp.logical_not(urgent(j)))

    for j in range(m):
        @pl.when(code_sent(j))
        def _():
            code_copy(j).start()

        @pl.when((c == 0) & (z == j) & (z < final))
        def _():
            low = j * pairs // window * window
            codes_in[z] = assign[:, low:low + window]

    late_core = (z == 0) & (c > owner)
    relay_core = (z > 0) & (z < final) & (c > owner)

    def forward(q, j):
        with scope("wait_far_sum"):
            arrived(run_in.at[q, j], run_recv.at[q, j])
        run_out[q, j] = run_out[q, j] + run_in[q, j]
        run_copy(q, j).start()

    def stage(q, _):
        g = group(q)
        at = part_rows(q)

        @pl.when(is_last & (((z == final) & (q == 0)) | ((z == final - 1) & (q == PIECES))))
        def _():
            invert_last()

        @pl.when((z > 0) & (z < nr - 2) & (q == (z + 1) * PIECES))
        def _():
            wait_ready()

        @pl.when(is_owner)
        def _():
            @pl.when(z == 0)
            def _():
                run_in[q, slot] = jnp.zeros((piece, span), F32)

            @pl.when(z > 0)
            def _():
                with scope("wait_own_sum"):
                    arrived(run_in.at[q, slot], run_recv.at[q, slot])

            @pl.when(g > z)
            def _():
                with scope("wait_delta"):
                    arrived(delta_in.at[g, at], d_recv.at[g, q % PIECES])

                run_in[q, slot] = run_in[q, slot] + delta_in[g, at]

            @pl.when(g == z)
            def _():
                run_in[q, slot] = run_in[q, slot] + delta[slot, at]

            error = dot3(run_in[q, slot], v_high[...], v_low[...])
            err_block[q] = error

            @pl.when(g == z)
            def _():
                err_own[slot, at] = error

            for col in range(nc):
                @pl.when((col > c) | ((col == 0) & (c > 0) & (g >= z)))
                def _():
                    core_copy(q, col).start()

            @pl.when((g < z) | ((g > z) & early_up(g)))
            def _():
                own_copy(q).start()

        @pl.when((c > owner) & (z < final))
        def _():
            with scope("wait_core"):
                arrived(err_block.at[q], core_recv.at[q])

        late = late_core & (q >= 2 * PIECES)
        @pl.when(is_last & (z < final))
        def _():
            j = m - 1
            change = dot3(
                err_block[q], u_high[:, j * span:(j + 1) * span], u_low[:, j * span:(j + 1) * span]
            )
            change = change - jnp.where((g == 0) & (z == 0), delta[j, at], 0.0)

            @pl.when((z <= 1) | (solver(g) != z))
            def _():
                last_out[q] = change

            @pl.when((z > 1) & (solver(g) == z))
            def _():
                last_in[first(g), z, q % PIECES] = change

            @pl.when((z > 1) & (solver(g) != z))
            def _():
                last_copy(q).start()

        for j in range(m):
            target = c * m + j

            @pl.when((target > z) & (target < final))
            def _():
                change = dot3(
                    err_block[q], u_high[:, j * span:(j + 1) * span], u_low[:, j * span:(j + 1) * span]
                )
                run_out[q, j] = jnp.where(g == z, delta[j, at], 0.0) - change

                @pl.when((z > 0) & jnp.logical_not(relay_core))
                def _():
                    with scope("wait_near_sum"):
                        arrived(run_in.at[q, j], run_recv.at[q, j])
                    run_out[q, j] = run_out[q, j] + run_in[q, j]

                @pl.when(jnp.logical_not(late | relay_core))
                def _():
                    run_copy(q, j).start()

                @pl.when(relay_core & (q >= PIECES))
                def _():
                    forward(q - PIECES, j)

        return 0

    lax.fori_loop(0, steps, stage, 0)

    @pl.when((z == 0) & (nr > 2))
    def _():
        wait_ready()

    for j in range(m):
        @pl.when(late_core & (c * m + j < final))
        def _():
            def release(q, _):
                run_copy(q, j).start()
                return 0

            lax.fori_loop(2 * PIECES, steps, release, 0)

        @pl.when(relay_core & (c * m + j < final))
        def _():
            def release(q, _):
                forward(q, j)
                return 0

            lax.fori_loop(steps - PIECES, steps, release, 0)

    @pl.when(late_core & is_last)
    def _():
        def release(i, _):
            zero_sum(zero_order(i)).start()
            return 0

        lax.fori_loop(0, steps, release, 0)

    def joined(q):
        with scope("wait_zero"):
            arrived(zero_in.at[q], zero_recv.at[q])
        return last_out[q] + zero_in[q]

    @pl.when(is_last & (z == 1) & (z < final))
    def _():
        def relayed(i, _):
            q = farthest(i)
            last_out[q] = joined(q)
            last_copy(q).start()
            return 0

        lax.fori_loop(0, steps - 2 * PIECES, relayed, 0)

    @pl.when(is_last & (z > 0) & (z < final - 1))
    def _():
        invert_last()

    def solved(which, h):
        with scope("wait_last"):
            for row in range(1, final):
                @pl.when(row != z)
                def _():
                    arrived(last_in.at[which, row, h], last_recv.at[which, row, h])
        total = -last_in[which, 1, h]
        for row in range(2, final):
            total = total - last_in[which, row, h]
        if which == 0:
            total = total + delta[m - 1, h * piece:(h + 1) * piece]
        return dot3(total, w_high[...], w_low[...])

    @pl.when(is_last & (z == 1))
    def _():
        for h in range(PIECES):
            last_in[1, 1, h] = joined(h)
            err_zero[h] = solved(1, h)
            zero_copy(h).start()
        for h in range(PIECES):
            last_in[0, 1, h] = joined(PIECES + h)

    def send_up():
        def upward(i, _):
            q = nearest(i)

            @pl.when((group(q) > z) & jnp.logical_not(early_up(group(q))))
            def _():
                own_copy(q).start()

            return 0

        lax.fori_loop(0, steps, upward, 0)

    @pl.when(is_last & (z > 0) & (z < final))
    def _():
        send_up()

    high_count = code_count // LOW
    fold = 2 * high_count
    chunk = 16
    half = chunk // 2

    def count(error_at, code_at):
        def gather(step, total):
            at = pl.ds(pl.multiple_of(step * chunk, chunk), chunk)
            iota_high = lax.broadcasted_iota(jnp.int32, (high_count, block), 0)
            iota_low = lax.broadcasted_iota(jnp.int32, (LOW, block), 0)
            left, right = [], []
            even = lax.broadcasted_iota(jnp.int32, (half, block), 1) % 2 == 0
            for b in range(k):
                code = code_at(b, at)
                code = jnp.where(even, code[:half], code[half:])
                value = error_at[at, b * block:(b + 1) * block]
                value = value * value
                upper, lower = value[:half], value[half:]
                value = jnp.where(even, upper + pltpu.roll(upper, block - 1, 1), lower + pltpu.roll(lower, 1, 1))
                coarse = value.astype(BF16).astype(F32)
                fine = value - coarse
                code_high, code_low = code // LOW, code % LOW
                top, bottom, marks = [], [], []
                for r in range(half):
                    hit = jnp.broadcast_to(code_high[r:r + 1], (high_count, block)) == iota_high
                    top.append(jnp.where(hit, jnp.broadcast_to(coarse[r:r + 1], (high_count, block)), 0.0).astype(BF16))
                    bottom.append(jnp.where(hit, jnp.broadcast_to(fine[r:r + 1], (high_count, block)), 0.0).astype(BF16))
                    low_hit = jnp.broadcast_to(code_low[r:r + 1], (LOW, block)) == iota_low
                    marks.append(jnp.where(low_hit, 1.0, 0.0).astype(BF16))
                left += [jnp.concatenate(top, axis=1), jnp.concatenate(bottom, axis=1)]
                right.append(jnp.concatenate(marks, axis=1))
            return total + lax.dot_general(
                jnp.concatenate(left, axis=0), jnp.concatenate(right, axis=0),
                (((1,), (1,)), ((), ())), preferred_element_type=F32,
            )

        total = lax.fori_loop(0, piece // chunk, gather, jnp.zeros((k * fold, k * LOW), F32), unroll=2)
        tally[:, :k * LOW] = tally[:, :k * LOW] + total

    def spread(store):
        spot = lax.broadcasted_iota(jnp.int32, (high_count, block), 1)
        level = lax.broadcasted_iota(jnp.int32, (high_count, block), 0)
        for b in range(k):
            total = tally[b * fold:b * fold + high_count] + tally[b * fold + high_count:(b + 1) * fold]
            total = take(total, b * LOW + spot % LOW)
            for part in range(code_count // block):
                mine = level == part * (block // LOW) + spot // LOW
                store(b, part, jnp.sum(jnp.where(mine, total, 0.0), axis=0, keepdims=True))
        tally[...] = jnp.zeros_like(tally)

    tally[...] = jnp.zeros_like(tally)
    mass_all[z] = jnp.zeros(mass_all.shape[1:], F32)
    counts = (c == 0) & (z < final)

    def row_sums(error):
        return lax.dot_general(
            jnp.ones((8, span), F32), error * error, (((1,), (1,)), ((), ())),
            precision=lax.Precision.HIGHEST, preferred_element_type=F32,
        )

    def up_copy(row, col):
        return remote(loss_up.at[row], loss_in.at[z], up_send.at[row, col], up_recv.at[z], row, col)

    def part_copy(row):
        return remote(mass_sent, mass_own.at[slot], part_send.at[row], part_recv.at[slot], row, owner)

    def part_remote(row):
        return counts & ((row != z) | (owner != 0))

    @pl.when(counts)
    def _():
        def own_part(q, _):
            g = group(q)

            @pl.when(g >= z)
            def _():
                with scope("wait_part"):
                    @pl.when(owner != 0)
                    def _():
                        arrived(err_block.at[q], core_recv.at[q])

                    @pl.when(((g != z) | (owner != 0)) & (q % PIECES == 0))
                    def _():
                        arrived(codes_in.at[g], code_recv.at[g])

                shift = 0 if window == pairs else lax.rem(slot * pairs, window)

                def code_at(b, at):
                    low = b * (block // 2)
                    tile = low // block * block
                    source = codes_in[g, pl.ds(q % PIECES * piece + at.start, chunk), tile:tile + block]
                    return take(source, shift + low - tile + lane[:chunk] // 2)

                count(err_block.at[q], code_at)

            @pl.when((g > z) & (q % PIECES == PIECES - 1))
            def _():
                error = jnp.concatenate([err_block[q - PIECES + 1 + h] for h in range(PIECES)], axis=0)
                loss_up[g, :, :rows] = row_sums(error)
                for col in range(nc):
                    up_copy(g, col).start()

            return 0

        lax.fori_loop(0, steps, own_part, 0)

        def store(b, part, value):
            mass_sent[b:b + 1, part * block:(part + 1) * block] = value

        spread(store)

        @pl.when(owner == 0)
        def _():
            mass_own[slot] = mass_sent[...]

    for row in range(nr):
        @pl.when(part_remote(row))
        def _():
            part_copy(row).start()

    def own_spread(j):
        def store(b, part, value):
            mass_all[z, j * k + b:j * k + b + 1, part * block:(part + 1) * block] = value

        spread(store)

    for j in range(m):
        @pl.when((c * m + j > z) & ((c * m + j < final) | (z == 0)))
        def _():
            for h in range(PIECES):
                with scope("wait_down"):
                    arrived(err_own.at[j, h * piece:(h + 1) * piece], own_recv.at[j, h])
                count(
                    err_own.at[j, h * piece:(h + 1) * piece],
                    lambda b, at: codes[j * k + b, pl.ds(h * piece + at.start, chunk), :],
                )
            own_spread(j)

        if j == 0:
            @pl.when(is_last & (z == 0))
            def _():
                send_up()

    @pl.when(is_last & (z > 0))
    def _():
        j = m - 1
        for h in range(PIECES):
            err_own[j, h * piece:(h + 1) * piece] = solved(0, h)
            count(
                err_own.at[j, h * piece:(h + 1) * piece],
                lambda b, at: codes[j * k + b, pl.ds(h * piece + at.start, chunk), :],
            )
        own_spread(j)

    def mass_copy(row):
        return remote(mass_all.at[z], mass_all.at[z], mass_send.at[row], mass_recv.at[z], row, c)

    def loss_copy(col):
        return remote(loss_all.at[c], loss_all.at[c], loss_send.at[col], loss_recv.at[c], z, col)

    for row in range(nr):
        @pl.when(row != z)
        def _():
            mass_copy(row).start()

    loss_all[c] = jnp.zeros(loss_all.shape[1:], F32)
    for j in range(m):
        @pl.when((c * m + j >= z) & ((c * m + j < final) | is_last))
        def _():
            loss_all[c, :, :rows] = loss_all[c, :, :rows] + row_sums(err_own[j])

    for col in range(nc):
        @pl.when(col != c)
        def _():
            loss_copy(col).start()

    for j in reversed(range(m)):
        @pl.when(c * m + j < z)
        def _():
            with scope("wait_up"):
                for h in range(PIECES):
                    arrived(err_own.at[j, h * piece:(h + 1) * piece], own_recv.at[j, h])

        errors_out[:, j * span:(j + 1) * span] = err_own[j]

    for j in range(m):
        @pl.when(c * m + j < z)
        def _():
            for h in range(PIECES):
                delta_copy(j, h).wait_send()

        @pl.when(code_sent(j))
        def _():
            code_copy(j).wait_send()

    @pl.when((z == final) & is_last)
    def _():
        for row in range(1, final):
            for i in range(k - 1):
                tri_copy(row, i).wait_send()

    def drain(q, _):
        g = group(q)
        for j in range(m):
            @pl.when((c * m + j > z) & (c * m + j < final))
            def _():
                run_copy(q, j).wait_send()

        @pl.when(is_last & (z == 0))
        def _():
            zero_sum(q).wait_send()

        @pl.when(is_last & (z > 0) & (z < final) & (solver(g) != z))
        def _():
            last_copy(q).wait_send()

        for col in range(nc):
            @pl.when(is_owner & ((col > c) | ((col == 0) & (c > 0) & (g >= z))))
            def _():
                core_copy(q, col).wait_send()

        early = early_up(g)

        @pl.when((is_owner & ((g < z) | ((g > z) & early))) | (is_last & (z < final) & (g > z) & jnp.logical_not(early)))
        def _():
            own_copy(q).wait_send()

        return 0

    with scope("drain"):
        lax.fori_loop(0, steps, drain, 0)

    @pl.when(is_last & (z == 1))
    def _():
        for h in range(PIECES):
            zero_copy(h).wait_send()

    for row in range(nr):
        @pl.when(row != z)
        def _():
            mass_copy(row).wait_send()

        @pl.when(part_remote(row))
        def _():
            part_copy(row).wait_send()

        @pl.when(counts & (row > z))
        def _():
            for col in range(nc):
                up_copy(row, col).wait_send()
    for col in range(nc):
        @pl.when(col != c)
        def _():
            loss_copy(col).wait_send()

    for col in range(nc):
        @pl.when(col != c)
        def _():
            with scope("wait_loss"):
                arrived(loss_all.at[col], loss_recv.at[col])
    loss_sum = loss_all[0, 0:1, :rows]
    for col in range(1, nc):
        loss_sum = loss_sum + loss_all[col, 0:1, :rows]
    loss_out[...] = loss_sum
    for row in range(final):
        @pl.when(row < z)
        def _():
            with scope("wait_loss_up"):
                arrived(loss_in.at[row], up_recv.at[row])
            loss_out[...] = loss_out[...] + loss_in[row, 0:1, :rows]

    for row in range(nr):
        @pl.when(row != z)
        def _():
            with scope("wait_mass"):
                arrived(mass_all.at[row], mass_recv.at[row])
    mass_sum = mass_all[0]
    for row in range(1, nr):
        mass_sum = mass_sum + mass_all[row]
    mass_out[...] = mass_sum
    for j in range(m):
        @pl.when(c * m + j < final)
        def _():
            @pl.when((c * m + j != z) | (c != 0))
            def _():
                with scope("wait_mass_part"):
                    arrived(mass_own.at[j], part_recv.at[j])
            mass_out[j * k:(j + 1) * k, :] = mass_out[j * k:(j + 1) * k, :] + mass_own[j]


def store(errors, loss, mass, errors_out, loss_out, mass_out, sems):
    copies = [
        pltpu.make_async_copy(source, target, sems.at[number])
        for number, (source, target) in enumerate(((errors, errors_out), (loss, loss_out), (mass, mass_out)))
    ]
    for copy in copies:
        copy.start()
    for copy in copies:
        copy.wait()


def local(nr, nc, weights, codebook, assign, chol_upper, inv_blocks):
    rows, width = weights.shape[1:]
    span = chol_upper.shape[1]
    m = width // span
    steps, piece = nr * PIECES, rows // PIECES
    blocks, code_count = codebook.shape[1], codebook.shape[3]
    block = inv_blocks.shape[2]
    k = span // block
    edges = max(k - 1, 1)
    dma = pltpu.SemaphoreType.DMA
    vmem = pl.BlockSpec(memory_space=pltpu.VMEM)
    hbm = pl.BlockSpec(memory_space=pltpu.HBM)
    shapes = ((rows, width), (1, rows), (blocks, code_count))
    results = pl.pallas_call(
        functools.partial(kernel, nr, nc),
        out_shape=tuple(pltpu.VMEM(shape, F32) for shape in shapes),
        in_specs=[hbm] * 5,
        out_specs=(vmem, vmem, vmem),
        scratch_shapes=[
            pltpu.VMEM(weights.shape[1:], F32),
            pltpu.VMEM(codebook.shape[1:], F32),
            pltpu.VMEM(assign.shape[1:], jnp.int32),
            pltpu.VMEM(inv_blocks.shape[1:], F32),
            pltpu.VMEM((span, width), F32),
            pltpu.VMEM((span, width), BF16),
            pltpu.VMEM((span, width), BF16),
            pltpu.VMEM((span, span), F32),
            pltpu.VMEM((span, span), F32),
            pltpu.VMEM((span, span), BF16),
            pltpu.VMEM((span, span), BF16),
            pltpu.VMEM((span, span), BF16),
            pltpu.VMEM((span, span), BF16),
            pltpu.VMEM((m, rows, span), F32),
            pltpu.VMEM((blocks, rows, block), jnp.int32),
            pltpu.VMEM((nr, rows, span), F32),
            pltpu.VMEM((nr, rows, max(span // 2, block)), jnp.int32),
            pltpu.VMEM((steps, m, piece, span), F32),
            pltpu.VMEM((steps, m, piece, span), F32),
            pltpu.VMEM((2, nr, PIECES, piece, span), F32),
            pltpu.VMEM((steps, piece, span), F32),
            pltpu.VMEM((steps, piece, span), F32),
            pltpu.VMEM((steps, piece, span), F32),
            pltpu.VMEM((m, rows, span), F32),
            pltpu.VMEM((PIECES, piece, span), F32),
            pltpu.VMEM((k * 2 * (code_count // LOW), block), F32),
            pltpu.VMEM((nr, blocks, code_count), F32),
            pltpu.VMEM((m, k, code_count), F32),
            pltpu.VMEM((k, code_count), F32),
            pltpu.VMEM((nc, 8, max(rows, 128)), F32),
            pltpu.VMEM((nr, 8, max(rows, 128)), F32),
            pltpu.VMEM((nr, 8, max(rows, 128)), F32),
            dma((5,)),
            dma((m, PIECES)), dma((nr, PIECES)),
            dma((m,)), dma((nr,)),
            dma((nr, edges)), dma((edges,)),
            dma((steps, m)), dma((steps, m)),
            dma((steps,)), dma((2, nr, PIECES)), dma((steps,)),
            dma((steps, nc)), dma((steps,)),
            dma((steps,)), dma((m, PIECES)), dma((PIECES,)),
            dma((nr,)), dma((m,)),
            dma((nr,)), dma((nr,)),
            dma((nc,)), dma((nc,)),
            dma((nr, nc)), dma((nr,)), pltpu.SemaphoreType.REGULAR,
        ],
        compiler_params=pltpu.CompilerParams(
            collective_id=0, has_side_effects=True, vmem_limit_bytes=40 * 1024 * 1024
        ),
    )(*(pltpu.with_memory_space_constraint(value[0], pltpu.HBM) for value in (
        weights, codebook, assign, inv_blocks, chol_upper,
    )))
    errors, loss, mass = pl.pallas_call(
        store,
        out_shape=tuple(jax.ShapeDtypeStruct(shape, F32) for shape in shapes),
        in_specs=[vmem] * 3,
        out_specs=[hbm] * 3,
        scratch_shapes=[dma((3,))],
        compiler_params=pltpu.CompilerParams(vmem_limit_bytes=1024 * 1024),
    )(*results)
    return errors[None], loss, mass[None]


def solution(mesh):
    return jax.shard_map(
        functools.partial(local, mesh.shape["row"], mesh.shape["col"]),
        mesh=mesh,
        in_specs=(
            P("ea", "row", "col"),
            P("ea", "col", None, None),
            P("ea", "row", "col"),
            P("ea", "row", "col"),
            P("ea", "col", None, None),
        ),
        out_specs=(P("ea", "row", "col"), P("ea", "row"), P("ea", "col", None)),
        check_vma=False,
    )
```

```python
import functools

import jax
import jax.numpy as jnp
from jax import lax
from jax.experimental import pallas as pl
from jax.experimental.pallas import tpu as pltpu
from jax.sharding import PartitionSpec as P

F32 = jnp.float32
BF16 = jnp.bfloat16
LOW = 16
PIECES = 2
scope = jax.named_scope


def halves(value):
    high = value.astype(BF16)
    return high, (value - high.astype(F32)).astype(BF16)


def dot(a, b):
    return jnp.dot(a, b, preferred_element_type=F32)


def dot3(a, b_high, b_low):
    rows = a.shape[0]
    high, low = halves(a)
    both = dot(jnp.concatenate([high, low], axis=0), b_high)
    return both[:rows] + both[rows:] + dot(high, b_low)


def dot_full(a, b):
    b_high, b_low = halves(b)
    return dot3(a, b_high, b_low)


def take(table, index):
    return jnp.take_along_axis(table, index, axis=1, mode="promise_in_bounds")


def kernel(
    nr, nc,
    weights_hbm, codebook_hbm, assign_hbm, inverse_hbm, factor,
    errors_out, loss_out, mass_out,
    weights, codebook, assign, inverse, u_raw, u_high, u_low, triangle, v_full, v_high, v_low, w_high, w_low,
    delta, codes, delta_in, codes_in, run_in, run_out, last_in, last_out, zero_in,
    err_block, err_own, err_zero, tally, mass_all, mass_own, mass_sent, loss_all, loss_up, loss_in,
    u_sem, d_send, d_recv, code_send, code_recv, tri_send, tri_recv, run_send, run_recv, last_send, last_recv, zero_recv,
    core_send, core_recv, own_send, own_recv, zero_send, part_send, part_recv, mass_send, mass_recv,
    loss_send, loss_recv, up_send, up_recv, ready,
):
    z = lax.axis_index("row")
    c = lax.axis_index("col")
    rows, width = weights.shape
    span = factor.shape[0]
    m = width // span
    block = inverse.shape[1]
    k = span // block
    code_count = codebook.shape[2]
    owner = z // m
    slot = z % m
    steps = nr * PIECES
    piece = rows // PIECES
    final = nr - 1
    pairs = span // 2
    window = max(pairs, block)
    is_owner = (c == owner) & (z < final)
    is_last = c == nc - 1

    def remote(src, dst, send, recv, row, col):
        return pltpu.make_async_remote_copy(
            src_ref=src, dst_ref=dst, send_sem=send, recv_sem=recv,
            device_id={"row": row, "col": col}, device_id_type=pl.DeviceIdType.MESH,
        )

    def arrived(ref, sem):
        pltpu.make_async_copy(ref, ref, sem).wait()

    loads = [
        pltpu.make_async_copy(source, target, u_sem.at[number])
        for number, (source, target) in enumerate((
            (assign_hbm, assign), (codebook_hbm, codebook), (weights_hbm, weights),
            (inverse_hbm, inverse),
        ))
    ]
    loads += [
        pltpu.make_async_copy(
            factor.at[:, j * span:(j + 1) * span], u_raw.at[:, j * span:(j + 1) * span], u_sem.at[4 + j]
        )
        for j in range(m)
    ]
    for load in loads:
        load.start()

    barrier = pltpu.get_barrier_semaphore()
    for step in range(1, nr * nc):
        other = lax.rem(z * nc + c + step, nr * nc)

        @pl.when(z <= other // nc + 1)
        def _():
            pl.semaphore_signal(
                barrier, inc=1, device_id={"row": other // nc, "col": other % nc},
                device_id_type=pl.DeviceIdType.MESH,
            )

    def enter():
        with scope("entry"):
            pl.semaphore_wait(barrier, (jnp.minimum(z + 1, nr - 1) + 1) * nc - 1)

    def wait_ready():
        with scope("wait_ready"):
            pl.semaphore_wait(ready, (nr - 2 - z) * nc)

    def order(place):
        if nr < 3:
            return place
        return jnp.where(place == nr - 2, nr - 1, jnp.where(place == nr - 1, nr - 2, place))

    def group(q):
        return order(q // PIECES)

    def early_up(g):
        return (z > 0) & (owner < nc - 1) & (g == nr - 1)

    def farthest(i):
        return order(nr - 1 - i // PIECES) * PIECES + i % PIECES

    def zero_order(i):
        turn = i // PIECES
        return farthest(jnp.where(turn == nr - 2, i + PIECES, jnp.where(turn == nr - 1, i - PIECES, i)))

    def nearest(i):
        return order(i // PIECES) * PIECES + i % PIECES

    def part_rows(q):
        return pl.ds(pl.multiple_of(q % PIECES * piece, piece), piece)

    def delta_copy(j, h):
        at = slice(h * piece, (h + 1) * piece)
        return remote(delta.at[j, at], delta_in.at[z, at], d_send.at[j], d_recv.at[z, h], c * m + j, c)

    def send_delta(j, when):
        @pl.when((c * m + j < z) & when)
        def _():
            for h in range(PIECES):
                delta_copy(j, h).start()

    def urgent(j):
        return (c * m + j == 0) & (z != nr - 2)

    def code_copy(j):
        low = j * pairs // window * window
        return remote(
            assign.at[:, low:low + window], codes_in.at[z], code_send.at[j], code_recv.at[z], c * m + j, 0
        )

    def code_sent(j):
        return (c * m + j <= z) & (c * m + j < final) & ((c > 0) | (c * m + j < z))

    def tri_copy(row, i):
        low = (m - 1) * span
        return remote(
            u_raw.at[i * block:(i + 1) * block, low + (i + 1) * block:low + span],
            triangle.at[i * block:(i + 1) * block, (i + 1) * block:span],
            tri_send, tri_recv, row, c,
        )

    def run_copy(q, j):
        return remote(run_out.at[q, j], run_in.at[q, j], run_send.at[j], run_recv.at[q, j], z + 1, c)

    def first(g):
        return jnp.where(g == 0, 1, 0)

    def solver(g):
        return jnp.maximum(g, 1)

    def last_copy(q):
        which, h = first(group(q)), q % PIECES
        return remote(last_out.at[q], last_in.at[which, h, z], last_send, last_recv.at[which, h], solver(group(q)), c)

    def zero_sum(q):
        return remote(last_out.at[q], zero_in.at[q], last_send, zero_recv.at[q], 1, c)

    def zero_copy(h):
        return remote(
            err_zero.at[h], err_own.at[m - 1, h * piece:(h + 1) * piece],
            zero_send, own_recv.at[m - 1, h], 0, c,
        )

    def core_copy(q, col):
        return remote(err_block.at[q], err_block.at[q], core_send.at[col], core_recv.at[q], z, col)

    def own_copy(q):
        return remote(
            err_block.at[q], err_own.at[slot, part_rows(q)],
            own_send.at[q], own_recv.at[slot, q % PIECES], group(q), owner,
        )

    with scope("first_loads"):
        for load in loads[:3]:
            load.wait()

    lane = lax.broadcasted_iota(jnp.int32, (rows, block), 1)

    def subtract(j):
        for b in range(j * k, (j + 1) * k):
            low = b * (block // 2)
            tile = low // block * block
            code = take(assign[:, tile:tile + block], low - tile + lane // 2)
            codes[b] = code
            inner = code % block
            value = jnp.zeros((rows, block), F32)
            for part in range(code_count // block):
                picked = []
                for comp in range(2):
                    table = codebook[b, comp:comp + 1, part * block:(part + 1) * block]
                    picked.append(take(jnp.broadcast_to(table, (rows, block)), inner))
                both = jnp.where(lane % 2 == 0, picked[0], picked[1])
                value = jnp.where(code // block == part, both, value)
            at = (b - j * k) * block
            delta[j, :, at:at + block] = weights[:, b * block:(b + 1) * block] - value

    subtract(0)

    @pl.when(z > 0)
    def _():
        enter()

    send_delta(0, urgent(0))

    for row in range(nr - 2):
        for col in range(nc):
            @pl.when(row + 1 < z)
            def _():
                pl.semaphore_signal(
                    ready, inc=1, device_id={"row": row, "col": col}, device_id_type=pl.DeviceIdType.MESH,
                )

    def rest():
        for j in range(1, m):
            subtract(j)

    def inverted(first, right):
        v_full[...] = jnp.zeros_like(v_full)

        def invert(lo, hi):
            if hi - lo == 1:
                v_full[lo * block:hi * block, lo * block:hi * block] = inverse[first + lo]
                return
            mid = (lo + hi) // 2
            invert(lo, mid)
            invert(mid, hi)
            top, middle, end = lo * block, mid * block, hi * block
            product = dot_full(v_full[top:middle, top:middle], right(top, middle, end))
            v_full[top:middle, middle:end] = -dot_full(product, v_full[middle:end, middle:end])

        invert(0, k)
        return halves(v_full[...])

    @pl.when(is_owner)
    def _():
        with scope("factor_loads"):
            loads[3].wait()
            for j in range(m):
                @pl.when(slot == j)
                def _():
                    loads[4 + j].wait()
        rest()
        base = slot * span
        high, low = inverted(slot * k, lambda top, middle, end: u_raw[
            top:middle, pl.ds(pl.multiple_of(base + middle, block), end - middle)
        ])
        v_high[...] = high
        v_low[...] = low

    @pl.when(jnp.logical_not(is_owner))
    def _():
        loads[3].wait()
        for j in range(m):
            loads[4 + j].wait()

        @pl.when((z == final) & is_last)
        def _():
            for row in reversed(range(1, final)):
                for i in range(k - 1):
                    tri_copy(row, i).start()

        rest()

    for j in range(m):
        @pl.when(is_owner & (slot != j))
        def _():
            loads[4 + j].wait()

    for j in range(m):
        @pl.when(c * m + j > z)
        def _():
            high, low = halves(u_raw[:, j * span:(j + 1) * span])
            u_high[:, j * span:(j + 1) * span] = high
            u_low[:, j * span:(j + 1) * span] = low

    def invert_last():
        @pl.when(z == final)
        def _():
            triangle[...] = u_raw[:, (m - 1) * span:]

        @pl.when(z < final)
        def _():
            with scope("wait_triangle"):
                if k > 1:
                    arrived(triangle.at[:block * (k - 1), :block * k // 2], tri_recv)

        high, low = inverted((m - 1) * k, lambda top, middle, end: triangle[top:middle, middle:end])
        w_high[...] = high
        w_low[...] = low

    @pl.when(z == 0)
    def _():
        enter()

    for j in range(m):
        send_delta(j, jnp.logical_not(urgent(j)))

    for j in range(m):
        @pl.when(code_sent(j))
        def _():
            code_copy(j).start()

        @pl.when((c == 0) & (z == j) & (z < final))
        def _():
            low = j * pairs // window * window
            codes_in[z] = assign[:, low:low + window]

    late_core = (z == 0) & (c > owner)
    relay_core = (z > 0) & (z < final) & (c > owner)

    def forward(q, j):
        with scope("wait_far_sum"):
            arrived(run_in.at[q, j], run_recv.at[q, j])
        run_out[q, j] = run_out[q, j] + run_in[q, j]
        run_copy(q, j).start()

    def stage(q, _):
        g = group(q)
        at = part_rows(q)

        @pl.when(is_last & (((z == final) & (q == 0)) | ((z == final - 1) & (q == PIECES))))
        def _():
            invert_last()

        @pl.when((z > 0) & (z < nr - 2) & (q == (z + 1) * PIECES))
        def _():
            wait_ready()

        @pl.when(is_owner)
        def _():
            @pl.when(z == 0)
            def _():
                run_in[q, slot] = jnp.zeros((piece, span), F32)

            @pl.when(z > 0)
            def _():
                with scope("wait_own_sum"):
                    arrived(run_in.at[q, slot], run_recv.at[q, slot])

            @pl.when(g > z)
            def _():
                with scope("wait_delta"):
                    arrived(delta_in.at[g, at], d_recv.at[g, q % PIECES])

                run_in[q, slot] = run_in[q, slot] + delta_in[g, at]

            @pl.when(g == z)
            def _():
                run_in[q, slot] = run_in[q, slot] + delta[slot, at]

            error = dot3(run_in[q, slot], v_high[...], v_low[...])
            err_block[q] = error

            @pl.when(g == z)
            def _():
                err_own[slot, at] = error

            for col in range(nc):
                @pl.when((col > c) | ((col == 0) & (c > 0)))
                def _():
                    core_copy(q, col).start()

            @pl.when((g < z) | ((g > z) & early_up(g)))
            def _():
                own_copy(q).start()

        @pl.when((c > owner) & (z < final))
        def _():
            with scope("wait_core"):
                arrived(err_block.at[q], core_recv.at[q])

        late = late_core & (q >= 2 * PIECES)
        @pl.when(is_last & (z < final))
        def _():
            j = m - 1
            change = dot3(
                err_block[q], u_high[:, j * span:(j + 1) * span], u_low[:, j * span:(j + 1) * span]
            )
            change = change - jnp.where((g == 0) & (z == 0), delta[j, at], 0.0)

            @pl.when((z <= 1) | (solver(g) != z))
            def _():
                last_out[q] = change

            @pl.when((z > 1) & (solver(g) == z))
            def _():
                last_in[first(g), q % PIECES, z] = change

            @pl.when((z > 1) & (solver(g) != z))
            def _():
                last_copy(q).start()

        for j in range(m):
            target = c * m + j

            @pl.when((target > z) & (target < final))
            def _():
                change = dot3(
                    err_block[q], u_high[:, j * span:(j + 1) * span], u_low[:, j * span:(j + 1) * span]
                )
                run_out[q, j] = jnp.where(g == z, delta[j, at], 0.0) - change

                @pl.when((z > 0) & jnp.logical_not(relay_core))
                def _():
                    with scope("wait_near_sum"):
                        arrived(run_in.at[q, j], run_recv.at[q, j])
                    run_out[q, j] = run_out[q, j] + run_in[q, j]

                @pl.when(jnp.logical_not(late | relay_core))
                def _():
                    run_copy(q, j).start()

                @pl.when(relay_core & (q >= PIECES))
                def _():
                    forward(q - PIECES, j)

        return 0

    lax.fori_loop(0, steps, stage, 0)

    @pl.when((z == 0) & (nr > 2))
    def _():
        wait_ready()

    for j in range(m):
        @pl.when(late_core & (c * m + j < final))
        def _():
            def release(q, _):
                run_copy(q, j).start()
                return 0

            lax.fori_loop(2 * PIECES, steps, release, 0)

        @pl.when(relay_core & (c * m + j < final))
        def _():
            def release(q, _):
                forward(q, j)
                return 0

            lax.fori_loop(steps - PIECES, steps, release, 0)

    @pl.when(late_core & is_last)
    def _():
        def release(i, _):
            zero_sum(zero_order(i)).start()
            return 0

        lax.fori_loop(0, steps, release, 0)

    def joined(q):
        with scope("wait_zero"):
            arrived(zero_in.at[q], zero_recv.at[q])
        return last_out[q] + zero_in[q]

    @pl.when(is_last & (z == 1) & (z < final))
    def _():
        def relayed(i, _):
            q = farthest(i)
            last_out[q] = joined(q)
            last_copy(q).start()
            return 0

        lax.fori_loop(0, steps - 2 * PIECES, relayed, 0)

    def send_up():
        def upward(i, _):
            q = nearest(i)

            @pl.when((group(q) > z) & jnp.logical_not(early_up(group(q))))
            def _():
                own_copy(q).start()

            return 0

        lax.fori_loop(0, steps, upward, 0)

    @pl.when(is_last & (z > 0) & (z < final - 1))
    def _():
        invert_last()

    @pl.when(is_last & (z > 0) & (z < final))
    def _():
        send_up()

    def solved(which, h):
        with scope("wait_last"):
            if nr > 3:
                @pl.when(z < final)
                def _():
                    arrived(last_in.at[which, h, :nr - 3], last_recv.at[which, h])

            @pl.when(z == final)
            def _():
                arrived(last_in.at[which, h, :nr - 2], last_recv.at[which, h])
        total = -last_in[which, h, 1]
        for row in range(2, final):
            total = total - last_in[which, h, row]
        if which == 0:
            total = total + delta[m - 1, h * piece:(h + 1) * piece]
        return dot3(total, w_high[...], w_low[...])

    @pl.when(is_last & (z == 1))
    def _():
        for h in range(PIECES):
            last_in[1, h, 1] = joined(h)
            err_zero[h] = solved(1, h)
            zero_copy(h).start()
    high_count = code_count // LOW
    fold = 2 * high_count
    chunk = 16
    half = chunk // 2

    def count(error_at, code_at):
        def gather(step, total):
            at = pl.ds(pl.multiple_of(step * chunk, chunk), chunk)
            iota_high = lax.broadcasted_iota(jnp.int32, (high_count, block), 0)
            iota_low = lax.broadcasted_iota(jnp.int32, (LOW, block), 0)
            left, right = [], []
            even = lax.broadcasted_iota(jnp.int32, (half, block), 1) % 2 == 0
            for b in range(k):
                code = code_at(b, at)
                code = jnp.where(even, code[:half], code[half:])
                value = error_at[at, b * block:(b + 1) * block]
                value = value * value
                upper, lower = value[:half], value[half:]
                value = jnp.where(even, upper + pltpu.roll(upper, block - 1, 1), lower + pltpu.roll(lower, 1, 1))
                coarse = value.astype(BF16).astype(F32)
                fine = value - coarse
                code_high, code_low = code // LOW, code % LOW
                top, bottom, marks = [], [], []
                for r in range(half):
                    hit = jnp.broadcast_to(code_high[r:r + 1], (high_count, block)) == iota_high
                    top.append(jnp.where(hit, jnp.broadcast_to(coarse[r:r + 1], (high_count, block)), 0.0).astype(BF16))
                    bottom.append(jnp.where(hit, jnp.broadcast_to(fine[r:r + 1], (high_count, block)), 0.0).astype(BF16))
                    low_hit = jnp.broadcast_to(code_low[r:r + 1], (LOW, block)) == iota_low
                    marks.append(jnp.where(low_hit, 1.0, 0.0).astype(BF16))
                left += [jnp.concatenate(top, axis=1), jnp.concatenate(bottom, axis=1)]
                right.append(jnp.concatenate(marks, axis=1))
            return total + lax.dot_general(
                jnp.concatenate(left, axis=0), jnp.concatenate(right, axis=0),
                (((1,), (1,)), ((), ())), preferred_element_type=F32,
            )

        total = lax.fori_loop(0, piece // chunk, gather, jnp.zeros((k * fold, k * LOW), F32), unroll=2)
        tally[:, :k * LOW] = tally[:, :k * LOW] + total

    def spread(store):
        spot = lax.broadcasted_iota(jnp.int32, (high_count, block), 1)
        level = lax.broadcasted_iota(jnp.int32, (high_count, block), 0)
        for b in range(k):
            total = tally[b * fold:b * fold + high_count] + tally[b * fold + high_count:(b + 1) * fold]
            total = take(total, b * LOW + spot % LOW)
            for part in range(code_count // block):
                mine = level == part * (block // LOW) + spot // LOW
                store(b, part, jnp.sum(jnp.where(mine, total, 0.0), axis=0, keepdims=True))
        tally[...] = jnp.zeros_like(tally)

    tally[...] = jnp.zeros_like(tally)
    mass_all[z] = jnp.zeros(mass_all.shape[1:], F32)
    counts = (c == 0) & (z < final)

    def row_sums(error):
        return lax.dot_general(
            jnp.ones((8, span), F32), error * error, (((1,), (1,)), ((), ())),
            precision=lax.Precision.HIGHEST, preferred_element_type=F32,
        )

    def up_copy(row, col):
        return remote(loss_up.at[row], loss_in.at[z], up_send.at[row], up_recv.at[z], row, col)

    def part_copy(row):
        return remote(mass_sent, mass_own.at[slot], part_send, part_recv.at[slot], row, owner)

    def part_remote(row):
        return counts & ((row != z) | (owner != 0))

    @pl.when(counts)
    def _():
        def own_part(q, _):
            g = group(q)

            @pl.when(owner != 0)
            def _():
                with scope("wait_part"):
                    arrived(err_block.at[q], core_recv.at[q])

            @pl.when(g >= z)
            def _():
                with scope("wait_code"):
                    @pl.when(((g != z) | (owner != 0)) & (q % PIECES == 0))
                    def _():
                        arrived(codes_in.at[g], code_recv.at[g])

                shift = 0 if window == pairs else lax.rem(slot * pairs, window)

                def code_at(b, at):
                    low = b * (block // 2)
                    tile = low // block * block
                    source = codes_in[g, pl.ds(q % PIECES * piece + at.start, chunk), tile:tile + block]
                    return take(source, shift + low - tile + lane[:chunk] // 2)

                count(err_block.at[q], code_at)

            @pl.when((g > z) & (q % PIECES == PIECES - 1))
            def _():
                error = jnp.concatenate([err_block[q - PIECES + 1 + h] for h in range(PIECES)], axis=0)
                loss_up[g, :, :rows] = row_sums(error)
                for col in range(nc):
                    up_copy(g, col).start()

            return 0

        lax.fori_loop(0, steps, own_part, 0)

        def store(b, part, value):
            mass_sent[b:b + 1, part * block:(part + 1) * block] = value

        spread(store)

        @pl.when(owner == 0)
        def _():
            mass_own[slot] = mass_sent[...]

    for row in range(nr):
        @pl.when(part_remote(row))
        def _():
            part_copy(row).start()

    def own_spread(j):
        def store(b, part, value):
            mass_all[z, j * k + b:j * k + b + 1, part * block:(part + 1) * block] = value

        spread(store)

    for j in range(m):
        @pl.when((c * m + j > z) & ((c * m + j < final) | (z == 0)))
        def _():
            for h in range(PIECES):
                with scope("wait_down"):
                    arrived(err_own.at[j, h * piece:(h + 1) * piece], own_recv.at[j, h])
                count(
                    err_own.at[j, h * piece:(h + 1) * piece],
                    lambda b, at: codes[j * k + b, pl.ds(h * piece + at.start, chunk), :],
                )
            own_spread(j)

        if j == 0:
            @pl.when(is_last & (z == 0))
            def _():
                send_up()

    @pl.when(is_last & (z > 0))
    def _():
        j = m - 1

        @pl.when(z == 1)
        def _():
            for h in range(PIECES):
                last_in[0, h, 1] = joined(PIECES + h)

        for h in range(PIECES):
            err_own[j, h * piece:(h + 1) * piece] = solved(0, h)
            count(
                err_own.at[j, h * piece:(h + 1) * piece],
                lambda b, at: codes[j * k + b, pl.ds(h * piece + at.start, chunk), :],
            )
        own_spread(j)

    def mass_copy(row):
        return remote(mass_all.at[z], mass_all.at[z], mass_send, mass_recv, row, c)

    def loss_copy(col):
        return remote(loss_all.at[c], loss_all.at[c], loss_send, loss_recv, z, col)

    for row in range(nr):
        @pl.when(row != z)
        def _():
            mass_copy(row).start()

    loss_all[c] = jnp.zeros(loss_all.shape[1:], F32)
    for j in range(m):
        @pl.when((c * m + j >= z) & ((c * m + j < final) | is_last))
        def _():
            loss_all[c, :, :rows] = loss_all[c, :, :rows] + row_sums(err_own[j])

    for col in range(nc):
        @pl.when(col != c)
        def _():
            loss_copy(col).start()

    for j in range(m):
        @pl.when(c * m + j < z)
        def _():
            arrived(delta.at[j], d_send.at[j])

        @pl.when(code_sent(j))
        def _():
            code_copy(j).wait_send()

        @pl.when((c * m + j > z) & (c * m + j < final))
        def _():
            arrived(run_out.at[:, j], run_send.at[j])

    if k > 1:
        @pl.when((z == final) & is_last)
        def _():
            arrived(u_raw.at[:, :(nr - 2) * block * (k - 1) // 2], tri_send)

    @pl.when(is_last & (z == 0))
    def _():
        arrived(last_out, last_send)

    @pl.when(is_last & (z == 1))
    def _():
        arrived(last_out.at[:steps - 2 * PIECES], last_send)
        arrived(err_zero, zero_send)

    @pl.when(is_last & (z > 1) & (z < final))
    def _():
        arrived(last_out.at[:steps - PIECES], last_send)

    for col in range(nc):
        @pl.when(is_owner & ((col > c) | ((col == 0) & (c > 0))))
        def _():
            arrived(err_block, core_send.at[col])

    @pl.when((is_owner | is_last) & (z < final))
    def _():
        def drain(q, _):
            g = group(q)
            early = early_up(g)

            @pl.when((is_owner & ((g < z) | ((g > z) & early))) | (is_last & (g > z) & jnp.logical_not(early)))
            def _():
                own_copy(q).wait_send()

            return 0

        with scope("drain"):
            lax.fori_loop(0, steps, drain, 0)

    part_size = mass_all.at[:, :k]

    @pl.when(counts)
    def _():
        for row in range(nr):
            @pl.when(row > z)
            def _():
                arrived(loss_all, up_send.at[row])

        @pl.when(owner == 0)
        def _():
            arrived(part_size.at[:nr - 1], part_send)

        @pl.when(owner != 0)
        def _():
            arrived(part_size, part_send)

    arrived(mass_all.at[:nr - 1], mass_send)
    arrived(loss_all.at[:nc - 1], loss_send)

    for j in reversed(range(m)):
        @pl.when(c * m + j < z)
        def _():
            with scope("wait_up"):
                for h in range(PIECES):
                    arrived(err_own.at[j, h * piece:(h + 1) * piece], own_recv.at[j, h])

        errors_out[:, j * span:(j + 1) * span] = err_own[j]

    with scope("wait_loss"):
        arrived(loss_all.at[:nc - 1], loss_recv)
    loss_sum = loss_all[0, 0:1, :rows]
    for col in range(1, nc):
        loss_sum = loss_sum + loss_all[col, 0:1, :rows]
    loss_out[...] = loss_sum
    for row in range(final):
        @pl.when(row < z)
        def _():
            with scope("wait_loss_up"):
                arrived(loss_in.at[row], up_recv.at[row])
            loss_out[...] = loss_out[...] + loss_in[row, 0:1, :rows]

    for j in range(m):
        @pl.when((c * m + j < final) & ((c * m + j != z) | (c != 0)))
        def _():
            with scope("wait_mass_part"):
                arrived(mass_own.at[j], part_recv.at[j])

    with scope("wait_mass"):
        arrived(mass_all.at[:nr - 1], mass_recv)
    mass_sum = mass_all[0]
    for row in range(1, nr):
        mass_sum = mass_sum + mass_all[row]
    mass_out[...] = mass_sum
    for j in range(m):
        @pl.when(c * m + j < final)
        def _():
            mass_out[j * k:(j + 1) * k, :] = mass_out[j * k:(j + 1) * k, :] + mass_own[j]


def store(errors, loss, mass, errors_out, loss_out, mass_out, sems):
    copies = [
        pltpu.make_async_copy(source, target, sems.at[number])
        for number, (source, target) in enumerate(((errors, errors_out), (loss, loss_out), (mass, mass_out)))
    ]
    for copy in copies:
        copy.start()
    for copy in copies:
        copy.wait()


def local(nr, nc, weights, codebook, assign, chol_upper, inv_blocks):
    rows, width = weights.shape[1:]
    span = chol_upper.shape[1]
    m = width // span
    steps, piece = nr * PIECES, rows // PIECES
    blocks, code_count = codebook.shape[1], codebook.shape[3]
    block = inv_blocks.shape[2]
    k = span // block
    dma = pltpu.SemaphoreType.DMA
    vmem = pl.BlockSpec(memory_space=pltpu.VMEM)
    hbm = pl.BlockSpec(memory_space=pltpu.HBM)
    shapes = ((rows, width), (1, rows), (blocks, code_count))
    results = pl.pallas_call(
        functools.partial(kernel, nr, nc),
        out_shape=tuple(pltpu.VMEM(shape, F32) for shape in shapes),
        in_specs=[hbm] * 5,
        out_specs=(vmem, vmem, vmem),
        scratch_shapes=[
            pltpu.VMEM(weights.shape[1:], F32),
            pltpu.VMEM(codebook.shape[1:], F32),
            pltpu.VMEM(assign.shape[1:], jnp.int32),
            pltpu.VMEM(inv_blocks.shape[1:], F32),
            pltpu.VMEM((span, width), F32),
            pltpu.VMEM((span, width), BF16),
            pltpu.VMEM((span, width), BF16),
            pltpu.VMEM((span, span), F32),
            pltpu.VMEM((span, span), F32),
            pltpu.VMEM((span, span), BF16),
            pltpu.VMEM((span, span), BF16),
            pltpu.VMEM((span, span), BF16),
            pltpu.VMEM((span, span), BF16),
            pltpu.VMEM((m, rows, span), F32),
            pltpu.VMEM((blocks, rows, block), jnp.int32),
            pltpu.VMEM((nr, rows, span), F32),
            pltpu.VMEM((nr, rows, max(span // 2, block)), jnp.int32),
            pltpu.VMEM((steps, m, piece, span), F32),
            pltpu.VMEM((steps, m, piece, span), F32),
            pltpu.VMEM((2, PIECES, nr, piece, span), F32),
            pltpu.VMEM((steps, piece, span), F32),
            pltpu.VMEM((steps, piece, span), F32),
            pltpu.VMEM((steps, piece, span), F32),
            pltpu.VMEM((m, rows, span), F32),
            pltpu.VMEM((PIECES, piece, span), F32),
            pltpu.VMEM((k * 2 * (code_count // LOW), block), F32),
            pltpu.VMEM((nr, blocks, code_count), F32),
            pltpu.VMEM((m, k, code_count), F32),
            pltpu.VMEM((k, code_count), F32),
            pltpu.VMEM((nc, 8, max(rows, 128)), F32),
            pltpu.VMEM((nr, 8, max(rows, 128)), F32),
            pltpu.VMEM((nr, 8, max(rows, 128)), F32),
            dma((4 + m,)),
            dma((m,)), dma((nr, PIECES)),
            dma((m,)), dma((nr,)),
            dma, dma,
            dma((m,)), dma((steps, m)),
            dma, dma((2, PIECES)), dma((steps,)),
            dma((nc,)), dma((steps,)),
            dma((steps,)), dma((m, PIECES)), dma,
            dma, dma((m,)),
            dma, dma,
            dma, dma,
            dma((nr,)), dma((nr,)), pltpu.SemaphoreType.REGULAR,
        ],
        compiler_params=pltpu.CompilerParams(
            collective_id=0, has_side_effects=True, vmem_limit_bytes=40 * 1024 * 1024
        ),
    )(*(pltpu.with_memory_space_constraint(value[0], pltpu.HBM) for value in (
        weights, codebook, assign, inv_blocks, chol_upper,
    )))
    errors, loss, mass = pl.pallas_call(
        store,
        out_shape=tuple(jax.ShapeDtypeStruct(shape, F32) for shape in shapes),
        in_specs=[vmem] * 3,
        out_specs=[hbm] * 3,
        scratch_shapes=[dma((3,))],
        compiler_params=pltpu.CompilerParams(vmem_limit_bytes=1024 * 1024),
    )(*results)
    return errors[None], loss, mass[None]


def solution(mesh):
    return jax.shard_map(
        functools.partial(local, mesh.shape["row"], mesh.shape["col"]),
        mesh=mesh,
        in_specs=(
            P("ea", "row", "col"),
            P("ea", "col", None, None),
            P("ea", "row", "col"),
            P("ea", "row", "col"),
            P("ea", "col", None, None),
        ),
        out_specs=(P("ea", "row", "col"), P("ea", "row"), P("ea", "col", None)),
        check_vma=False,
    )
```

```python
import functools

import jax
import jax.numpy as jnp
from jax import lax
from jax.experimental import pallas as pl
from jax.experimental.pallas import tpu as pltpu
from jax.sharding import PartitionSpec as P

F32 = jnp.float32
BF16 = jnp.bfloat16
LOW = 16
PIECES = 2
scope = jax.named_scope


def halves(value):
    high = value.astype(BF16)
    return high, (value - high.astype(F32)).astype(BF16)


def dot(a, b):
    return jnp.dot(a, b, preferred_element_type=F32)


def dot3(a, b_high, b_low):
    rows = a.shape[0]
    high, low = halves(a)
    both = dot(jnp.concatenate([high, low], axis=0), b_high)
    return both[:rows] + both[rows:] + dot(high, b_low)


def dot_full(a, b):
    b_high, b_low = halves(b)
    return dot3(a, b_high, b_low)


def take(table, index):
    return jnp.take_along_axis(table, index, axis=1, mode="promise_in_bounds")


def kernel(
    nr, nc,
    weights_hbm, codebook_hbm, assign_hbm, inverse_hbm, factor,
    errors_out, loss_out, mass_out,
    weights, codebook, assign, inverse, u_raw, u_high, u_low, triangle, v_full, v_high, v_low, w_high, w_low,
    delta, codes, delta_in, codes_in, run_in, run_out, last_in, last_out,
    err_block, err_own, err_zero, tally, mass_all, mass_own, mass_sent, loss_all, loss_up, loss_in,
    u_sem, d_send, code_send, code_recv, tri_send, tri_recv, run_send, run_recv, last_send, last_recv,
    core_send, core_recv, own_send, own_recv, zero_send, part_send, part_recv, mass_send, mass_recv,
    loss_send, loss_recv, up_send, up_recv, ready,
):
    z = lax.axis_index("row")
    c = lax.axis_index("col")
    rows, width = weights.shape
    span = factor.shape[0]
    m = width // span
    block = inverse.shape[1]
    k = span // block
    code_count = codebook.shape[2]
    owner = z // m
    slot = z % m
    steps = nr * PIECES
    piece = rows // PIECES
    final = nr - 1
    pairs = span // 2
    window = max(pairs, block)
    is_owner = (c == owner) & (z < final)
    is_last = c == nc - 1

    def remote(src, dst, send, recv, row, col):
        return pltpu.make_async_remote_copy(
            src_ref=src, dst_ref=dst, send_sem=send, recv_sem=recv,
            device_id={"row": row, "col": col}, device_id_type=pl.DeviceIdType.MESH,
        )

    def arrived(ref, sem):
        pltpu.make_async_copy(ref, ref, sem).wait()

    loads = [
        pltpu.make_async_copy(source, target, u_sem.at[number])
        for number, (source, target) in enumerate((
            (assign_hbm, assign), (codebook_hbm, codebook), (weights_hbm, weights),
            (inverse_hbm, inverse),
        ))
    ]
    loads += [
        pltpu.make_async_copy(
            factor.at[:, j * span:(j + 1) * span], u_raw.at[:, j * span:(j + 1) * span], u_sem.at[4 + j]
        )
        for j in range(m)
    ]
    for load in loads:
        load.start()

    barrier = pltpu.get_barrier_semaphore()
    for step in range(1, nr * nc):
        other = lax.rem(z * nc + c + step, nr * nc)

        @pl.when(z <= other // nc + 1)
        def _():
            pl.semaphore_signal(
                barrier, inc=1, device_id={"row": other // nc, "col": other % nc},
                device_id_type=pl.DeviceIdType.MESH,
            )

    def enter():
        with scope("entry"):
            pl.semaphore_wait(barrier, (jnp.minimum(z + 1, nr - 1) + 1) * nc - 1)

    def wait_ready():
        with scope("wait_ready"):
            pl.semaphore_wait(ready, (nr - 2 - z) * nc)

    def order(place):
        if nr < 3:
            return place
        return jnp.where(place == nr - 2, nr - 1, jnp.where(place == nr - 1, nr - 2, place))

    def group(q):
        return order(q // PIECES)

    def early_up(g):
        return (z > 0) & (owner < nc - 1) & (g == nr - 1)

    def farthest(i):
        return order(nr - 1 - i // PIECES) * PIECES + i % PIECES

    def zero_order(i):
        turn = i // PIECES
        return farthest(jnp.where(turn == nr - 2, i + PIECES, jnp.where(turn == nr - 1, i - PIECES, i)))

    def nearest(i):
        return order(i // PIECES) * PIECES + i % PIECES

    def part_rows(q):
        return pl.ds(pl.multiple_of(q % PIECES * piece, piece), piece)

    def delta_copy(j, h):
        at = slice(h * piece, (h + 1) * piece)
        return remote(delta.at[j, at], delta_in.at[z, at], d_send.at[j], core_recv.at[z * PIECES + h], c * m + j, c)

    def send_delta(j, when):
        @pl.when((c * m + j < z) & when)
        def _():
            for h in range(PIECES):
                delta_copy(j, h).start()

    def urgent(j):
        return (c * m + j == 0) & (z != nr - 2)

    def code_copy(j):
        low = j * pairs // window * window
        return remote(
            assign.at[:, low:low + window], codes_in.at[z], code_send.at[j], code_recv, c * m + j, 0
        )

    def code_sent(j):
        return (c * m + j <= z) & (c * m + j < final) & ((c > 0) | (c * m + j < z))

    def tri_copy(row, i):
        low = (m - 1) * span
        return remote(
            u_raw.at[i * block:(i + 1) * block, low + (i + 1) * block:low + span],
            triangle.at[i * block:(i + 1) * block, (i + 1) * block:span],
            tri_send, tri_recv, row, c,
        )

    def run_copy(q, j):
        return remote(run_out.at[q, j], run_in.at[q, j], run_send.at[j], run_recv.at[q, j], z + 1, c)

    def first(g):
        return jnp.where(g == 0, 1, 0)

    def solver(g):
        return jnp.maximum(g, 1)

    def last_copy(q):
        which, h = first(group(q)), q % PIECES
        return remote(last_out.at[q], last_in.at[which, h, z], last_send, last_recv.at[which, h], solver(group(q)), c)

    def zero_sum(q):
        return remote(last_out.at[q], run_in.at[q, m - 1], last_send, run_recv.at[q, m - 1], 1, c)

    def zero_copy(h):
        return remote(
            err_zero.at[h], err_own.at[m - 1, h * piece:(h + 1) * piece],
            zero_send, own_recv.at[m - 1, h], 0, c,
        )

    def core_copy(q, col):
        return remote(err_block.at[q], err_block.at[q], core_send.at[col], core_recv.at[q], z, col)

    def own_copy(q):
        return remote(
            err_block.at[q], err_own.at[slot, part_rows(q)],
            own_send, own_recv.at[slot, q % PIECES], group(q), owner,
        )

    with scope("first_loads"):
        for load in loads[:3]:
            load.wait()

    lane = lax.broadcasted_iota(jnp.int32, (rows, block), 1)

    def subtract(j):
        for b in range(j * k, (j + 1) * k):
            low = b * (block // 2)
            tile = low // block * block
            code = take(assign[:, tile:tile + block], low - tile + lane // 2)
            codes[b] = code
            inner = code % block
            value = jnp.zeros((rows, block), F32)
            for part in range(code_count // block):
                picked = []
                for comp in range(2):
                    table = codebook[b, comp:comp + 1, part * block:(part + 1) * block]
                    picked.append(take(jnp.broadcast_to(table, (rows, block)), inner))
                both = jnp.where(lane % 2 == 0, picked[0], picked[1])
                value = jnp.where(code // block == part, both, value)
            at = (b - j * k) * block
            delta[j, :, at:at + block] = weights[:, b * block:(b + 1) * block] - value

    subtract(0)

    @pl.when(z > 0)
    def _():
        enter()

    send_delta(0, urgent(0))

    for row in range(nr - 2):
        for col in range(nc):
            @pl.when(row + 1 < z)
            def _():
                pl.semaphore_signal(
                    ready, inc=1, device_id={"row": row, "col": col}, device_id_type=pl.DeviceIdType.MESH,
                )

    def rest():
        for j in range(1, m):
            subtract(j)

    def inverted(first, right):
        v_full[...] = jnp.zeros_like(v_full)

        def invert(lo, hi):
            if hi - lo == 1:
                v_full[lo * block:hi * block, lo * block:hi * block] = inverse[first + lo]
                return
            mid = (lo + hi) // 2
            invert(lo, mid)
            invert(mid, hi)
            top, middle, end = lo * block, mid * block, hi * block
            product = dot_full(v_full[top:middle, top:middle], right(top, middle, end))
            v_full[top:middle, middle:end] = -dot_full(product, v_full[middle:end, middle:end])

        invert(0, k)
        return halves(v_full[...])

    @pl.when(is_owner)
    def _():
        with scope("factor_loads"):
            loads[3].wait()
            for j in range(m):
                @pl.when(slot == j)
                def _():
                    loads[4 + j].wait()
        rest()
        base = slot * span
        high, low = inverted(slot * k, lambda top, middle, end: u_raw[
            top:middle, pl.ds(pl.multiple_of(base + middle, block), end - middle)
        ])
        v_high[...] = high
        v_low[...] = low

    @pl.when(jnp.logical_not(is_owner))
    def _():
        loads[3].wait()
        for j in range(m):
            loads[4 + j].wait()

        @pl.when((z == final) & is_last)
        def _():
            for row in reversed(range(1, final)):
                for i in range(k - 1):
                    tri_copy(row, i).start()

        rest()

    for j in range(m):
        @pl.when(is_owner & (slot != j))
        def _():
            loads[4 + j].wait()

    for j in range(m):
        @pl.when(c * m + j > z)
        def _():
            high, low = halves(u_raw[:, j * span:(j + 1) * span])
            u_high[:, j * span:(j + 1) * span] = high
            u_low[:, j * span:(j + 1) * span] = low

    def invert_last():
        @pl.when(z == final)
        def _():
            triangle[...] = u_raw[:, (m - 1) * span:]

        @pl.when(z < final)
        def _():
            with scope("wait_triangle"):
                if k > 1:
                    arrived(triangle.at[:block * (k - 1), :block * k // 2], tri_recv)

        high, low = inverted((m - 1) * k, lambda top, middle, end: triangle[top:middle, middle:end])
        w_high[...] = high
        w_low[...] = low

    @pl.when(z == 0)
    def _():
        enter()

    for j in range(m):
        send_delta(j, jnp.logical_not(urgent(j)))

    for j in range(m):
        @pl.when(code_sent(j))
        def _():
            code_copy(j).start()

        @pl.when((c == 0) & (z == j) & (z < final))
        def _():
            low = j * pairs // window * window
            codes_in[z] = assign[:, low:low + window]

    late_core = (z == 0) & (c > owner)
    relay_core = (z > 0) & (z < final) & (c > owner)

    def forward(q, j):
        with scope("wait_far_sum"):
            arrived(run_in.at[q, j], run_recv.at[q, j])
        run_out[q, j] = run_out[q, j] + run_in[q, j]
        run_copy(q, j).start()

    def stage(q, _):
        g = group(q)
        at = part_rows(q)

        turn = jnp.where(z == final, 0, PIECES)

        @pl.when(is_last & (z >= final - 1) & (q == turn))
        def _():
            invert_last()

        @pl.when((z > 0) & (z < nr - 2) & (q == (z + 1) * PIECES))
        def _():
            wait_ready()

        @pl.when(is_owner)
        def _():
            @pl.when(z == 0)
            def _():
                run_in[q, slot] = jnp.zeros((piece, span), F32)

            @pl.when(z > 0)
            def _():
                with scope("wait_own_sum"):
                    arrived(run_in.at[q, slot], run_recv.at[q, slot])

            @pl.when(g > z)
            def _():
                with scope("wait_delta"):
                    arrived(delta_in.at[g, at], core_recv.at[g * PIECES + q % PIECES])

                run_in[q, slot] = run_in[q, slot] + delta_in[g, at]

            @pl.when(g == z)
            def _():
                run_in[q, slot] = run_in[q, slot] + delta[slot, at]

            error = dot3(run_in[q, slot], v_high[...], v_low[...])
            err_block[q] = error

            @pl.when(g == z)
            def _():
                err_own[slot, at] = error

            for col in range(nc):
                @pl.when((col > c) | ((col == 0) & (c > 0)))
                def _():
                    core_copy(q, col).start()

            @pl.when((g < z) | ((g > z) & early_up(g)))
            def _():
                own_copy(q).start()

        @pl.when((c > owner) & (z < final))
        def _():
            with scope("wait_core"):
                arrived(err_block.at[q], core_recv.at[q])

        late = late_core & (q >= 2 * PIECES)
        @pl.when(is_last & (z < final))
        def _():
            j = m - 1
            change = dot3(
                err_block[q], u_high[:, j * span:(j + 1) * span], u_low[:, j * span:(j + 1) * span]
            )
            change = change - jnp.where((g == 0) & (z == 0), delta[j, at], 0.0)

            @pl.when((z <= 1) | (solver(g) != z))
            def _():
                last_out[q] = change

            @pl.when((z > 1) & (solver(g) == z))
            def _():
                last_in[first(g), q % PIECES, z] = change

            @pl.when((z > 1) & (solver(g) != z))
            def _():
                last_copy(q).start()

        for j in range(m):
            target = c * m + j

            @pl.when((target > z) & (target < final))
            def _():
                change = dot3(
                    err_block[q], u_high[:, j * span:(j + 1) * span], u_low[:, j * span:(j + 1) * span]
                )
                run_out[q, j] = jnp.where(g == z, delta[j, at], 0.0) - change

                @pl.when((z > 0) & jnp.logical_not(relay_core))
                def _():
                    with scope("wait_near_sum"):
                        arrived(run_in.at[q, j], run_recv.at[q, j])
                    run_out[q, j] = run_out[q, j] + run_in[q, j]

                @pl.when(jnp.logical_not(late | relay_core))
                def _():
                    run_copy(q, j).start()

                @pl.when(relay_core & (q >= PIECES))
                def _():
                    forward(q - PIECES, j)

        return 0

    lax.fori_loop(0, steps, stage, 0)

    @pl.when((z == 0) & (nr > 2))
    def _():
        wait_ready()

    for j in range(m):
        @pl.when(late_core & (c * m + j < final))
        def _():
            def release(q, _):
                run_copy(q, j).start()
                return 0

            lax.fori_loop(2 * PIECES, steps, release, 0)

        @pl.when(relay_core & (c * m + j < final))
        def _():
            def release(q, _):
                forward(q, j)
                return 0

            lax.fori_loop(steps - PIECES, steps, release, 0)

    @pl.when(late_core & is_last)
    def _():
        def release(i, _):
            zero_sum(zero_order(i)).start()
            return 0

        lax.fori_loop(0, steps, release, 0)

    def joined(q):
        with scope("wait_zero"):
            arrived(run_in.at[q, m - 1], run_recv.at[q, m - 1])
        return last_out[q] + run_in[q, m - 1]

    @pl.when(is_last & (z > 0) & (z < final - 1))
    def _():
        invert_last()

    @pl.when(is_last & (z == 1) & (z < final))
    def _():
        def relayed(i, _):
            q = farthest(i)
            last_out[q] = joined(q)
            last_copy(q).start()
            return 0

        lax.fori_loop(0, steps - 2 * PIECES, relayed, 0)

    def send_up():
        def upward(i, _):
            q = nearest(i)

            @pl.when((group(q) > z) & jnp.logical_not(early_up(group(q))))
            def _():
                own_copy(q).start()

            return 0

        lax.fori_loop(0, steps, upward, 0)

    @pl.when(is_last & (z == 0))
    def _():
        with scope("wait_left"):
            arrived(last_out, last_send)

    @pl.when(is_last & (z < final))
    def _():
        send_up()

    def solved(which, h):
        with scope("wait_last"):
            if nr > 3:
                @pl.when(z < final)
                def _():
                    arrived(last_in.at[which, h, :nr - 3], last_recv.at[which, h])

            @pl.when(z == final)
            def _():
                arrived(last_in.at[which, h, :nr - 2], last_recv.at[which, h])
        total = -last_in[which, h, 1]
        for row in range(2, final):
            total = total - last_in[which, h, row]
        if which == 0:
            total = total + delta[m - 1, h * piece:(h + 1) * piece]
        return dot3(total, w_high[...], w_low[...])

    @pl.when(is_last & (z == 1))
    def _():
        for h in range(PIECES):
            last_in[1, h, 1] = joined(h)
            err_zero[h] = solved(1, h)
            zero_copy(h).start()
    high_count = code_count // LOW
    fold = 2 * high_count
    chunk = 16
    half = chunk // 2

    def count(error_at, code_at):
        def gather(step, total):
            at = pl.ds(pl.multiple_of(step * chunk, chunk), chunk)
            iota_high = lax.broadcasted_iota(jnp.int32, (high_count, block), 0)
            iota_low = lax.broadcasted_iota(jnp.int32, (LOW, block), 0)
            left, right = [], []
            even = lax.broadcasted_iota(jnp.int32, (half, block), 1) % 2 == 0
            for b in range(k):
                code = code_at(b, at)
                code = jnp.where(even, code[:half], code[half:])
                value = error_at[at, b * block:(b + 1) * block]
                value = value * value
                upper, lower = value[:half], value[half:]
                value = jnp.where(even, upper + pltpu.roll(upper, block - 1, 1), lower + pltpu.roll(lower, 1, 1))
                coarse = value.astype(BF16).astype(F32)
                fine = value - coarse
                code_high, code_low = code // LOW, code % LOW
                top, bottom, marks = [], [], []
                for r in range(half):
                    hit = jnp.broadcast_to(code_high[r:r + 1], (high_count, block)) == iota_high
                    top.append(jnp.where(hit, jnp.broadcast_to(coarse[r:r + 1], (high_count, block)), 0.0).astype(BF16))
                    bottom.append(jnp.where(hit, jnp.broadcast_to(fine[r:r + 1], (high_count, block)), 0.0).astype(BF16))
                    low_hit = jnp.broadcast_to(code_low[r:r + 1], (LOW, block)) == iota_low
                    marks.append(jnp.where(low_hit, 1.0, 0.0).astype(BF16))
                left += [jnp.concatenate(top, axis=1), jnp.concatenate(bottom, axis=1)]
                right.append(jnp.concatenate(marks, axis=1))
            return total + lax.dot_general(
                jnp.concatenate(left, axis=0), jnp.concatenate(right, axis=0),
                (((1,), (1,)), ((), ())), preferred_element_type=F32,
            )

        total = lax.fori_loop(0, piece // chunk, gather, jnp.zeros((k * fold, k * LOW), F32), unroll=2)
        tally[:, :k * LOW] = tally[:, :k * LOW] + total

    def spread(store):
        spot = lax.broadcasted_iota(jnp.int32, (high_count, block), 1)
        level = lax.broadcasted_iota(jnp.int32, (high_count, block), 0)
        for b in range(k):
            total = tally[b * fold:b * fold + high_count] + tally[b * fold + high_count:(b + 1) * fold]
            total = take(total, b * LOW + spot % LOW)
            for part in range(code_count // block):
                mine = level == part * (block // LOW) + spot // LOW
                store(b, part, jnp.sum(jnp.where(mine, total, 0.0), axis=0, keepdims=True))
        tally[...] = jnp.zeros_like(tally)

    tally[...] = jnp.zeros_like(tally)
    mass_all[z] = jnp.zeros(mass_all.shape[1:], F32)
    counts = (c == 0) & (z < final)

    def row_sums(error):
        return lax.dot_general(
            jnp.ones((8, span), F32), error * error, (((1,), (1,)), ((), ())),
            precision=lax.Precision.HIGHEST, preferred_element_type=F32,
        )

    def up_copy(row, col):
        return remote(loss_up.at[row], loss_in.at[z], up_send, up_recv, row, col)

    def part_copy(row):
        return remote(mass_sent, mass_own.at[slot], part_send, part_recv.at[slot], row, owner)

    def part_remote(row):
        return counts & ((row != z) | (owner != 0))

    for row in range(final):
        for other in range(2):
            number = final - row + other

            @pl.when(counts & (z == row) & ((owner != 0) == (other == 1)))
            def _():
                with scope("wait_code"):
                    arrived(codes_in.at[:number], code_recv)

    @pl.when(counts)
    def _():
        def own_part(q, _):
            g = group(q)

            @pl.when(owner != 0)
            def _():
                with scope("wait_part"):
                    arrived(err_block.at[q], core_recv.at[q])

            @pl.when(g >= z)
            def _():
                shift = 0 if window == pairs else lax.rem(slot * pairs, window)

                def code_at(b, at):
                    low = b * (block // 2)
                    tile = low // block * block
                    source = codes_in[g, pl.ds(q % PIECES * piece + at.start, chunk), tile:tile + block]
                    return take(source, shift + low - tile + lane[:chunk] // 2)

                count(err_block.at[q], code_at)

            @pl.when((g > z) & (q % PIECES == PIECES - 1))
            def _():
                error = jnp.concatenate([err_block[q - PIECES + 1 + h] for h in range(PIECES)], axis=0)
                loss_up[g, :, :rows] = row_sums(error)
                for col in range(nc):
                    up_copy(g, col).start()

            return 0

        lax.fori_loop(0, steps, own_part, 0)

        def store(b, part, value):
            mass_sent[b:b + 1, part * block:(part + 1) * block] = value

        spread(store)

        @pl.when(owner == 0)
        def _():
            mass_own[slot] = mass_sent[...]

    for row in range(nr):
        @pl.when(part_remote(row))
        def _():
            part_copy(row).start()

    def own_spread(j):
        def store(b, part, value):
            mass_all[z, j * k + b:j * k + b + 1, part * block:(part + 1) * block] = value

        spread(store)

    for j in range(m):
        @pl.when((c * m + j > z) & ((c * m + j < final) | (z == 0)))
        def _():
            for h in range(PIECES):
                with scope("wait_down"):
                    arrived(err_own.at[j, h * piece:(h + 1) * piece], own_recv.at[j, h])
                count(
                    err_own.at[j, h * piece:(h + 1) * piece],
                    lambda b, at: codes[j * k + b, pl.ds(h * piece + at.start, chunk), :],
                )
            own_spread(j)

    @pl.when(is_last & (z > 0))
    def _():
        j = m - 1

        @pl.when(z == 1)
        def _():
            for h in range(PIECES):
                last_in[0, h, 1] = joined(PIECES + h)

        for h in range(PIECES):
            err_own[j, h * piece:(h + 1) * piece] = solved(0, h)
            count(
                err_own.at[j, h * piece:(h + 1) * piece],
                lambda b, at: codes[j * k + b, pl.ds(h * piece + at.start, chunk), :],
            )
        own_spread(j)

    def mass_copy(row):
        return remote(mass_all.at[z], mass_all.at[z], mass_send, mass_recv, row, c)

    def loss_copy(col):
        return remote(loss_all.at[c], loss_all.at[c], loss_send, loss_recv, z, col)

    with scope("send_mass"):
        for row in range(nr):
            @pl.when(row != z)
            def _():
                mass_copy(row).start()

    loss_all[c] = jnp.zeros(loss_all.shape[1:], F32)
    for j in range(m):
        @pl.when((c * m + j >= z) & ((c * m + j < final) | is_last))
        def _():
            loss_all[c, :, :rows] = loss_all[c, :, :rows] + row_sums(err_own[j])

    for col in range(nc):
        @pl.when(col != c)
        def _():
            loss_copy(col).start()

    for j in range(m):
        @pl.when(c * m + j < z)
        def _():
            arrived(delta.at[j], d_send.at[j])

        @pl.when(code_sent(j))
        def _():
            code_copy(j).wait_send()

        @pl.when((c * m + j > z) & (c * m + j < final))
        def _():
            arrived(run_out.at[:, j], run_send.at[j])

    if k > 1:
        @pl.when((z == final) & is_last)
        def _():
            arrived(u_raw.at[:, :(nr - 2) * block * (k - 1) // 2], tri_send)

    @pl.when(is_last & (z == 1))
    def _():
        arrived(last_out.at[:steps - 2 * PIECES], last_send)
        arrived(err_zero, zero_send)

    @pl.when(is_last & (z > 1) & (z < final))
    def _():
        arrived(last_out.at[:steps - PIECES], last_send)

    for col in range(nc):
        @pl.when(is_owner & ((col > c) | ((col == 0) & (c > 0))))
        def _():
            arrived(err_block, core_send.at[col])

    for row in range(final):
        early = 1 if row > 0 and row // m < nc - 1 else 0
        up = final - row - early
        both = row // m == nc - 1

        @pl.when((z == row) & is_owner)
        def _():
            number = row + early + (up if both else 0)
            if number:
                arrived(err_block.at[:number * PIECES], own_send)

        if not both and up:
            @pl.when((z == row) & is_last)
            def _():
                arrived(err_block.at[:up * PIECES], own_send)

    part_size = mass_all.at[:, :k]

    @pl.when(counts)
    def _():
        for row in range(final):
            @pl.when(z == row)
            def _():
                arrived(loss_up.at[:(final - row) * nc], up_send)

        @pl.when(owner == 0)
        def _():
            arrived(part_size.at[:nr - 1], part_send)

        @pl.when(owner != 0)
        def _():
            arrived(part_size, part_send)

    arrived(mass_all.at[:nr - 1], mass_send)
    arrived(loss_all.at[:nc - 1], loss_send)

    for j in reversed(range(m)):
        @pl.when(c * m + j < z)
        def _():
            with scope("wait_up"):
                for h in range(PIECES):
                    arrived(err_own.at[j, h * piece:(h + 1) * piece], own_recv.at[j, h])

        errors_out[:, j * span:(j + 1) * span] = err_own[j]

    with scope("wait_loss"):
        arrived(loss_all.at[:nc - 1], loss_recv)
    loss_sum = loss_all[0, 0:1, :rows]
    for col in range(1, nc):
        loss_sum = loss_sum + loss_all[col, 0:1, :rows]
    loss_out[...] = loss_sum
    for row in range(1, nr):
        @pl.when(z == row)
        def _():
            with scope("wait_loss_up"):
                arrived(loss_in.at[:row], up_recv)
            total = loss_out[...]
            for lower in range(row):
                total = total + loss_in[lower, 0:1, :rows]
            loss_out[...] = total

    for j in range(m):
        @pl.when((c * m + j < final) & ((c * m + j != z) | (c != 0)))
        def _():
            with scope("wait_mass_part"):
                arrived(mass_own.at[j], part_recv.at[j])

    with scope("wait_mass"):
        arrived(mass_all.at[:nr - 1], mass_recv)
    mass_sum = mass_all[0]
    for row in range(1, nr):
        mass_sum = mass_sum + mass_all[row]
    mass_out[...] = mass_sum
    for j in range(m):
        @pl.when(c * m + j < final)
        def _():
            mass_out[j * k:(j + 1) * k, :] = mass_out[j * k:(j + 1) * k, :] + mass_own[j]


def store(errors, loss, mass, errors_out, loss_out, mass_out, sems):
    copies = [
        pltpu.make_async_copy(source, target, sems.at[number])
        for number, (source, target) in enumerate(((errors, errors_out), (loss, loss_out), (mass, mass_out)))
    ]
    for copy in copies:
        copy.start()
    for copy in copies:
        copy.wait()


def local(nr, nc, weights, codebook, assign, chol_upper, inv_blocks):
    rows, width = weights.shape[1:]
    span = chol_upper.shape[1]
    m = width // span
    steps, piece = nr * PIECES, rows // PIECES
    blocks, code_count = codebook.shape[1], codebook.shape[3]
    block = inv_blocks.shape[2]
    k = span // block
    dma = pltpu.SemaphoreType.DMA
    vmem = pl.BlockSpec(memory_space=pltpu.VMEM)
    hbm = pl.BlockSpec(memory_space=pltpu.HBM)
    shapes = ((rows, width), (1, rows), (blocks, code_count))
    results = pl.pallas_call(
        functools.partial(kernel, nr, nc),
        out_shape=tuple(pltpu.VMEM(shape, F32) for shape in shapes),
        in_specs=[hbm] * 5,
        out_specs=(vmem, vmem, vmem),
        scratch_shapes=[
            pltpu.VMEM(weights.shape[1:], F32),
            pltpu.VMEM(codebook.shape[1:], F32),
            pltpu.VMEM(assign.shape[1:], jnp.int32),
            pltpu.VMEM(inv_blocks.shape[1:], F32),
            pltpu.VMEM((span, width), F32),
            pltpu.VMEM((span, width), BF16),
            pltpu.VMEM((span, width), BF16),
            pltpu.VMEM((span, span), F32),
            pltpu.VMEM((span, span), F32),
            pltpu.VMEM((span, span), BF16),
            pltpu.VMEM((span, span), BF16),
            pltpu.VMEM((span, span), BF16),
            pltpu.VMEM((span, span), BF16),
            pltpu.VMEM((m, rows, span), F32),
            pltpu.VMEM((blocks, rows, block), jnp.int32),
            pltpu.VMEM((nr, rows, span), F32),
            pltpu.VMEM((nr, rows, max(span // 2, block)), jnp.int32),
            pltpu.VMEM((steps, m, piece, span), F32),
            pltpu.VMEM((steps, m, piece, span), F32),
            pltpu.VMEM((2, PIECES, nr, piece, span), F32),
            pltpu.VMEM((steps, piece, span), F32),
            pltpu.VMEM((steps, piece, span), F32),
            pltpu.VMEM((m, rows, span), F32),
            pltpu.VMEM((PIECES, piece, span), F32),
            pltpu.VMEM((k * 2 * (code_count // LOW), block), F32),
            pltpu.VMEM((nr, blocks, code_count), F32),
            pltpu.VMEM((m, k, code_count), F32),
            pltpu.VMEM((k, code_count), F32),
            pltpu.VMEM((nc, 8, max(rows, 128)), F32),
            pltpu.VMEM((nr * nc, 8, max(rows, 128)), F32),
            pltpu.VMEM((nr, 8, max(rows, 128)), F32),
            dma((4 + m,)),
            dma((m,)),
            dma((m,)), dma,
            dma, dma,
            dma((m,)), dma((steps, m)),
            dma, dma((2, PIECES)),
            dma((nc,)), dma((steps,)),
            dma, dma((m, PIECES)), dma,
            dma, dma((m,)),
            dma, dma,
            dma, dma,
            dma, dma, pltpu.SemaphoreType.REGULAR,
        ],
        compiler_params=pltpu.CompilerParams(
            collective_id=0, has_side_effects=True, vmem_limit_bytes=40 * 1024 * 1024
        ),
    )(*(pltpu.with_memory_space_constraint(value[0], pltpu.HBM) for value in (
        weights, codebook, assign, inv_blocks, chol_upper,
    )))
    errors, loss, mass = pl.pallas_call(
        store,
        out_shape=tuple(jax.ShapeDtypeStruct(shape, F32) for shape in shapes),
        in_specs=[vmem] * 3,
        out_specs=[hbm] * 3,
        scratch_shapes=[dma((3,))],
        compiler_params=pltpu.CompilerParams(vmem_limit_bytes=1024 * 1024),
    )(*results)
    return errors[None], loss, mass[None]


def solution(mesh):
    return jax.shard_map(
        functools.partial(local, mesh.shape["row"], mesh.shape["col"]),
        mesh=mesh,
        in_specs=(
            P("ea", "row", "col"),
            P("ea", "col", None, None),
            P("ea", "row", "col"),
            P("ea", "row", "col"),
            P("ea", "col", None, None),
        ),
        out_specs=(P("ea", "row", "col"), P("ea", "row"), P("ea", "col", None)),
        check_vma=False,
    )
```

```python
import functools

import jax
import jax.numpy as jnp
from jax import lax
from jax.experimental import pallas as pl
from jax.experimental.pallas import tpu as pltpu
from jax.sharding import PartitionSpec as P

F32 = jnp.float32
BF16 = jnp.bfloat16
LOW = 16
PIECES = 2
scope = jax.named_scope


def halves(value):
    high = value.astype(BF16)
    return high, (value - high.astype(F32)).astype(BF16)


def dot(a, b):
    return jnp.dot(a, b, preferred_element_type=F32)


def dot3(a, b_high, b_low):
    rows = a.shape[0]
    high, low = halves(a)
    both = dot(jnp.concatenate([high, low], axis=0), b_high)
    return both[:rows] + both[rows:] + dot(high, b_low)


def dot_full(a, b):
    b_high, b_low = halves(b)
    return dot3(a, b_high, b_low)


def take(table, index):
    return jnp.take_along_axis(table, index, axis=1, mode="promise_in_bounds")


def kernel(
    nr, nc,
    weights_hbm, codebook_hbm, assign_hbm, inverse_hbm, factor,
    errors_out, loss_out, mass_out,
    weights, codebook, assign, inverse, u_raw, u_high, u_low, triangle, v_full, v_high, v_low, w_high, w_low,
    delta, codes, delta_in, codes_in, run_in, run_out, last_in, last_out,
    err_block, err_own, err_zero, tally, mass_all, mass_own, mass_sent, loss_all, loss_up, loss_in,
    u_sem, d_send, code_send, code_recv, tri_send, tri_recv, run_send, run_recv, last_send, last_recv,
    core_send, core_recv, own_send, own_recv, zero_send, part_send, part_recv, mass_send, mass_recv,
    loss_send, loss_recv, up_send, up_recv, ready,
):
    z = lax.axis_index("row")
    c = lax.axis_index("col")
    rows, width = weights.shape
    span = factor.shape[0]
    m = width // span
    block = inverse.shape[1]
    k = span // block
    code_count = codebook.shape[2]
    owner = z // m
    slot = z % m
    steps = nr * PIECES
    piece = rows // PIECES
    final = nr - 1
    pairs = span // 2
    window = max(pairs, block)
    is_owner = (c == owner) & (z < final)
    is_last = c == nc - 1

    def remote(src, dst, send, recv, row, col):
        return pltpu.make_async_remote_copy(
            src_ref=src, dst_ref=dst, send_sem=send, recv_sem=recv,
            device_id={"row": row, "col": col}, device_id_type=pl.DeviceIdType.MESH,
        )

    def arrived(ref, sem):
        pltpu.make_async_copy(ref, ref, sem).wait()

    loads = [
        pltpu.make_async_copy(source, target, u_sem.at[number])
        for number, (source, target) in enumerate((
            (assign_hbm, assign), (codebook_hbm, codebook), (weights_hbm, weights),
            (inverse_hbm, inverse),
        ))
    ]
    loads += [
        pltpu.make_async_copy(
            factor.at[:, j * span:(j + 1) * span], u_raw.at[:, j * span:(j + 1) * span], u_sem.at[4 + j]
        )
        for j in range(m)
    ]
    for load in loads:
        load.start()

    barrier = pltpu.get_barrier_semaphore()
    for step in range(1, nr * nc):
        other = lax.rem(z * nc + c + nr * nc - step, nr * nc)

        @pl.when(z <= other // nc + 1)
        def _():
            pl.semaphore_signal(
                barrier, inc=1, device_id={"row": other // nc, "col": other % nc},
                device_id_type=pl.DeviceIdType.MESH,
            )

    def enter():
        with scope("entry"):
            pl.semaphore_wait(barrier, (jnp.minimum(z + 1, nr - 1) + 1) * nc - 1)

    def wait_ready():
        with scope("wait_ready"):
            pl.semaphore_wait(ready, (nr - 2 - z) * nc)

    def order(place):
        if nr < 3:
            return place
        return jnp.where(place == nr - 2, nr - 1, jnp.where(place == nr - 1, nr - 2, place))

    def group(q):
        return order(q // PIECES)

    def early_up(g):
        return (z > 0) & (owner < nc - 1) & (g == nr - 1)

    def farthest(i):
        return order(nr - 1 - i // PIECES) * PIECES + i % PIECES

    def zero_order(i):
        turn = i // PIECES
        return farthest(jnp.where(turn == nr - 2, i + PIECES, jnp.where(turn == nr - 1, i - PIECES, i)))

    def nearest(i):
        return order(i // PIECES) * PIECES + i % PIECES

    def part_rows(q):
        return pl.ds(pl.multiple_of(q % PIECES * piece, piece), piece)

    def delta_copy(j, h):
        at = slice(h * piece, (h + 1) * piece)
        return remote(delta.at[j, at], delta_in.at[z, at], d_send.at[j], core_recv.at[z * PIECES + h], c * m + j, c)

    def send_delta(j, when):
        @pl.when((c * m + j < z) & when)
        def _():
            for h in range(PIECES):
                delta_copy(j, h).start()

    def urgent(j):
        return (c * m + j == 0) & (z != nr - 2)

    def code_copy(j):
        low = j * pairs // window * window
        return remote(
            assign.at[:, low:low + window], codes_in.at[z], code_send.at[j], code_recv, c * m + j, 0
        )

    def code_sent(j):
        return (c * m + j <= z) & (c * m + j < final) & ((c > 0) | (c * m + j < z))

    def tri_copy(row, i):
        low = (m - 1) * span
        return remote(
            u_raw.at[i * block:(i + 1) * block, low + (i + 1) * block:low + span],
            triangle.at[i * block:(i + 1) * block, (i + 1) * block:span],
            tri_send, tri_recv, row, c,
        )

    def run_copy(q, j):
        return remote(run_out.at[q, j], run_in.at[q, j], run_send.at[j], run_recv.at[q, j], z + 1, c)

    def first(g):
        return jnp.where(g == 0, 1, 0)

    def solver(g):
        return jnp.maximum(g, 1)

    def last_copy(q):
        which, h = first(group(q)), q % PIECES
        return remote(last_out.at[q], last_in.at[which, h, z], last_send, last_recv.at[which, h], solver(group(q)), c)

    def zero_sum(q):
        return remote(last_out.at[q], run_in.at[q, m - 1], last_send, run_recv.at[q, m - 1], 1, c)

    def zero_copy(h):
        return remote(
            err_zero.at[h], err_own.at[m - 1, h * piece:(h + 1) * piece],
            zero_send, own_recv.at[m - 1, h], 0, c,
        )

    def core_copy(q, col):
        return remote(err_block.at[q], err_block.at[q], core_send.at[col], core_recv.at[q], z, col)

    def own_copy(q):
        return remote(
            err_block.at[q], err_own.at[slot, part_rows(q)],
            own_send, own_recv.at[slot, q % PIECES], group(q), owner,
        )

    with scope("first_loads"):
        for load in loads[:3]:
            load.wait()

    lane = lax.broadcasted_iota(jnp.int32, (rows, block), 1)

    def subtract(j):
        for b in range(j * k, (j + 1) * k):
            low = b * (block // 2)
            tile = low // block * block
            code = take(assign[:, tile:tile + block], low - tile + lane // 2)
            codes[b] = code
            inner = code % block
            value = jnp.zeros((rows, block), F32)
            for part in range(code_count // block):
                picked = []
                for comp in range(2):
                    table = codebook[b, comp:comp + 1, part * block:(part + 1) * block]
                    picked.append(take(jnp.broadcast_to(table, (rows, block)), inner))
                both = jnp.where(lane % 2 == 0, picked[0], picked[1])
                value = jnp.where(code // block == part, both, value)
            at = (b - j * k) * block
            delta[j, :, at:at + block] = weights[:, b * block:(b + 1) * block] - value

    subtract(0)

    @pl.when(z > 0)
    def _():
        enter()

    send_delta(0, urgent(0))

    for row in range(nr - 2):
        for col in range(nc):
            @pl.when(row + 1 < z)
            def _():
                pl.semaphore_signal(
                    ready, inc=1, device_id={"row": row, "col": col}, device_id_type=pl.DeviceIdType.MESH,
                )

    def rest():
        for j in range(1, m):
            subtract(j)

    def inverted(first, right):
        v_full[...] = jnp.zeros_like(v_full)

        def invert(lo, hi):
            if hi - lo == 1:
                v_full[lo * block:hi * block, lo * block:hi * block] = inverse[first + lo]
                return
            mid = (lo + hi) // 2
            invert(lo, mid)
            invert(mid, hi)
            top, middle, end = lo * block, mid * block, hi * block
            product = dot_full(v_full[top:middle, top:middle], right(top, middle, end))
            v_full[top:middle, middle:end] = -dot_full(product, v_full[middle:end, middle:end])

        invert(0, k)
        return halves(v_full[...])

    @pl.when(is_owner)
    def _():
        with scope("factor_loads"):
            loads[3].wait()
            for j in range(m):
                @pl.when(slot == j)
                def _():
                    loads[4 + j].wait()
        rest()
        base = slot * span
        high, low = inverted(slot * k, lambda top, middle, end: u_raw[
            top:middle, pl.ds(pl.multiple_of(base + middle, block), end - middle)
        ])
        v_high[...] = high
        v_low[...] = low

    @pl.when(jnp.logical_not(is_owner))
    def _():
        loads[3].wait()
        for j in range(m):
            loads[4 + j].wait()

        @pl.when((z == final) & is_last)
        def _():
            for row in reversed(range(1, final)):
                for i in range(k - 1):
                    tri_copy(row, i).start()

        rest()

    for j in range(m):
        @pl.when(is_owner & (slot != j))
        def _():
            loads[4 + j].wait()

    for j in range(m):
        @pl.when(c * m + j > z)
        def _():
            high, low = halves(u_raw[:, j * span:(j + 1) * span])
            u_high[:, j * span:(j + 1) * span] = high
            u_low[:, j * span:(j + 1) * span] = low

    def invert_last():
        @pl.when(z == final)
        def _():
            triangle[...] = u_raw[:, (m - 1) * span:]

        @pl.when(z < final)
        def _():
            with scope("wait_triangle"):
                if k > 1:
                    arrived(triangle.at[:block * (k - 1), :block * k // 2], tri_recv)

        high, low = inverted((m - 1) * k, lambda top, middle, end: triangle[top:middle, middle:end])
        w_high[...] = high
        w_low[...] = low

    @pl.when(z == 0)
    def _():
        enter()

    for j in range(m):
        send_delta(j, jnp.logical_not(urgent(j)))

    for j in range(m):
        @pl.when(code_sent(j))
        def _():
            code_copy(j).start()

        @pl.when((c == 0) & (z == j) & (z < final))
        def _():
            low = j * pairs // window * window
            codes_in[z] = assign[:, low:low + window]

    late_core = (z == 0) & (c > owner)
    relay_core = (z > 0) & (z < final) & (c > owner)

    def forward(q, j):
        with scope("wait_far_sum"):
            arrived(run_in.at[q, j], run_recv.at[q, j])
        run_out[q, j] = run_out[q, j] + run_in[q, j]
        run_copy(q, j).start()

    def stage(q, _):
        g = group(q)
        at = part_rows(q)

        turn = jnp.where(z == final, 0, PIECES)

        @pl.when(is_last & (z >= final - 1) & (q == turn))
        def _():
            invert_last()

        @pl.when((z > 0) & (z < nr - 2) & (q == (z + 1) * PIECES))
        def _():
            wait_ready()

        @pl.when(is_owner)
        def _():
            @pl.when(z == 0)
            def _():
                run_in[q, slot] = jnp.zeros((piece, span), F32)

            @pl.when(z > 0)
            def _():
                with scope("wait_own_sum"):
                    arrived(run_in.at[q, slot], run_recv.at[q, slot])

            @pl.when(g > z)
            def _():
                with scope("wait_delta"):
                    arrived(delta_in.at[g, at], core_recv.at[g * PIECES + q % PIECES])

                run_in[q, slot] = run_in[q, slot] + delta_in[g, at]

            @pl.when(g == z)
            def _():
                run_in[q, slot] = run_in[q, slot] + delta[slot, at]

            error = dot3(run_in[q, slot], v_high[...], v_low[...])
            err_block[q] = error

            @pl.when(g == z)
            def _():
                err_own[slot, at] = error

            for col in range(nc):
                @pl.when((col > c) | ((col == 0) & (c > 0)))
                def _():
                    core_copy(q, col).start()

            @pl.when((g < z) | ((g > z) & early_up(g)))
            def _():
                own_copy(q).start()

        @pl.when((c > owner) & (z < final))
        def _():
            with scope("wait_core"):
                arrived(err_block.at[q], core_recv.at[q])

        late = late_core & (q >= 2 * PIECES)
        @pl.when(is_last & (z < final))
        def _():
            j = m - 1
            change = dot3(
                err_block[q], u_high[:, j * span:(j + 1) * span], u_low[:, j * span:(j + 1) * span]
            )
            change = change - jnp.where((g == 0) & (z == 0), delta[j, at], 0.0)

            @pl.when((z <= 1) | (solver(g) != z))
            def _():
                last_out[q] = change

            @pl.when((z > 1) & (solver(g) == z))
            def _():
                last_in[first(g), q % PIECES, z] = change

            @pl.when((z > 1) & (solver(g) != z))
            def _():
                last_copy(q).start()

        for j in range(m):
            target = c * m + j

            @pl.when((target > z) & (target < final))
            def _():
                change = dot3(
                    err_block[q], u_high[:, j * span:(j + 1) * span], u_low[:, j * span:(j + 1) * span]
                )
                run_out[q, j] = jnp.where(g == z, delta[j, at], 0.0) - change

                @pl.when((z > 0) & jnp.logical_not(relay_core))
                def _():
                    with scope("wait_near_sum"):
                        arrived(run_in.at[q, j], run_recv.at[q, j])
                    run_out[q, j] = run_out[q, j] + run_in[q, j]

                @pl.when(jnp.logical_not(late | relay_core))
                def _():
                    run_copy(q, j).start()

                @pl.when(relay_core & (q >= PIECES))
                def _():
                    forward(q - PIECES, j)

        return 0

    lax.fori_loop(0, steps, stage, 0)

    @pl.when((z == 0) & (nr > 2))
    def _():
        wait_ready()

    def joined(q):
        with scope("wait_zero"):
            arrived(run_in.at[q, m - 1], run_recv.at[q, m - 1])
        return last_out[q] + run_in[q, m - 1]

    def contribute(low, high):
        @pl.when(late_core & is_last)
        def _():
            def release(i, _):
                zero_sum(zero_order(i)).start()
                return 0

            lax.fori_loop(low, high, release, 0)

        @pl.when(is_last & (z == 1) & (z < final))
        def _():
            def relayed(i, _):
                q = farthest(i)
                last_out[q] = joined(q)
                last_copy(q).start()
                return 0

            lax.fori_loop(low, min(high, steps - 2 * PIECES), relayed, 0)

    for j in range(m):
        @pl.when(late_core & (c * m + j < final))
        def _():
            def release(q, _):
                run_copy(q, j).start()
                return 0

            lax.fori_loop(2 * PIECES, steps - PIECES, release, 0)

    contribute(0, PIECES)

    for j in range(m):
        @pl.when((late_core | relay_core) & (c * m + j < final))
        def _():
            def release(q, _):
                @pl.when(z > 0)
                def _():
                    forward(q, j)

                @pl.when(z == 0)
                def _():
                    run_copy(q, j).start()

                return 0

            lax.fori_loop(steps - PIECES, steps, release, 0)

    contribute(PIECES, steps)

    @pl.when(is_last & (z > 0) & (z < final - 1))
    def _():
        invert_last()

    def send_up():
        def upward(i, _):
            q = nearest(i)

            @pl.when((group(q) > z) & jnp.logical_not(early_up(group(q))))
            def _():
                own_copy(q).start()

            return 0

        lax.fori_loop(0, steps, upward, 0)

    @pl.when(is_last & (z == 0))
    def _():
        with scope("wait_left"):
            arrived(last_out, last_send)

    @pl.when(is_last & (z < final))
    def _():
        send_up()

    def solved(which, h):
        with scope("wait_last"):
            if nr > 3:
                @pl.when(z < final)
                def _():
                    arrived(last_in.at[which, h, :nr - 3], last_recv.at[which, h])

            @pl.when(z == final)
            def _():
                arrived(last_in.at[which, h, :nr - 2], last_recv.at[which, h])
        total = -last_in[which, h, 1]
        for row in range(2, final):
            total = total - last_in[which, h, row]
        if which == 0:
            total = total + delta[m - 1, h * piece:(h + 1) * piece]
        return dot3(total, w_high[...], w_low[...])

    @pl.when(is_last & (z == 1))
    def _():
        for h in range(PIECES):
            last_in[1, h, 1] = joined(h)
            err_zero[h] = solved(1, h)
            zero_copy(h).start()
    high_count = code_count // LOW
    fold = 2 * high_count
    chunk = 16
    half = chunk // 2

    def count(error_at, code_at):
        def gather(step, total):
            at = pl.ds(pl.multiple_of(step * chunk, chunk), chunk)
            iota_high = lax.broadcasted_iota(jnp.int32, (high_count, block), 0)
            iota_low = lax.broadcasted_iota(jnp.int32, (LOW, block), 0)
            left, right = [], []
            even = lax.broadcasted_iota(jnp.int32, (half, block), 1) % 2 == 0
            for b in range(k):
                code = code_at(b, at)
                code = jnp.where(even, code[:half], code[half:])
                value = error_at[at, b * block:(b + 1) * block]
                value = value * value
                upper, lower = value[:half], value[half:]
                value = jnp.where(even, upper + pltpu.roll(upper, block - 1, 1), lower + pltpu.roll(lower, 1, 1))
                coarse = value.astype(BF16).astype(F32)
                fine = value - coarse
                code_high, code_low = code // LOW, code % LOW
                top, bottom, marks = [], [], []
                for r in range(half):
                    hit = jnp.broadcast_to(code_high[r:r + 1], (high_count, block)) == iota_high
                    top.append(jnp.where(hit, jnp.broadcast_to(coarse[r:r + 1], (high_count, block)), 0.0).astype(BF16))
                    bottom.append(jnp.where(hit, jnp.broadcast_to(fine[r:r + 1], (high_count, block)), 0.0).astype(BF16))
                    low_hit = jnp.broadcast_to(code_low[r:r + 1], (LOW, block)) == iota_low
                    marks.append(jnp.where(low_hit, 1.0, 0.0).astype(BF16))
                left += [jnp.concatenate(top, axis=1), jnp.concatenate(bottom, axis=1)]
                right.append(jnp.concatenate(marks, axis=1))
            return total + lax.dot_general(
                jnp.concatenate(left, axis=0), jnp.concatenate(right, axis=0),
                (((1,), (1,)), ((), ())), preferred_element_type=F32,
            )

        total = lax.fori_loop(0, piece // chunk, gather, jnp.zeros((k * fold, k * LOW), F32), unroll=2)
        tally[:, :k * LOW] = tally[:, :k * LOW] + total

    def spread(store):
        spot = lax.broadcasted_iota(jnp.int32, (high_count, block), 1)
        level = lax.broadcasted_iota(jnp.int32, (high_count, block), 0)
        for b in range(k):
            total = tally[b * fold:b * fold + high_count] + tally[b * fold + high_count:(b + 1) * fold]
            total = take(total, b * LOW + spot % LOW)
            for part in range(code_count // block):
                mine = level == part * (block // LOW) + spot // LOW
                store(b, part, jnp.sum(jnp.where(mine, total, 0.0), axis=0, keepdims=True))
        tally[...] = jnp.zeros_like(tally)

    tally[...] = jnp.zeros_like(tally)
    mass_all[z] = jnp.zeros(mass_all.shape[1:], F32)
    counts = (c == 0) & (z < final)

    def row_sums(error):
        return lax.dot_general(
            jnp.ones((8, span), F32), error * error, (((1,), (1,)), ((), ())),
            precision=lax.Precision.HIGHEST, preferred_element_type=F32,
        )

    def up_copy(row, col):
        return remote(loss_up.at[row], loss_in.at[z], up_send, up_recv, row, col)

    def part_copy(row):
        return remote(mass_sent, mass_own.at[slot], part_send, part_recv.at[slot], row, owner)

    def part_remote(row):
        return counts & ((row != z) | (owner != 0))

    for row in range(final):
        for other in range(2):
            number = final - row + other

            @pl.when(counts & (z == row) & ((owner != 0) == (other == 1)))
            def _():
                with scope("wait_code"):
                    arrived(codes_in.at[:number], code_recv)

    @pl.when(counts)
    def _():
        def own_part(q, _):
            g = group(q)

            @pl.when(owner != 0)
            def _():
                with scope("wait_part"):
                    arrived(err_block.at[q], core_recv.at[q])

            @pl.when(g >= z)
            def _():
                shift = 0 if window == pairs else lax.rem(slot * pairs, window)

                def code_at(b, at):
                    low = b * (block // 2)
                    tile = low // block * block
                    source = codes_in[g, pl.ds(q % PIECES * piece + at.start, chunk), tile:tile + block]
                    return take(source, shift + low - tile + lane[:chunk] // 2)

                count(err_block.at[q], code_at)

            @pl.when((g > z) & (q % PIECES == PIECES - 1))
            def _():
                error = jnp.concatenate([err_block[q - PIECES + 1 + h] for h in range(PIECES)], axis=0)
                loss_up[g, :, :rows] = row_sums(error)
                for col in range(nc):
                    up_copy(g, col).start()

            return 0

        lax.fori_loop(0, steps, own_part, 0)

        def store(b, part, value):
            mass_sent[b:b + 1, part * block:(part + 1) * block] = value

        spread(store)

        @pl.when(owner == 0)
        def _():
            mass_own[slot] = mass_sent[...]

    for row in range(nr):
        @pl.when(part_remote(row))
        def _():
            part_copy(row).start()

    def own_spread(j):
        def store(b, part, value):
            mass_all[z, j * k + b:j * k + b + 1, part * block:(part + 1) * block] = value

        spread(store)

    for j in range(m):
        @pl.when((c * m + j > z) & ((c * m + j < final) | (z == 0)))
        def _():
            for h in range(PIECES):
                with scope("wait_down"):
                    arrived(err_own.at[j, h * piece:(h + 1) * piece], own_recv.at[j, h])
                count(
                    err_own.at[j, h * piece:(h + 1) * piece],
                    lambda b, at: codes[j * k + b, pl.ds(h * piece + at.start, chunk), :],
                )
            own_spread(j)

    @pl.when(is_last & (z > 0))
    def _():
        j = m - 1

        @pl.when(z == 1)
        def _():
            for h in range(PIECES):
                last_in[0, h, 1] = joined(PIECES + h)

        for h in range(PIECES):
            err_own[j, h * piece:(h + 1) * piece] = solved(0, h)
            count(
                err_own.at[j, h * piece:(h + 1) * piece],
                lambda b, at: codes[j * k + b, pl.ds(h * piece + at.start, chunk), :],
            )
        own_spread(j)

    def mass_copy(row):
        return remote(mass_all.at[z], mass_all.at[z], mass_send, mass_recv, row, c)

    def loss_copy(col):
        return remote(loss_all.at[c], loss_all.at[c], loss_send, loss_recv, z, col)

    with scope("send_mass"):
        for row in range(nr):
            @pl.when(row != z)
            def _():
                mass_copy(row).start()

    loss_all[c] = jnp.zeros(loss_all.shape[1:], F32)
    for j in range(m):
        @pl.when((c * m + j >= z) & ((c * m + j < final) | is_last))
        def _():
            loss_all[c, :, :rows] = loss_all[c, :, :rows] + row_sums(err_own[j])

    for col in range(nc):
        @pl.when(col != c)
        def _():
            loss_copy(col).start()

    for j in range(m):
        @pl.when(c * m + j < z)
        def _():
            arrived(delta.at[j], d_send.at[j])

        @pl.when(code_sent(j))
        def _():
            code_copy(j).wait_send()

        @pl.when((c * m + j > z) & (c * m + j < final))
        def _():
            arrived(run_out.at[:, j], run_send.at[j])

    if k > 1:
        @pl.when((z == final) & is_last)
        def _():
            arrived(u_raw.at[:, :(nr - 2) * block * (k - 1) // 2], tri_send)

    @pl.when(is_last & (z == 1))
    def _():
        arrived(last_out.at[:steps - 2 * PIECES], last_send)
        arrived(err_zero, zero_send)

    @pl.when(is_last & (z > 1) & (z < final))
    def _():
        arrived(last_out.at[:steps - PIECES], last_send)

    for col in range(nc):
        @pl.when(is_owner & ((col > c) | ((col == 0) & (c > 0))))
        def _():
            arrived(err_block, core_send.at[col])

    for row in range(final):
        early = 1 if row > 0 and row // m < nc - 1 else 0
        up = final - row - early
        both = row // m == nc - 1

        @pl.when((z == row) & is_owner)
        def _():
            number = row + early + (up if both else 0)
            if number:
                arrived(err_block.at[:number * PIECES], own_send)

        if not both and up:
            @pl.when((z == row) & is_last)
            def _():
                arrived(err_block.at[:up * PIECES], own_send)

    part_size = mass_all.at[:, :k]

    @pl.when(counts)
    def _():
        for row in range(final):
            @pl.when(z == row)
            def _():
                arrived(loss_up.at[:(final - row) * nc], up_send)

        @pl.when(owner == 0)
        def _():
            arrived(part_size.at[:nr - 1], part_send)

        @pl.when(owner != 0)
        def _():
            arrived(part_size, part_send)

    arrived(mass_all.at[:nr - 1], mass_send)
    arrived(loss_all.at[:nc - 1], loss_send)

    for j in reversed(range(m)):
        @pl.when(c * m + j < z)
        def _():
            with scope("wait_up"):
                for h in range(PIECES):
                    arrived(err_own.at[j, h * piece:(h + 1) * piece], own_recv.at[j, h])

        errors_out[:, j * span:(j + 1) * span] = err_own[j]

    with scope("wait_loss"):
        arrived(loss_all.at[:nc - 1], loss_recv)
    loss_sum = loss_all[0, 0:1, :rows]
    for col in range(1, nc):
        loss_sum = loss_sum + loss_all[col, 0:1, :rows]
    loss_out[...] = loss_sum
    for row in range(1, nr):
        @pl.when(z == row)
        def _():
            with scope("wait_loss_up"):
                arrived(loss_in.at[:row], up_recv)
            total = loss_out[...]
            for lower in range(row):
                total = total + loss_in[lower, 0:1, :rows]
            loss_out[...] = total

    for j in range(m):
        @pl.when((c * m + j < final) & ((c * m + j != z) | (c != 0)))
        def _():
            with scope("wait_mass_part"):
                arrived(mass_own.at[j], part_recv.at[j])

    with scope("wait_mass"):
        arrived(mass_all.at[:nr - 1], mass_recv)
    mass_sum = mass_all[0]
    for row in range(1, nr):
        mass_sum = mass_sum + mass_all[row]
    mass_out[...] = mass_sum
    for j in range(m):
        @pl.when(c * m + j < final)
        def _():
            mass_out[j * k:(j + 1) * k, :] = mass_out[j * k:(j + 1) * k, :] + mass_own[j]


def store(errors, loss, mass, errors_out, loss_out, mass_out, sems):
    copies = [
        pltpu.make_async_copy(source, target, sems.at[number])
        for number, (source, target) in enumerate(((errors, errors_out), (loss, loss_out), (mass, mass_out)))
    ]
    for copy in copies:
        copy.start()
    for copy in copies:
        copy.wait()


def local(nr, nc, weights, codebook, assign, chol_upper, inv_blocks):
    rows, width = weights.shape[1:]
    span = chol_upper.shape[1]
    m = width // span
    steps, piece = nr * PIECES, rows // PIECES
    blocks, code_count = codebook.shape[1], codebook.shape[3]
    block = inv_blocks.shape[2]
    k = span // block
    dma = pltpu.SemaphoreType.DMA
    vmem = pl.BlockSpec(memory_space=pltpu.VMEM)
    hbm = pl.BlockSpec(memory_space=pltpu.HBM)
    shapes = ((rows, width), (1, rows), (blocks, code_count))
    results = pl.pallas_call(
        functools.partial(kernel, nr, nc),
        out_shape=tuple(pltpu.VMEM(shape, F32) for shape in shapes),
        in_specs=[hbm] * 5,
        out_specs=(vmem, vmem, vmem),
        scratch_shapes=[
            pltpu.VMEM(weights.shape[1:], F32),
            pltpu.VMEM(codebook.shape[1:], F32),
            pltpu.VMEM(assign.shape[1:], jnp.int32),
            pltpu.VMEM(inv_blocks.shape[1:], F32),
            pltpu.VMEM((span, width), F32),
            pltpu.VMEM((span, width), BF16),
            pltpu.VMEM((span, width), BF16),
            pltpu.VMEM((span, span), F32),
            pltpu.VMEM((span, span), F32),
            pltpu.VMEM((span, span), BF16),
            pltpu.VMEM((span, span), BF16),
            pltpu.VMEM((span, span), BF16),
            pltpu.VMEM((span, span), BF16),
            pltpu.VMEM((m, rows, span), F32),
            pltpu.VMEM((blocks, rows, block), jnp.int32),
            pltpu.VMEM((nr, rows, span), F32),
            pltpu.VMEM((nr, rows, max(span // 2, block)), jnp.int32),
            pltpu.VMEM((steps, m, piece, span), F32),
            pltpu.VMEM((steps, m, piece, span), F32),
            pltpu.VMEM((2, PIECES, nr, piece, span), F32),
            pltpu.VMEM((steps, piece, span), F32),
            pltpu.VMEM((steps, piece, span), F32),
            pltpu.VMEM((m, rows, span), F32),
            pltpu.VMEM((PIECES, piece, span), F32),
            pltpu.VMEM((k * 2 * (code_count // LOW), block), F32),
            pltpu.VMEM((nr, blocks, code_count), F32),
            pltpu.VMEM((m, k, code_count), F32),
            pltpu.VMEM((k, code_count), F32),
            pltpu.VMEM((nc, 8, max(rows, 128)), F32),
            pltpu.VMEM((nr * nc, 8, max(rows, 128)), F32),
            pltpu.VMEM((nr, 8, max(rows, 128)), F32),
            dma((4 + m,)),
            dma((m,)),
            dma((m,)), dma,
            dma, dma,
            dma((m,)), dma((steps, m)),
            dma, dma((2, PIECES)),
            dma((nc,)), dma((steps,)),
            dma, dma((m, PIECES)), dma,
            dma, dma((m,)),
            dma, dma,
            dma, dma,
            dma, dma, pltpu.SemaphoreType.REGULAR,
        ],
        compiler_params=pltpu.CompilerParams(
            collective_id=0, has_side_effects=True, vmem_limit_bytes=40 * 1024 * 1024
        ),
    )(*(pltpu.with_memory_space_constraint(value[0], pltpu.HBM) for value in (
        weights, codebook, assign, inv_blocks, chol_upper,
    )))
    errors, loss, mass = pl.pallas_call(
        store,
        out_shape=tuple(jax.ShapeDtypeStruct(shape, F32) for shape in shapes),
        in_specs=[vmem] * 3,
        out_specs=[hbm] * 3,
        scratch_shapes=[dma((3,))],
        compiler_params=pltpu.CompilerParams(vmem_limit_bytes=1024 * 1024),
    )(*results)
    return errors[None], loss, mass[None]


def solution(mesh):
    return jax.shard_map(
        functools.partial(local, mesh.shape["row"], mesh.shape["col"]),
        mesh=mesh,
        in_specs=(
            P("ea", "row", "col"),
            P("ea", "col", None, None),
            P("ea", "row", "col"),
            P("ea", "row", "col"),
            P("ea", "col", None, None),
        ),
        out_specs=(P("ea", "row", "col"), P("ea", "row"), P("ea", "col", None)),
        check_vma=False,
    )
```
